128 devices in a mesh: gx: 8 (over z, core), gy: 16 (over x, y).
Axes of the slice: x: 4, y: 4, z: 4, core: 2. Of those that a mesh axis runs over, the one named last changes fastest.
Arguments:
- tprime: float32 [512, 512, 128], P('gx', 'gy'), may hold values from -5 to 5
- vapor: float32 [512, 512, 128], P('gx', 'gy'), may hold values from -0.2 to 0.2
- wind_u: float32 [512, 512, 128], P('gx', 'gy'), may hold values from -2.5 to 2.5
- wind_v: float32 [512, 512, 128], P('gx', 'gy'), may hold values from -2.5 to 2.5
- wind_w: float32 [512, 512, 128], P('gx', 'gy'), may hold values from -2.5 to 2.5
- radius: float32 [131072, 128], P(('gx', 'gy')), may hold values from 4 to 20
- min_radius: float32 [131072, 128], P(('gx', 'gy')), may hold values from 1 to 4
- multiplicity: float32 [131072, 128], P(('gx', 'gy')), may hold values from 0.5 to 2
- drop_counts: int32 [131072], P(('gx', 'gy')), may hold values from 0 to 128, as said below
- cell_index: int32 [131072], P(('gx', 'gy')), may hold values from 0 to 262143
- move_list: int32 [131072], P(('gx', 'gy')), may hold values from -1 to 1023, as said below
Outputs:
- temperature_out: float32 [512, 512, 128], P('gx', 'gy')
- vapor_out: float32 [512, 512, 128], P('gx', 'gy')
- radius_out: float32 [65536, 128], P(('gx', 'gy'))
- multiplicity_out: float32 [65536, 128], P(('gx', 'gy'))
The draws below stay inside these ranges and needn't reach their ends.
Inputs may be any that keep to these rules, and one draw needn't show every extreme that they name: `move_list`: each entry is -1 for an empty home slot, else o * 8 + k: the block goes to owner o as the k-th block from its device to o. Within one device no value repeats, every owner receives exactly 512 blocks, some device holds 1024 live blocks and uses k = 7. `drop_counts`: 0 exactly in the home slots whose move_list entry is -1, else 1 to 128.
All inputs are finite; a program needn't handle non-finite values.
Results may differ from the reference program's by a relative error of at most 0.0003.
Values sent between devices are 32-bit elements; how exact they have to be, the bound alone decides.
A program may use at most 64 MiB of HBM per device.

```python
import math
import jax
import jax.numpy as jnp
from jax import lax

CX = 64
CY = 32
CZ = 128
DROPS = 128
SUBSTEPS = 6
BLK_DEV = 512
HOME = 1024
CAP = 8
NX = 512
NY = 512
HOME_ALL = 131072
N_GX = 8
N_GY = 16
DEVICES = 128


def layout(key):
    base = jax.random.fold_in(key, 11)
    keys = jax.random.split(base, 5)
    half = DEVICES // 2
    shuffled = jax.random.permutation(keys[0], DEVICES).astype(jnp.int32)
    extra = jax.random.randint(keys[1], (half,), 0, HOME - BLK_DEV + 1, dtype=jnp.int32)
    extra = extra.at[0].set(HOME - BLK_DEV)
    loads = jnp.zeros((DEVICES,), jnp.int32).at[shuffled[0::2]].set(BLK_DEV + extra).at[shuffled[1::2]].set(BLK_DEV - extra)
    slot_keys = jax.random.split(keys[2], DEVICES)
    ranks = jax.vmap(lambda k: jax.random.permutation(k, HOME))(slot_keys).astype(jnp.int32)
    live = ranks < loads[:, None]
    within = (jnp.cumsum(live.astype(jnp.int32), axis=1) - 1).astype(jnp.int32)
    before = (jnp.cumsum(loads) - loads).astype(jnp.int32)
    global_rank = before[:, None] + within
    owners = jax.random.permutation(keys[3], DEVICES).astype(jnp.int32)
    owner = owners[global_rank % DEVICES]
    code = jnp.where(live, owner * CAP + within // DEVICES, -1).astype(jnp.int32)
    drawn = jax.random.randint(keys[4], (DEVICES, HOME), 1, DROPS + 1, dtype=jnp.int32)
    counts = jnp.where(live, drawn, 0).astype(jnp.int32)
    return (code.reshape(-1), counts.reshape(-1))


def draw_move_list(key, part):
    return layout(key)[0]


def draw_drop_counts(key, part):
    return layout(key)[1]


def with_ends(values, rng, smallest, largest):
    index_at = [jax.random.randint(jax.random.fold_in(rng, axis), (), 0, length) for axis, length in enumerate(values.shape)]
    main_axis = values.shape.index(max(values.shape))
    next_to = index_at[:main_axis] + [(index_at[main_axis] + 1) % values.shape[main_axis]] + index_at[main_axis + 1:]
    return values.at[tuple(index_at)].set(smallest).at[tuple(next_to)].set(largest)


def steps_of(stream_key, shape, cuts, smallest, high):
    factor_of = 1.0
    for axis_at, parts in cuts:
        draws = jax.random.uniform(jax.random.fold_in(jax.random.fold_in(stream_key, 6), axis_at), (parts,), jnp.float32, smallest / len(cuts), high / len(cuts))
        factor_of = factor_of * jnp.repeat(jnp.exp(draws), shape[axis_at] // parts).reshape((-1,) + (1,) * (len(shape) - 1 - axis_at))
    return factor_of


def gaussian(key, dims, deviation, bound, cuts=(), kind=jnp.bfloat16):
    values = deviation * jax.random.normal(key, dims, jnp.float32)
    if cuts:
        values = values * steps_of(key, dims, cuts, -0.22, 0.18)
    return jnp.clip(values, -bound, bound).astype(kind)


def setup_inputs(seed: int = 0) -> dict:
    seeds = jax.random.split(jax.random.key(seed), 12)
    tprime = gaussian(seeds[0], (NX, NY, CZ), 1.0, 5.0, ((0, 8), (1, 16)), jnp.float32)
    vapor = gaussian(seeds[1], (NX, NY, CZ), 0.03, 0.2, ((0, 8), (1, 16)), jnp.float32)
    wind_u = gaussian(seeds[2], (NX, NY, CZ), 0.4, 2.5, ((0, 8), (1, 16)), jnp.float32)
    wind_v = gaussian(seeds[3], (NX, NY, CZ), 0.4, 2.5, ((0, 8), (1, 16)), jnp.float32)
    wind_w = gaussian(seeds[4], (NX, NY, CZ), 0.4, 2.5, ((0, 8), (1, 16)), jnp.float32)
    radius = jnp.clip(jnp.exp(math.log(20.0) - 1.609438 * jax.random.uniform(seeds[5], (HOME_ALL, DROPS), jnp.float32) ** steps_of(seeds[5], (HOME_ALL, DROPS), ((0, 128),), -0.2, 0.2)), 4.0, 20.0)
    min_radius = jnp.clip(jnp.exp(math.log(4.0) - 1.3862944 * jax.random.uniform(seeds[6], (HOME_ALL, DROPS), jnp.float32) ** steps_of(seeds[6], (HOME_ALL, DROPS), ((0, 128),), -0.2, 0.2)), 1.0, 4.0)
    multiplicity = jnp.clip(jnp.exp(math.log(2.0) - 1.3862944 * jax.random.uniform(seeds[7], (HOME_ALL, DROPS), jnp.float32) ** steps_of(seeds[7], (HOME_ALL, DROPS), ((0, 128),), -0.2, 0.2)), 0.5, 2.0)
    drop_counts = draw_drop_counts(jax.random.fold_in(seeds[11], 71), 0)
    cell_index = with_ends(jax.random.randint(seeds[9], (HOME_ALL,), 0, CX * CY * CZ), jax.random.fold_in(seeds[9], 1), 0, (CX * CY * CZ) - 1).astype(jnp.int32)
    move_list = draw_move_list(jax.random.fold_in(seeds[11], 71), 0)
    return {"tprime": tprime, "vapor": vapor, "wind_u": wind_u, "wind_v": wind_v, "wind_w": wind_w, "radius": radius, "min_radius": min_radius, "multiplicity": multiplicity, "drop_counts": drop_counts, "cell_index": cell_index, "move_list": move_list}


clausius = 0.07
growth = 200.0 / 3.0
solute = 0.05
condense = 5e-07
latent = 10.0
collect = 1e-07
time_step = 2.0
advect_step = 0.6

def physics(radius, floor_radius, mult, cell_temp, cell_vapor):
    r2 = radius * radius
    floor2 = floor_radius * floor_radius
    temp = cell_temp
    wet = cell_vapor
    for _ in range(SUBSTEPS):
        sat = (1.0 + wet) * jnp.exp(-clausius * temp) - 1.0
        rad = jnp.sqrt(r2)
        ratio = floor_radius / rad
        grown = jnp.maximum(r2 + growth * (sat[:, None] + solute * ratio * ratio * ratio), floor2)
        condensed = lax.optimization_barrier(jnp.sum(mult * (grown * jnp.sqrt(grown) - r2 * rad), axis=1))
        wet = wet - condense * condensed
        temp = temp + latent * condense * condensed
        r2 = grown
    rad = jnp.sqrt(r2)
    mass = r2 * rad
    summed = rad[:, :, None] + rad[:, None, :]
    kernel = summed * summed * jnp.abs(r2[:, :, None] - r2[:, None, :])
    sweep = jnp.where(rad[:, :, None] > rad[:, None, :], kernel, 0.0)
    gain = collect * lax.optimization_barrier(jnp.sum(sweep * (mult * mass)[:, None, :], axis=2))
    loss = collect * lax.optimization_barrier(jnp.sum(sweep * mult[:, :, None], axis=1))
    radius_new = jnp.where(mult > 0.0, jnp.cbrt(mass + time_step * gain), 0.0)
    mult_new = mult * jnp.exp(-time_step * loss)
    heat = jnp.stack([temp - cell_temp, wet - cell_vapor], axis=1)
    return (radius_new, mult_new, heat)

def grouped(items, limit):
    count = items[0].shape[0]
    group = math.gcd(count, limit)

    def apply(pieces):
        return physics(*pieces)
    stacked = tuple((a.reshape((count // group, group) + a.shape[1:]) for a in items))
    result = lax.map(apply, stacked)
    return tuple((a.reshape((count,) + a.shape[2:]) for a in result))

def tendency(padded, along_x, along_y, along_z):
    middle_y = padded[:, :, 1:-1]
    flux_x = along_x * (0.5 * (middle_y[:, :-1] + middle_y[:, 1:]))
    middle_x = padded[:, 1:-1]
    flux_y = along_y * (0.5 * (middle_x[:, :, :-1] + middle_x[:, :, 1:]))
    core = padded[:, 1:-1, 1:-1]
    flux_z = along_z * (0.5 * (core[..., :-1] + core[..., 1:]))
    edge = jnp.zeros(core.shape[:-1] + (1,), core.dtype)
    flux_z = jnp.concatenate([edge, flux_z, edge], axis=-1)
    return -(flux_x[:, 1:] - flux_x[:, :-1]) - (flux_y[:, :, 1:] - flux_y[:, :, :-1]) - (flux_z[..., 1:] - flux_z[..., :-1])

def wrapped(stacked):
    return jnp.pad(stacked, ((0, 0), (1, 1), (1, 1), (0, 0)), mode='wrap')

def reference(tprime, vapor, wind_u, wind_v, wind_w, radius, min_radius, multiplicity, drop_counts, cell_index, move_list):
    devices = N_GX * N_GY
    home_all = radius.shape[0]
    blocks = jnp.arange(home_all, dtype=jnp.int32)
    device = (blocks // HOME).astype(jnp.int32)
    live = move_list >= 0
    owner = jnp.where(live, move_list // CAP, devices).astype(jnp.int32)
    column = (device * CAP + jnp.where(live, move_list % CAP, 0)).astype(jnp.int32)
    table = jnp.full((devices, devices * CAP), home_all, jnp.int32).at[owner, column].set(blocks, mode='drop')
    filled = table < home_all
    position = (jnp.cumsum(filled.astype(jnp.int32), axis=1) - 1).astype(jnp.int32)
    position = jnp.where(filled, position, BLK_DEV).astype(jnp.int32)
    rows = jnp.broadcast_to(jnp.arange(devices, dtype=jnp.int32)[:, None], table.shape)
    chosen = jnp.zeros((devices, BLK_DEV), jnp.int32).at[rows, position].set(table, mode='drop').reshape(-1)
    local_x = cell_index // (CY * CZ)
    local_y = cell_index // CZ % CY
    level = cell_index % CZ
    global_x = device // N_GY * CX + local_x
    global_y = device % N_GY * CY + local_y
    flat = ((global_x * NY + global_y) * CZ + level).astype(jnp.int32)
    cell_temp = tprime.reshape(-1)[flat]
    cell_vapor = vapor.reshape(-1)[flat]
    alive = jnp.arange(DROPS, dtype=jnp.int32)[None, :] < drop_counts[:, None]
    live_mult = jnp.where(alive, multiplicity, 0.0)
    radius_out, multiplicity_out, heat = grouped((radius[chosen], min_radius[chosen], live_mult[chosen], cell_temp[chosen], cell_vapor[chosen]), 256)
    home_heat = jnp.zeros((home_all, 2), heat.dtype).at[chosen].set(heat)
    heated_t = tprime.reshape(-1).at[flat].add(jnp.where(live, home_heat[:, 0], 0.0)).reshape(tprime.shape)
    heated_v = vapor.reshape(-1).at[flat].add(jnp.where(live, home_heat[:, 1], 0.0)).reshape(vapor.shape)
    winds = wrapped(jnp.stack([wind_u, wind_v]))
    along_x = 0.5 * (winds[0, :-1, 1:-1] + winds[0, 1:, 1:-1])
    along_y = 0.5 * (winds[1, 1:-1, :-1] + winds[1, 1:-1, 1:])
    along_z = 0.5 * (wind_w[..., :-1] + wind_w[..., 1:])
    start = jnp.stack([heated_t, heated_v])
    section = start
    for weight in (1.0 / 3.0, 0.5, 1.0):
        section = start + advect_step * weight * tendency(wrapped(section), along_x, along_y, along_z)
    return (section[0], section[1], radius_out, multiplicity_out)
```

```python
import jax
import jax.numpy as jnp
from jax import lax
from jax.experimental import pallas as pl
from jax.experimental.pallas import tpu as pltpu
from jax.sharding import PartitionSpec as P

SUBSTEPS = 6
BLK_DEV = 512


clausius = 0.07
growth = 200.0 / 3.0
solute = 0.05
condense = 5e-07
latent = 10.0
collect = 1e-07
time_step = 2.0
advect_step = 0.6


def cut_along(array, dim, size):
    before, after = (array.shape[:dim], array.shape[dim + 1 :])
    return jnp.moveaxis(array.reshape(*before, size, -1, *after), dim, 0)


def laid_out(parts, dim):
    lengths = list(parts.shape[1:])
    lengths[dim] *= parts.shape[0]
    return jnp.moveaxis(parts, 0, dim).reshape(lengths)


def exchange_both(array, axis, axes, splits, concats):
    sizes = [lax.axis_size(a) for a in axes]
    parts = cut_along(array, splits[0], sizes[0])
    parts = jnp.moveaxis(cut_along(parts, splits[1] + 1, sizes[1]), 0, 1)
    inside = parts.shape[2:]
    parts = parts.reshape(-1, *inside)
    parts = lax.all_to_all(parts, axis, split_axis=0, concat_axis=0, tiled=True)
    parts = laid_out(parts.reshape(*sizes, *inside), concats[0] + 1)
    return laid_out(parts, concats[1])


def with_halo(array, sides, width):
    edges = {}
    for axis, dim in sides:
        size, length = (lax.axis_size(axis), array.shape[dim])
        up = [(i, (i + 1) % size) for i in range(size)]
        last = lax.slice_in_dim(array, length - width, length, axis=dim)
        first = lax.slice_in_dim(array, 0, width, axis=dim)
        edges[dim] = (
            lax.ppermute(last, axis, up),
            lax.ppermute(first, axis, [(b, a) for a, b in up]),
        )
    done = []
    for _, dim in sides:
        low, high = edges[dim]
        around = [(width, width) if d in done else (0, 0) for d in range(array.ndim)]
        array = jnp.concatenate([jnp.pad(low, around), array, jnp.pad(high, around)], axis=dim)
        done.append(dim)
    return array


def batcher(n):
    out = []
    p = 1
    while p < n:
        k = p
        while k >= 1:
            for j in range(k % p, n - k, 2 * k):
                for i in range(min(k, n - j - k)):
                    if (i + j) // (2 * p) == (i + j + k) // (2 * p):
                        out.append((i + j, i + j + k))
            k //= 2
        p *= 2
    return out

NET16 = batcher(16)

def halves(top, n=16):
    out = []
    d = top
    while d >= 1:
        for i in range(n):
            if not i & d:
                out.append((i, i + d))
        d //= 2
    return out

def make_passes():
    passes = []
    up, down = list(range(16)), list(range(15, -1, -1))
    passes.append((4, [(lambda t: t * 32, up, up, NET16), (lambda t: t * 32, [16 + o for o in up], [16 + o for o in down], NET16)]))
    for level in (32, 64, 128):
        step = level // 16
        if level == 128:
            passes.append((step, [(lambda t: t, [step * o for o in up], [step * o for o in up], halves(8))]))
        else:
            per = step
            passes.append((128 // level, [(lambda t, b=b, level=level: t * level + b, [step * o for o in up], [step * o for o in up], halves(8)) for b in range(per)]))
        ces = halves(step // 2)
        if level == 128:
            passes.append((8, [(lambda t: t * 16, up, up, ces)]))
        else:
            sets = []
            for s in range(2 * level // 16):
                loads = [16 * s + o for o in up]
                stores = loads if s * 16 < level else [level + 2 * level - 1 - o for o in loads]
                sets.append((lambda t, level=level: t * 2 * level, loads, stores, ces))
            passes.append((128 // (2 * level), sets))
    return passes

PASSES = make_passes()
N_CE = sum(trips * sum(len(s[3]) for s in sets) for trips, sets in PASSES)

def moves(sets):
    return any(set(s[1]) != set(s[2]) for s in sets)

def row(ref, d):
    if isinstance(d, int):
        return ref.at[pl.ds(d * 8, 8), :]
    return ref.at[pl.ds(pl.multiple_of(d * 8, 8), 8), :]

def loop(trips, body):
    if trips == 1:
        body(0)
    else:
        def step(t, c):
            body(t)
            return c
        lax.fori_loop(0, trips, step, 0)

def sort_blocks(keys, vals, marks):
    at = 0
    side = 0
    for trips, sets in PASSES:
        count = sum(len(s[3]) for s in sets)
        key, val = keys[side], vals[side]
        if moves(sets):
            side = 1 - side
        key_to, val_to = keys[side], vals[side]
        def body(t, sets=sets, at=at, count=count, key=key, val=val, key_to=key_to, val_to=val_to):
            m = at + t * count
            for base, loads, stores, ces in sets:
                b = base(t)
                ks = [row(key, b + o)[...] for o in loads]
                vs = [row(val, b + o)[...] for o in loads]
                for i, j in ces:
                    c = ks[i] > ks[j]
                    row(marks, m)[...] = jnp.where(c, 1.0, 0.0)
                    m = m + 1
                    ks[i], ks[j] = jnp.minimum(ks[i], ks[j]), jnp.maximum(ks[i], ks[j])
                    vs[i], vs[j] = jnp.where(c, vs[j], vs[i]), jnp.where(c, vs[i], vs[j])
                for o, k, v in zip(stores, ks, vs):
                    row(key_to, b + o)[...] = k
                    row(val_to, b + o)[...] = v
        loop(trips, body)
        at += trips * count

def unsort_blocks(firsts, seconds, marks):
    at = N_CE
    side = 0
    for trips, sets in reversed(PASSES):
        count = sum(len(s[3]) for s in sets)
        at -= trips * count
        xa, xb = firsts[side], seconds[side]
        if moves(sets):
            side = 1 - side
        xa_to, xb_to = firsts[side], seconds[side]
        def body(t, sets=sets, at=at, count=count, xa=xa, xb=xb, xa_to=xa_to, xb_to=xb_to):
            m = at + t * count
            for base, loads, stores, ces in sets:
                b = base(t)
                xs = [row(xa, b + o)[...] for o in stores]
                ys = [row(xb, b + o)[...] for o in stores]
                for q in reversed(range(len(ces))):
                    i, j = ces[q]
                    c = row(marks, m + q)[...] > 0.5
                    xs[i], xs[j] = jnp.where(c, xs[j], xs[i]), jnp.where(c, xs[i], xs[j])
                    ys[i], ys[j] = jnp.where(c, ys[j], ys[i]), jnp.where(c, ys[i], ys[j])
                m = m + len(ces)
                for o, x, y in zip(loads, xs, ys):
                    row(xa_to, b + o)[...] = x
                    row(xb_to, b + o)[...] = y
        loop(trips, body)

def physics_kernel(rad_ref, flo_ref, mul_ref, cnt_ref, ct_ref, cv_ref, ro_ref, mo_ref, heat_ref, R, S, C, F, M, marks):
    def enter(g, c):
        at = pl.ds(pl.multiple_of(g * 128, 128), 128)
        to = pl.ds(g, 128, stride=8)
        R[to, :] = rad_ref[at, :].T
        F[to, :] = flo_ref[at, :].T
        M[to, :] = mul_ref[at, :].T
        return c
    lax.fori_loop(0, 8, enter, 0)
    counts = cnt_ref[...]
    zero = jnp.zeros((8, 128), jnp.float32)
    U = 8

    def init(t, w):
        for u in range(U):
            d = t * U + u
            r = row(R, d)[...]
            f = row(F, d)[...]
            m = jnp.where(counts > d, row(M, d)[...], 0.0)
            r2 = r * r
            f2 = f * f
            row(M, d)[...] = m
            row(R, d)[...] = r2
            row(S, d)[...] = lax.rsqrt(r2)
            row(F, d)[...] = f2
            row(C, d)[...] = (growth * solute) * f2 * f
            w = w + m * (r2 * r)
        return w
    weight = lax.fori_loop(0, 128 // U, init, zero)
    temp = ct_ref[...]
    wet = cv_ref[...]
    for _ in range(SUBSTEPS):
        sat = growth * ((1.0 + wet) * jnp.exp(-clausius * temp) - 1.0)
        def sub(t, w):
            for u in range(U):
                d = t * U + u
                r2 = row(R, d)[...]
                rs = row(S, d)[...]
                g = jnp.maximum(r2 + (sat + row(C, d)[...] * (rs * rs * rs)), row(F, d)[...])
                ns = lax.rsqrt(g)
                row(R, d)[...] = g
                row(S, d)[...] = ns
                w = w + row(M, d)[...] * (g * (g * ns))
            return w
        after = lax.fori_loop(0, 128 // U, sub, zero)
        condensed = after - weight
        weight = after
        wet = wet - condense * condensed
        temp = temp + latent * condense * condensed
    heat_ref[0] = temp - ct_ref[...]
    heat_ref[1] = wet - cv_ref[...]

    def radii(t, c):
        for u in range(U):
            d = t * U + u
            row(R, d)[...] = row(R, d)[...] * row(S, d)[...]
        return c
    lax.fori_loop(0, 128 // U, radii, 0)
    sort_blocks((R, S), (M, C), marks)

    def both(t, carry):
        a0, a1, a3, a4, b0, b1, b3, b4 = carry
        for u in range(U):
            d = t * U + u
            r = row(R, d)[...]
            m = row(M, d)[...]
            r2 = r * r
            r3 = r2 * r
            r4 = r2 * r2
            gain = r4 * a0 + 2.0 * (r3 * a1 - r * a3) - a4
            w = m * r3
            a0 = a0 + w
            a1 = a1 + w * r
            a3 = a3 + w * r3
            a4 = a4 + w * r4
            grown = r3 + (time_step * collect) * gain
            row(S, d)[...] = jnp.where(m > 0.0, jnp.exp(jnp.log(grown) * (1.0 / 3.0)), 0.0)
            d = 127 - d
            r = row(R, d)[...]
            m = row(M, d)[...]
            r2 = r * r
            r3 = r2 * r
            r4 = r2 * r2
            loss = b4 + 2.0 * (r * b3 - r3 * b1) - r4 * b0
            b0 = b0 + m
            b1 = b1 + m * r
            b3 = b3 + m * r3
            b4 = b4 + m * r4
            row(C, d)[...] = m * jnp.exp((-time_step * collect) * loss)
        return a0, a1, a3, a4, b0, b1, b3, b4
    lax.fori_loop(0, 128 // U, both, (zero,) * 8)
    unsort_blocks((S, R), (C, F), marks)

    def leave(g, c):
        at = pl.ds(pl.multiple_of(g * 128, 128), 128)
        frm = pl.ds(g, 128, stride=8)
        ro_ref[at, :] = S[frm, :].T
        mo_ref[at, :] = C[frm, :].T
        return c
    lax.fori_loop(0, 8, leave, 0)

def physics(radius, floor_radius, mult, counts, cell_temp, cell_vapor):
    f32 = jnp.float32
    return pl.pallas_call(
        physics_kernel,
        out_shape=(jax.ShapeDtypeStruct((1024, 128), f32), jax.ShapeDtypeStruct((1024, 128), f32), jax.ShapeDtypeStruct((2, 8, 128), f32)),
        in_specs=[pl.BlockSpec(memory_space=pltpu.VMEM)] * 6,
        out_specs=[pl.BlockSpec(memory_space=pltpu.VMEM)] * 3,
        scratch_shapes=[pltpu.VMEM((1024, 128), f32)] * 5 + [pltpu.VMEM((N_CE * 8, 128), f32)],
        compiler_params=pltpu.CompilerParams(vmem_limit_bytes=40 * 2**20),
        cost_estimate=pl.CostEstimate(flops=30_000_000, bytes_accessed=3_000_000, transcendentals=1_000_000),
        name="physics",
    )(radius, floor_radius, mult, counts, cell_temp, cell_vapor)


def tendency(padded, along_x, along_y, along_z):
    middle_y = padded[:, :, 1:-1]
    flux_x = along_x * (0.5 * (middle_y[:, :-1] + middle_y[:, 1:]))
    middle_x = padded[:, 1:-1]
    flux_y = along_y * (0.5 * (middle_x[:, :, :-1] + middle_x[:, :, 1:]))
    core = padded[:, 1:-1, 1:-1]
    flux_z = along_z * (0.5 * (core[..., :-1] + core[..., 1:]))
    edge = jnp.zeros(core.shape[:-1] + (1,), core.dtype)
    flux_z = jnp.concatenate([edge, flux_z, edge], axis=-1)
    return (
        -(flux_x[:, 1:] - flux_x[:, :-1])
        - (flux_y[:, :, 1:] - flux_y[:, :, :-1])
        - (flux_z[..., 1:] - flux_z[..., :-1])
    )


def selector(index, count):
    return (jnp.arange(count, dtype=jnp.int32)[:, None] == index[None, :]).astype(jnp.float32)


def select_rows(matrix, value):
    flat = value.reshape((value.shape[0], -1))
    picked = jnp.dot(
        matrix, flat, precision=lax.Precision.HIGHEST, preferred_element_type=jnp.float32
    )
    return picked.reshape((matrix.shape[0],) + value.shape[1:])


def select_back(matrix, value):
    picked = lax.dot_general(
        matrix,
        value,
        (((0,), (0,)), ((), ())),
        precision=lax.Precision.HIGHEST,
        preferred_element_type=jnp.float32,
    )
    return picked


def single(value, cap):
    lead = (lax.axis_size("gx"), lax.axis_size("gy"), cap)
    moved = exchange_both(
        value.reshape(lead + value.shape[1:]), ("gx", "gy"), ("gx", "gy"), (0, 1), (0, 1)
    )
    return moved.reshape(value.shape)


def compact(taken):
    position = jnp.cumsum(taken.astype(jnp.int32)) - 1
    target = jnp.where(taken, position, BLK_DEV)
    return selector(target, BLK_DEV)


def advance(state):
    padded = with_halo(state, (("gx", 1), ("gy", 2)), 1)
    return padded


def body(
    tprime,
    vapor,
    wind_u,
    wind_v,
    wind_w,
    radius,
    min_radius,
    multiplicity,
    drop_counts,
    cell_index,
    move_list,
):
    devices = lax.axis_size("gx") * lax.axis_size("gy")
    home = radius.shape[0]
    drops = radius.shape[1]
    cap = (home + devices - 1) // devices
    slots = devices * cap
    columns = tprime.shape[0] * tprime.shape[1]
    levels = tprime.shape[2]
    live = move_list >= 0
    target = jnp.where(live, move_list, slots)
    placing = selector(target, slots)
    column_pick = selector(cell_index // levels, columns).T
    level_pick = selector(cell_index % levels, levels).T
    fields = jnp.concatenate(
        [tprime.reshape(columns, levels), vapor.reshape(columns, levels)], axis=1
    )
    at_column = select_rows(column_pick, fields)
    cell_temp = jnp.sum(at_column[:, :levels] * level_pick, axis=1)
    cell_vapor = jnp.sum(at_column[:, levels:] * level_pick, axis=1)
    square = (8, home // 8)
    radius_new, mult_new, heat = physics(
        radius,
        min_radius,
        multiplicity,
        drop_counts.reshape(square),
        cell_temp.reshape(square),
        cell_vapor.reshape(square),
    )
    bulk = single(select_rows(placing, jnp.concatenate([radius_new, mult_new], axis=1)), cap)
    gather_rows = compact(bulk[:, drops] > 0.0)
    picked = select_rows(gather_rows, bulk)
    radius_out = picked[:, :drops]
    multiplicity_out = picked[:, drops:]
    heat_t = heat[0].reshape(home)
    heat_v = heat[1].reshape(home)
    weighted = jnp.concatenate([level_pick * heat_t[:, None], level_pick * heat_v[:, None]], axis=1)
    added = select_back(column_pick, weighted)
    heated_t = (fields[:, :levels] + added[:, :levels]).reshape(tprime.shape)
    heated_v = (fields[:, levels:] + added[:, levels:]).reshape(vapor.shape)
    winds = with_halo(jnp.stack([wind_u, wind_v]), (("gx", 1), ("gy", 2)), 1)
    along_x = 0.5 * (winds[0, :-1, 1:-1] + winds[0, 1:, 1:-1])
    along_y = 0.5 * (winds[1, 1:-1, :-1] + winds[1, 1:-1, 1:])
    along_z = 0.5 * (wind_w[..., :-1] + wind_w[..., 1:])
    start = jnp.stack([heated_t, heated_v])
    section = start
    for weight in (1.0 / 3.0, 0.5, 1.0):
        section = start + advect_step * weight * tendency(
            advance(section), along_x, along_y, along_z
        )
    return (section[0], section[1], radius_out, multiplicity_out)


def solution(mesh):
    placed = (
        P("gx", "gy", None),
        P("gx", "gy", None),
        P("gx", "gy", None),
        P("gx", "gy", None),
        P("gx", "gy", None),
        P(("gx", "gy"), None),
        P(("gx", "gy"), None),
        P(("gx", "gy"), None),
        P(("gx", "gy")),
        P(("gx", "gy")),
        P(("gx", "gy")),
    )
    return jax.shard_map(
        body,
        mesh=mesh,
        in_specs=placed,
        out_specs=(
            P("gx", "gy", None),
            P("gx", "gy", None),
            P(("gx", "gy"), None),
            P(("gx", "gy"), None),
        ),
        check_vma=False,
    )
```

```python
import functools

import jax
import jax.numpy as jnp
from jax import lax
from jax.experimental import pallas as pl
from jax.experimental.pallas import tpu as pltpu
from jax.sharding import PartitionSpec as P

MESH = pl.DeviceIdType.MESH
f32 = jnp.float32
SUBSTEPS = 6
WX, WY = 66, 48

clausius = 0.07
growth = 200.0 / 3.0
solute = 0.05
condense = 5e-07
latent = 10.0
collect = 1e-07
time_step = 2.0
advect_step = 0.6


def batcher(n):
    out = []
    p = 1
    while p < n:
        k = p
        while k >= 1:
            for j in range(k % p, n - k, 2 * k):
                for i in range(min(k, n - j - k)):
                    if (i + j) // (2 * p) == (i + j + k) // (2 * p):
                        out.append((i + j, i + j + k))
            k //= 2
        p *= 2
    return out

NET16 = batcher(16)

def halves(top, n=16):
    out = []
    d = top
    while d >= 1:
        for i in range(n):
            if not i & d:
                out.append((i, i + d))
        d //= 2
    return out

def make_passes():
    passes = []
    up, down = list(range(16)), list(range(15, -1, -1))
    passes.append((4, [(lambda t: t * 32, up, up, NET16), (lambda t: t * 32, [16 + o for o in up], [16 + o for o in down], NET16)]))
    for level in (32, 64, 128):
        step = level // 16
        if level == 128:
            passes.append((step, [(lambda t: t, [step * o for o in up], [step * o for o in up], halves(8))]))
        else:
            per = step
            passes.append((128 // level, [(lambda t, b=b, level=level: t * level + b, [step * o for o in up], [step * o for o in up], halves(8)) for b in range(per)]))
        ces = halves(step // 2)
        if level == 128:
            passes.append((8, [(lambda t: t * 16, up, up, ces)]))
        else:
            sets = []
            for s in range(2 * level // 16):
                loads = [16 * s + o for o in up]
                stores = loads if s * 16 < level else [level + 2 * level - 1 - o for o in loads]
                sets.append((lambda t, level=level: t * 2 * level, loads, stores, ces))
            passes.append((128 // (2 * level), sets))
    return passes

PASSES = make_passes()
N_CE = sum(trips * sum(len(s[3]) for s in sets) for trips, sets in PASSES)

def moves(sets):
    return any(set(s[1]) != set(s[2]) for s in sets)

def row(ref, d):
    if isinstance(d, int):
        return ref.at[pl.ds(d * 8, 8), :]
    return ref.at[pl.ds(pl.multiple_of(d * 8, 8), 8), :]

def loop(trips, body):
    if trips == 1:
        body(0)
    else:
        def step(t, c):
            body(t)
            return c
        lax.fori_loop(0, trips, step, 0)

def sort_blocks(keys, vals, marks):
    at = 0
    side = 0
    for trips, sets in PASSES:
        count = sum(len(s[3]) for s in sets)
        key, val = keys[side], vals[side]
        if moves(sets):
            side = 1 - side
        key_to, val_to = keys[side], vals[side]
        def body(t, sets=sets, at=at, count=count, key=key, val=val, key_to=key_to, val_to=val_to):
            m = at + t * count
            for base, loads, stores, ces in sets:
                b = base(t)
                ks = [row(key, b + o)[...] for o in loads]
                vs = [row(val, b + o)[...] for o in loads]
                for i, j in ces:
                    c = ks[i] > ks[j]
                    row(marks, m)[...] = jnp.where(c, 1.0, 0.0)
                    m = m + 1
                    ks[i], ks[j] = jnp.minimum(ks[i], ks[j]), jnp.maximum(ks[i], ks[j])
                    vs[i], vs[j] = jnp.where(c, vs[j], vs[i]), jnp.where(c, vs[i], vs[j])
                for o, k, v in zip(stores, ks, vs):
                    row(key_to, b + o)[...] = k
                    row(val_to, b + o)[...] = v
        loop(trips, body)
        at += trips * count

def unsort_blocks(firsts, seconds, marks):
    at = N_CE
    side = 0
    for trips, sets in reversed(PASSES):
        count = sum(len(s[3]) for s in sets)
        at -= trips * count
        xa, xb = firsts[side], seconds[side]
        if moves(sets):
            side = 1 - side
        xa_to, xb_to = firsts[side], seconds[side]
        def body(t, sets=sets, at=at, count=count, xa=xa, xb=xb, xa_to=xa_to, xb_to=xb_to):
            m = at + t * count
            for base, loads, stores, ces in sets:
                b = base(t)
                xs = [row(xa, b + o)[...] for o in stores]
                ys = [row(xb, b + o)[...] for o in stores]
                for q in reversed(range(len(ces))):
                    i, j = ces[q]
                    c = row(marks, m + q)[...] > 0.5
                    xs[i], xs[j] = jnp.where(c, xs[j], xs[i]), jnp.where(c, xs[i], xs[j])
                    ys[i], ys[j] = jnp.where(c, ys[j], ys[i]), jnp.where(c, ys[i], ys[j])
                m = m + len(ces)
                for o, x, y in zip(loads, xs, ys):
                    row(xa_to, b + o)[...] = x
                    row(xb_to, b + o)[...] = y
        loop(trips, body)

def physics_kernel(rad_ref, flo_ref, mul_ref, cnt_ref, ct_ref, cv_ref, move_ref, send_ref, heat_ref, R, S, C, F, M, marks, X):
    def enter(g, c):
        at = pl.ds(pl.multiple_of(g * 128, 128), 128)
        to = pl.ds(g, 128, stride=8)
        R[to, :] = rad_ref[at, :].T
        F[to, :] = flo_ref[at, :].T
        M[to, :] = mul_ref[at, :].T
        return c
    lax.fori_loop(0, 8, enter, 0)
    counts = cnt_ref[...]
    zero = jnp.zeros((8, 128), jnp.float32)
    U = 8

    def init(t, w):
        for u in range(U):
            d = t * U + u
            r = row(R, d)[...]
            f = row(F, d)[...]
            m = jnp.where(counts > d, row(M, d)[...], 0.0)
            r2 = r * r
            f2 = f * f
            row(M, d)[...] = m
            row(R, d)[...] = r2
            row(S, d)[...] = lax.rsqrt(r2)
            row(F, d)[...] = f2
            row(C, d)[...] = (growth * solute) * f2 * f
            w = w + m * (r2 * r)
        return w
    weight = lax.fori_loop(0, 128 // U, init, zero)
    temp = ct_ref[...]
    wet = cv_ref[...]
    for _ in range(SUBSTEPS):
        sat = growth * ((1.0 + wet) * jnp.exp(-clausius * temp) - 1.0)
        def sub(t, w):
            for u in range(U):
                d = t * U + u
                r2 = row(R, d)[...]
                rs = row(S, d)[...]
                g = jnp.maximum(r2 + (sat + row(C, d)[...] * (rs * rs * rs)), row(F, d)[...])
                ns = lax.rsqrt(g)
                row(R, d)[...] = g
                row(S, d)[...] = ns
                w = w + row(M, d)[...] * (g * (g * ns))
            return w
        after = lax.fori_loop(0, 128 // U, sub, zero)
        condensed = after - weight
        weight = after
        wet = wet - condense * condensed
        temp = temp + latent * condense * condensed
    heat_ref[0:8, :] = temp - ct_ref[...]
    heat_ref[8:16, :] = wet - cv_ref[...]

    def radii(t, c):
        for u in range(U):
            d = t * U + u
            row(R, d)[...] = row(R, d)[...] * row(S, d)[...]
        return c
    lax.fori_loop(0, 128 // U, radii, 0)
    sort_blocks((R, S), (M, C), marks)

    def both(t, carry):
        a0, a1, a3, a4, b0, b1, b3, b4 = carry
        for u in range(U):
            d = t * U + u
            r = row(R, d)[...]
            m = row(M, d)[...]
            r2 = r * r
            r3 = r2 * r
            r4 = r2 * r2
            gain = r4 * a0 + 2.0 * (r3 * a1 - r * a3) - a4
            w = m * r3
            a0 = a0 + w
            a1 = a1 + w * r
            a3 = a3 + w * r3
            a4 = a4 + w * r4
            grown = r3 + (time_step * collect) * gain
            row(S, d)[...] = jnp.where(m > 0.0, jnp.exp(jnp.log(grown) * (1.0 / 3.0)), 0.0)
            d = 127 - d
            r = row(R, d)[...]
            m = row(M, d)[...]
            r2 = r * r
            r3 = r2 * r
            r4 = r2 * r2
            loss = b4 + 2.0 * (r * b3 - r3 * b1) - r4 * b0
            b0 = b0 + m
            b1 = b1 + m * r
            b3 = b3 + m * r3
            b4 = b4 + m * r4
            row(C, d)[...] = m * jnp.exp((-time_step * collect) * loss)
        return a0, a1, a3, a4, b0, b1, b3, b4
    lax.fori_loop(0, 128 // U, both, (zero,) * 8)
    unsort_blocks((S, R), (C, F), marks)

    def leave(g, c):
        at = pl.ds(pl.multiple_of(g * 128, 128), 128)
        frm = pl.ds(g, 128, stride=8)
        for q, ref in enumerate((S, C)):
            for k, part in enumerate(split3(ref[frm, :].T)):
                X[at, k * 256 + q * 128:k * 256 + q * 128 + 128] = part
        return c
    lax.fori_loop(0, 8, leave, 0)
    moves_to = move_ref[...]

    def place(n, c):
        at = pl.multiple_of(n * 128, 128)
        ids = lax.broadcasted_iota(jnp.int32, (128, 1024), 0) + at
        hot = jnp.where(ids == moves_to, 1.0, 0.0).astype(jnp.bfloat16)
        d = jnp.dot(hot, X[...], preferred_element_type=f32)
        send_ref[pl.ds(at, 128), :] = d[:, 0:256] + (d[:, 256:512] + d[:, 512:768])
        return c
    lax.fori_loop(0, 8, place, 0)


def physics(radius, floor_radius, mult, counts, cell_temp, cell_vapor, move_list):
    return pl.pallas_call(
        physics_kernel,
        out_shape=(jax.ShapeDtypeStruct((1024, 256), f32), jax.ShapeDtypeStruct((16, 128), f32)),
        in_specs=[pl.BlockSpec(memory_space=pltpu.VMEM)] * 7,
        out_specs=[pl.BlockSpec(memory_space=pltpu.VMEM)] * 2,
        scratch_shapes=[pltpu.VMEM((1024, 128), f32)] * 5 + [pltpu.VMEM((N_CE * 8, 128), f32), pltpu.VMEM((1024, 768), jnp.bfloat16)],
        compiler_params=pltpu.CompilerParams(vmem_limit_bytes=40 * 2**20),
        cost_estimate=pl.CostEstimate(flops=1_700_000_000, bytes_accessed=3_000_000, transcendentals=1_000_000),
        name="physics",
    )(radius, floor_radius, mult, counts, cell_temp, cell_vapor, move_list)


def mod(a, n):
    return lax.rem(a + n, n)


def split2(x):
    hi = x.astype(jnp.bfloat16)
    lo = (x - hi.astype(f32)).astype(jnp.bfloat16)
    return hi, lo


def comm_kernel(nx, ny, send_ref, t_ref, v_ref, u_ref, vv_ref, w_ref, cell_ref, zed_ref, heat_ref,
                to_ref, vo_ref, recv_ref,
                E, AX, AL, AH, AZ, UE, VE, yout, yin, vout, vin, W,
                a2a_send, a2a_recv, xs, xr, ys, yr, ws, wr):
    ix, iy = lax.axis_index("gx"), lax.axis_index("gy")
    me = ix * ny + iy
    count = nx * ny
    right, left = (mod(ix + 1, nx), iy), (mod(ix - 1, nx), iy)
    upper, lower = (ix, mod(iy + 1, ny)), (ix, mod(iy - 1, ny))

    barrier = pltpu.get_barrier_semaphore()

    def greet(i, c):
        p = mod(me + i, count)
        pl.semaphore_signal(barrier, inc=1, device_id=(p // ny, lax.rem(p, ny)), device_id_type=MESH)
        return c
    lax.fori_loop(1, count, greet, 0)

    vout[0] = vv_ref[pl.ds(31, 64, stride=32), :]
    vout[1] = vv_ref[pl.ds(0, 64, stride=32), :]
    pl.semaphore_wait(barrier, count - 1)

    def remote(src, dst, s, r, to):
        return pltpu.make_async_remote_copy(src_ref=src, dst_ref=dst, send_sem=s, recv_sem=r, device_id=to, device_id_type=MESH)

    winds = [
        remote(u_ref.at[pl.ds(63 * 32, 32), :], UE.at[0], ws.at[0], wr.at[0], right),
        remote(u_ref.at[pl.ds(0, 32), :], UE.at[1], ws.at[1], wr.at[1], left),
        remote(vout.at[0], vin.at[0], ws.at[2], wr.at[2], upper),
        remote(vout.at[1], vin.at[1], ws.at[3], wr.at[3], lower),
    ]
    for c in winds:
        c.start()

    def chunk(i):
        p = mod(me + i, count)
        return remote(
            send_ref.at[pl.ds(pl.multiple_of(p * 8, 8), 8), :],
            recv_ref.at[pl.ds(pl.multiple_of(me * 8, 8), 8), :],
            a2a_send, a2a_recv, (p // ny, lax.rem(p, ny)))

    def send_some(lo, hi):
        def body(i, c):
            chunk(i).start()
            return c
        lax.fori_loop(lo, hi, body, 0)

    send_some(1, count // 3)
    mine = pl.ds(pl.multiple_of(me * 8, 8), 8)
    recv_ref[mine, :] = send_ref[mine, :]

    zed = lax.rem(zed_ref[...], 128).astype(f32).T.astype(jnp.int32)
    heat = heat_ref[...].T
    lanes = lax.broadcasted_iota(jnp.int32, (128, 128), 1)
    for g in range(8):
        level = lanes == zed[:, g:g + 1]
        at = pl.ds(g * 128, 128)
        for q in range(2):
            h = jnp.where(level, heat[:, q * 8 + g:q * 8 + g + 1], 0.0)
            hi, lo = split2(h)
            W[at, q * 128:q * 128 + 128] = hi
            W[at, 256 + q * 128:256 + q * 128 + 128] = lo
    cells = lax.shift_right_logical(cell_ref[...], 7)

    def scatter(k, c):
        at = pl.multiple_of(k * 128, 128)
        ids = lax.broadcasted_iota(jnp.int32, (128, 1024), 0) + at
        hot = jnp.where(ids == cells, 1.0, 0.0).astype(jnp.bfloat16)
        d = jnp.dot(hot, W[...], preferred_element_type=f32)
        for q, ref in ((0, t_ref), (1, v_ref)):
            add = d[:, q * 128:q * 128 + 128] + d[:, 256 + q * 128:256 + q * 128 + 128]
            new = ref[pl.ds(at, 128), :] + add
            for j in range(4):
                E[q, pl.ds(pl.multiple_of((k * 4 + j + 1) * WY + 8, 8), 32), :] = new[j * 32:j * 32 + 32]
        return c
    lax.fori_loop(0, 16, scatter, 0)

    def plane(x):
        return x * WY + 8

    def exchange(s):
        moves = []
        for q in range(2):
            e = E.at[2 * s + q]
            moves.append(remote(e.at[pl.ds(plane(64), 32), :], e.at[pl.ds(plane(0), 32), :], xs.at[4 * s + 2 * q], xr.at[4 * s + 2 * q], right))
            moves.append(remote(e.at[pl.ds(plane(1), 32), :], e.at[pl.ds(plane(65), 32), :], xs.at[4 * s + 2 * q + 1], xr.at[4 * s + 2 * q + 1], left))
            yout[2 * s, pl.ds(64 * q, 64), :] = E[2 * s + q, pl.ds(plane(1) + 31, 64, stride=WY), :]
            yout[2 * s + 1, pl.ds(64 * q, 64), :] = E[2 * s + q, pl.ds(plane(1), 64, stride=WY), :]
        moves.append(remote(yout.at[2 * s], yin.at[2 * s], ys.at[2 * s], yr.at[2 * s], upper))
        moves.append(remote(yout.at[2 * s + 1], yin.at[2 * s + 1], ys.at[2 * s + 1], yr.at[2 * s + 1], lower))
        for c in moves:
            c.start()
        return moves

    def arrive(s, moves):
        for c in moves:
            c.wait_recv()
        for q in range(2):
            E[2 * s + q, pl.ds(plane(1) - 1, 64, stride=WY), :] = yin[2 * s, pl.ds(64 * q, 64), :]
            E[2 * s + q, pl.ds(plane(1) + 32, 64, stride=WY), :] = yin[2 * s + 1, pl.ds(64 * q, 64), :]

    moves = exchange(0)
    send_some(count // 3, 2 * count // 3)
    for c in winds:
        c.wait_recv()

    AX[pl.ds(0, 32), :] = 0.25 * (UE[0] + u_ref[pl.ds(0, 32), :])
    AX[pl.ds(64 * 32, 32), :] = 0.25 * (u_ref[pl.ds(63 * 32, 32), :] + UE[1])
    VE[pl.ds(7, 64, stride=WY), :] = vin[0]
    VE[pl.ds(40, 64, stride=WY), :] = vin[1]
    last = lax.broadcasted_iota(jnp.int32, (32, 128), 1) == 127

    def enter(x, c):
        at = pl.ds(pl.multiple_of(x * 32, 32), 32)
        VE[pl.ds(pl.multiple_of(x * WY + 8, 8), 32), :] = vv_ref[at, :]
        return c
    lax.fori_loop(0, 64, enter, 0)

    def faces(x, c):
        at = pl.ds(pl.multiple_of(x * 32, 32), 32)
        here = vv_ref[at, :]
        AL[at, :] = 0.25 * (here + VE[pl.ds(x * WY + 7, 32), :])
        AH[at, :] = 0.25 * (here + VE[pl.ds(x * WY + 9, 32), :])
        w = w_ref[at, :]
        AZ[at, :] = jnp.where(last, 0.0, 0.25 * (w + pltpu.roll(w, 127, 1)))
        return c
    lax.fori_loop(0, 64, faces, 0)

    def face_x(x, c):
        AX[pl.ds(pl.multiple_of(x * 32, 32), 32), :] = 0.25 * (u_ref[pl.ds(pl.multiple_of(x * 32 - 32, 32), 32), :] + u_ref[pl.ds(pl.multiple_of(x * 32, 32), 32), :])
        return c
    lax.fori_loop(1, 64, face_x, 0)

    for s, weight in enumerate((advect_step / 3.0, advect_step / 2.0, advect_step)):
        arrive(s, moves)
        for q in range(2):
            src = E.at[2 * s + q]
            start = E.at[q]
            def step(x, carry, q=q, src=src, start=start, s=s, weight=weight):
                f, low = carry
                at = pl.ds(pl.multiple_of(x * 32, 32), 32)
                p = pl.multiple_of((x + 1) * WY + 8, 8)
                after = src[pl.ds(pl.multiple_of(p + WY, 8), 32), :]
                high = AX[pl.ds(pl.multiple_of(x * 32 + 32, 32), 32), :] * (f + after)
                fy = AH[at, :] * (f + src[pl.ds(p + 1, 32), :]) - AL[at, :] * (src[pl.ds(p - 1, 32), :] + f)
                fz = AZ[at, :] * (f + pltpu.roll(f, 127, 1))
                out = start[pl.ds(p, 32), :] - weight * ((high - low) + fy + (fz - pltpu.roll(fz, 1, 1)))
                if s < 2:
                    E[2 * s + 2 + q, pl.ds(p, 32), :] = out
                else:
                    (to_ref, vo_ref)[q][at, :] = out
                return after, high
            f0 = src[pl.ds(plane(1), 32), :]
            lax.fori_loop(0, 64, step, (f0, AX[pl.ds(0, 32), :] * (src[pl.ds(plane(0), 32), :] + f0)))
        for c in moves:
            c.wait_send()
        if s < 2:
            moves = exchange(s + 1)
        if s == 0:
            send_some(2 * count // 3, count)
    for c in winds:
        c.wait_send()
    whole = remote(recv_ref.at[pl.ds(8, 8 * (count - 1)), :], recv_ref.at[pl.ds(8, 8 * (count - 1)), :], a2a_send, a2a_recv, right)
    whole.wait_send()
    whole.wait_recv()


def comm(mesh_shape, send, t, v, u, vv, w, cells, zed, heat):
    nx, ny = mesh_shape
    VM = pl.BlockSpec(memory_space=pltpu.VMEM)
    bf16 = jnp.bfloat16
    DMA = pltpu.SemaphoreType.DMA
    return pl.pallas_call(
        functools.partial(comm_kernel, nx, ny),
        out_shape=(jax.ShapeDtypeStruct((2048, 128), f32), jax.ShapeDtypeStruct((2048, 128), f32), jax.ShapeDtypeStruct((1024, 256), f32)),
        in_specs=[VM] * 9,
        out_specs=[VM] * 3,
        scratch_shapes=[
            pltpu.VMEM((6, WX * WY, 128), f32),
            pltpu.VMEM((65 * 32, 128), f32), pltpu.VMEM((2048, 128), f32), pltpu.VMEM((2048, 128), f32), pltpu.VMEM((2048, 128), f32),
            pltpu.VMEM((2, 32, 128), f32), pltpu.VMEM((64 * WY, 128), f32),
            pltpu.VMEM((6, 128, 128), f32), pltpu.VMEM((6, 128, 128), f32),
            pltpu.VMEM((2, 64, 128), f32), pltpu.VMEM((2, 64, 128), f32),
            pltpu.VMEM((1024, 512), bf16),
            DMA, DMA, DMA((12,)), DMA((12,)), DMA((6,)), DMA((6,)), DMA((4,)), DMA((4,)),
        ],
        compiler_params=pltpu.CompilerParams(vmem_limit_bytes=56 * 2**20, collective_id=0, has_side_effects=True),
        cost_estimate=pl.CostEstimate(flops=3_000_000_000, bytes_accessed=8_000_000, transcendentals=0),
        name="exchange",
    )(send, t, v, u, vv, w, cells, zed, heat)


def triangle(n):
    return lax.broadcasted_iota(jnp.int32, (n, n), 0) < lax.broadcasted_iota(jnp.int32, (n, n), 1)


def split3(x):
    hi = x.astype(jnp.bfloat16)
    rest = x - hi.astype(f32)
    mid = rest.astype(jnp.bfloat16)
    return hi, mid, (rest - mid.astype(f32)).astype(jnp.bfloat16)


def compact_kernel(recv_ref, ro_ref, mo_ref, X):
    rows = []
    for g in range(8):
        rows.append(recv_ref[pl.ds(g * 128, 128), 128:256].T[0:1])
    first = jnp.concatenate(rows, axis=0)
    taken = jnp.where(first > 0.0, 1.0, 0.0)
    within = jnp.dot(taken.astype(jnp.bfloat16), jnp.where(triangle(128), 1.0, 0.0).astype(jnp.bfloat16), preferred_element_type=f32)
    total = jnp.sum(taken, axis=1, keepdims=True)
    pos = []
    before = jnp.zeros((1, 1), f32)
    for g in range(8):
        pos.append(jnp.where(first[g:g + 1] > 0.0, within[g:g + 1] + before, -1.0))
        before = before + total[g:g + 1]
    pos = jnp.concatenate(pos, axis=1).astype(jnp.int32)
    for g in range(8):
        at = pl.ds(g * 128, 128)
        for k, part in enumerate(split3(recv_ref[at, :])):
            X[at, k * 256:k * 256 + 256] = part
    for n in range(4):
        ids = lax.broadcasted_iota(jnp.int32, (128, 1024), 0) + n * 128
        hot = jnp.where(ids == pos, 1.0, 0.0).astype(jnp.bfloat16)
        d = jnp.dot(hot, X[...], preferred_element_type=f32)
        d = d[:, 0:256] + (d[:, 256:512] + d[:, 512:768])
        ro_ref[pl.ds(n * 128, 128), :] = d[:, 0:128]
        mo_ref[pl.ds(n * 128, 128), :] = d[:, 128:256]


def compacted(recv):
    VM = pl.BlockSpec(memory_space=pltpu.VMEM)
    return pl.pallas_call(
        compact_kernel,
        out_shape=(jax.ShapeDtypeStruct((512, 128), f32), jax.ShapeDtypeStruct((512, 128), f32)),
        in_specs=[VM], out_specs=[VM, VM],
        scratch_shapes=[pltpu.VMEM((1024, 768), jnp.bfloat16)],
        compiler_params=pltpu.CompilerParams(vmem_limit_bytes=16 * 2**20),
        cost_estimate=pl.CostEstimate(flops=800_000_000, bytes_accessed=2_000_000, transcendentals=0),
        name="compact",
    )(recv)


def selector(index, count):
    return (jnp.arange(count, dtype=jnp.int32)[:, None] == index[None, :]).astype(jnp.float32)


def select_rows(matrix, value):
    flat = value.reshape((value.shape[0], -1))
    picked = jnp.dot(
        matrix, flat, precision=lax.Precision.HIGHEST, preferred_element_type=jnp.float32
    )
    return picked.reshape((matrix.shape[0],) + value.shape[1:])


def body(
    shape,
    tprime,
    vapor,
    wind_u,
    wind_v,
    wind_w,
    radius,
    min_radius,
    multiplicity,
    drop_counts,
    cell_index,
    move_list,
):
    home = radius.shape[0]
    columns = tprime.shape[0] * tprime.shape[1]
    levels = tprime.shape[2]
    flat = [a.reshape(columns, levels) for a in (tprime, vapor, wind_u, wind_v, wind_w)]
    column_pick = selector(cell_index // levels, columns).T
    level_pick = selector(cell_index % levels, levels).T
    at_column = select_rows(column_pick, jnp.concatenate(flat[:2], axis=1))
    cell_temp = jnp.sum(at_column[:, :levels] * level_pick, axis=1)
    cell_vapor = jnp.sum(at_column[:, levels:] * level_pick, axis=1)
    square = (8, home // 8)
    send, heat = physics(
        radius,
        min_radius,
        multiplicity,
        drop_counts.reshape(square),
        cell_temp.reshape(square),
        cell_vapor.reshape(square),
        move_list.reshape(1, home),
    )
    temperature, humidity, recv = comm(
        shape, send, *flat, cell_index.reshape(1, home), cell_index.reshape(square), heat
    )
    radius_out, multiplicity_out = compacted(recv)
    return (
        temperature.reshape(tprime.shape),
        humidity.reshape(vapor.shape),
        radius_out,
        multiplicity_out,
    )


def solution(mesh):
    placed = (
        P("gx", "gy", None),
        P("gx", "gy", None),
        P("gx", "gy", None),
        P("gx", "gy", None),
        P("gx", "gy", None),
        P(("gx", "gy"), None),
        P(("gx", "gy"), None),
        P(("gx", "gy"), None),
        P(("gx", "gy")),
        P(("gx", "gy")),
        P(("gx", "gy")),
    )
    return jax.shard_map(
        functools.partial(body, (mesh.shape["gx"], mesh.shape["gy"])),
        mesh=mesh,
        in_specs=placed,
        out_specs=(
            P("gx", "gy", None),
            P("gx", "gy", None),
            P(("gx", "gy"), None),
            P(("gx", "gy"), None),
        ),
        check_vma=False,
    )
```

```python
import functools

import jax
import jax.numpy as jnp
from jax import lax
from jax.experimental import pallas as pl
from jax.experimental.pallas import tpu as pltpu
from jax.sharding import PartitionSpec as P

MESH = pl.DeviceIdType.MESH
f32 = jnp.float32
SUBSTEPS = 6
WX, WY = 66, 48
UNROLL = 8

clausius = 0.07
growth = 200.0 / 3.0
solute = 0.05
condense = 5e-07
latent = 10.0
collect = 1e-07
time_step = 2.0
advect_step = 0.6


def batcher(n):
    out = []
    p = 1
    while p < n:
        k = p
        while k >= 1:
            for j in range(k % p, n - k, 2 * k):
                for i in range(min(k, n - j - k)):
                    if (i + j) // (2 * p) == (i + j + k) // (2 * p):
                        out.append((i + j, i + j + k))
            k //= 2
        p *= 2
    return out

NET16 = batcher(16)

def halves(top, n=16):
    out = []
    d = top
    while d >= 1:
        for i in range(n):
            if not i & d:
                out.append((i, i + d))
        d //= 2
    return out

def make_passes():
    passes = []
    up, down = list(range(16)), list(range(15, -1, -1))
    passes.append((4, [(lambda t: t * 32, up, up, NET16), (lambda t: t * 32, [16 + o for o in up], [16 + o for o in down], NET16)]))
    for level in (32, 64, 128):
        step = level // 16
        if level == 128:
            passes.append((step, [(lambda t: t, [step * o for o in up], [step * o for o in up], halves(8))]))
        else:
            per = step
            passes.append((128 // level, [(lambda t, b=b, level=level: t * level + b, [step * o for o in up], [step * o for o in up], halves(8)) for b in range(per)]))
        ces = halves(step // 2)
        if level == 128:
            passes.append((8, [(lambda t: t * 16, up, up, ces)]))
        else:
            sets = []
            for s in range(2 * level // 16):
                loads = [16 * s + o for o in up]
                stores = loads if s * 16 < level else [level + 2 * level - 1 - o for o in loads]
                sets.append((lambda t, level=level: t * 2 * level, loads, stores, ces))
            passes.append((128 // (2 * level), sets))
    return passes

PASSES = make_passes()
N_CE = sum(trips * sum(len(s[3]) for s in sets) for trips, sets in PASSES)

def moves(sets):
    return any(set(s[1]) != set(s[2]) for s in sets)

def row(ref, d):
    if isinstance(d, int):
        return ref.at[pl.ds(d * 8, 8), :]
    return ref.at[pl.ds(pl.multiple_of(d * 8, 8), 8), :]

def loop(trips, body):
    if trips == 1:
        body(0)
    else:
        def step(t, c):
            body(t)
            return c
        lax.fori_loop(0, trips, step, 0)

def sort_blocks(keys, vals, marks):
    at = 0
    side = 0
    for trips, sets in PASSES:
        count = sum(len(s[3]) for s in sets)
        key, val = keys[side], vals[side]
        if moves(sets):
            side = 1 - side
        key_to, val_to = keys[side], vals[side]
        def body(t, sets=sets, at=at, count=count, key=key, val=val, key_to=key_to, val_to=val_to):
            m = at + t * count
            for base, loads, stores, ces in sets:
                b = base(t)
                ks = [row(key, b + o)[...] for o in loads]
                vs = [row(val, b + o)[...] for o in loads]
                for i, j in ces:
                    c = ks[i] > ks[j]
                    row(marks, m)[...] = jnp.where(c, 1.0, 0.0)
                    m = m + 1
                    ks[i], ks[j] = jnp.minimum(ks[i], ks[j]), jnp.maximum(ks[i], ks[j])
                    vs[i], vs[j] = jnp.where(c, vs[j], vs[i]), jnp.where(c, vs[i], vs[j])
                for o, k, v in zip(stores, ks, vs):
                    row(key_to, b + o)[...] = k
                    row(val_to, b + o)[...] = v
        loop(trips, body)
        at += trips * count

def unsort_blocks(firsts, seconds, marks):
    at = N_CE
    side = 0
    for trips, sets in reversed(PASSES):
        count = sum(len(s[3]) for s in sets)
        at -= trips * count
        xa, xb = firsts[side], seconds[side]
        if moves(sets):
            side = 1 - side
        xa_to, xb_to = firsts[side], seconds[side]
        def body(t, sets=sets, at=at, count=count, xa=xa, xb=xb, xa_to=xa_to, xb_to=xb_to):
            m = at + t * count
            for base, loads, stores, ces in sets:
                b = base(t)
                xs = [row(xa, b + o)[...] for o in stores]
                ys = [row(xb, b + o)[...] for o in stores]
                for q in reversed(range(len(ces))):
                    i, j = ces[q]
                    c = row(marks, m + q)[...] > 0.5
                    xs[i], xs[j] = jnp.where(c, xs[j], xs[i]), jnp.where(c, xs[i], xs[j])
                    ys[i], ys[j] = jnp.where(c, ys[j], ys[i]), jnp.where(c, ys[i], ys[j])
                m = m + len(ces)
                for o, x, y in zip(loads, xs, ys):
                    row(xa_to, b + o)[...] = x
                    row(xb_to, b + o)[...] = y
        loop(trips, body)

def gather_cells(index, t_ref, v_ref, cell_ref, ct, cv, T, V):
    def rows(k, c):
        for j in range(16):
            b = k * 16 + j
            at = lax.shift_right_logical(index[b], 7)
            T[pl.ds(b, 1), :] = t_ref[pl.ds(at, 1), :]
            V[pl.ds(b, 1), :] = v_ref[pl.ds(at, 1), :]
        return c
    lax.fori_loop(0, 64, rows, 0)
    level = lax.rem(cell_ref[...], 128)
    depth = lax.broadcasted_iota(jnp.int32, (128, 128), 0)
    for g in range(8):
        here = depth == level[g:g + 1]
        for staged, cell in ((T, ct), (V, cv)):
            picked = jnp.where(here, staged[pl.ds(g * 128, 128), :].T, 0.0)
            cell[pl.ds(g, 1), :] = jnp.sum(picked, axis=0, keepdims=True)


def physics_kernel(index, t_ref, v_ref, rad_ref, flo_ref, mul_ref, cnt_ref, cell_ref, move_ref, send_ref, heat_ref, R, S, C, F, M, marks, X, ct_ref, cv_ref):
    gather_cells(index, t_ref, v_ref, cell_ref, ct_ref, cv_ref, S, C)

    def enter(g, c):
        at = pl.ds(pl.multiple_of(g * 128, 128), 128)
        to = pl.ds(g, 128, stride=8)
        R[to, :] = rad_ref[at, :].T
        F[to, :] = flo_ref[at, :].T
        M[to, :] = mul_ref[at, :].T
        return c
    lax.fori_loop(0, 8, enter, 0)
    counts = cnt_ref[...]
    zero = jnp.zeros((8, 128), jnp.float32)
    U = 8

    def init(t, w):
        for u in range(U):
            d = t * U + u
            r = row(R, d)[...]
            f = row(F, d)[...]
            m = jnp.where(counts > d, row(M, d)[...], 0.0)
            r2 = r * r
            f2 = f * f
            row(M, d)[...] = m
            row(R, d)[...] = r2
            row(S, d)[...] = lax.rsqrt(r2)
            row(F, d)[...] = f2
            row(C, d)[...] = (growth * solute) * f2 * f
            w = w + m * (r2 * r)
        return w
    weight = lax.fori_loop(0, 128 // U, init, zero)
    temp = ct_ref[...]
    wet = cv_ref[...]
    for _ in range(SUBSTEPS):
        sat = growth * ((1.0 + wet) * jnp.exp(-clausius * temp) - 1.0)
        def sub(t, w):
            for u in range(U):
                d = t * U + u
                r2 = row(R, d)[...]
                rs = row(S, d)[...]
                g = jnp.maximum(r2 + (sat + row(C, d)[...] * (rs * rs * rs)), row(F, d)[...])
                ns = lax.rsqrt(g)
                row(R, d)[...] = g
                row(S, d)[...] = ns
                w = w + row(M, d)[...] * (g * (g * ns))
            return w
        after = lax.fori_loop(0, 128 // U, sub, zero)
        condensed = after - weight
        weight = after
        wet = wet - condense * condensed
        temp = temp + latent * condense * condensed
    heat_ref[0:8, :] = temp - ct_ref[...]
    heat_ref[8:16, :] = wet - cv_ref[...]

    def radii(t, c):
        for u in range(U):
            d = t * U + u
            row(R, d)[...] = row(R, d)[...] * row(S, d)[...]
        return c
    lax.fori_loop(0, 128 // U, radii, 0)
    sort_blocks((R, S), (M, C), marks)

    def both(t, carry):
        a0, a1, a3, a4, b0, b1, b3, b4 = carry
        for u in range(U):
            d = t * U + u
            r = row(R, d)[...]
            m = row(M, d)[...]
            r2 = r * r
            r3 = r2 * r
            r4 = r2 * r2
            gain = r4 * a0 + 2.0 * (r3 * a1 - r * a3) - a4
            w = m * r3
            a0 = a0 + w
            a1 = a1 + w * r
            a3 = a3 + w * r3
            a4 = a4 + w * r4
            grown = r3 + (time_step * collect) * gain
            row(S, d)[...] = jnp.where(m > 0.0, jnp.exp(jnp.log(grown) * (1.0 / 3.0)), 0.0)
            d = 127 - d
            r = row(R, d)[...]
            m = row(M, d)[...]
            r2 = r * r
            r3 = r2 * r
            r4 = r2 * r2
            loss = b4 + 2.0 * (r * b3 - r3 * b1) - r4 * b0
            b0 = b0 + m
            b1 = b1 + m * r
            b3 = b3 + m * r3
            b4 = b4 + m * r4
            row(C, d)[...] = m * jnp.exp((-time_step * collect) * loss)
        return a0, a1, a3, a4, b0, b1, b3, b4
    lax.fori_loop(0, 128 // U, both, (zero,) * 8)
    unsort_blocks((S, R), (C, F), marks)

    def leave(g, c):
        at = pl.ds(pl.multiple_of(g * 128, 128), 128)
        frm = pl.ds(g, 128, stride=8)
        for q, ref in enumerate((S, C)):
            for k, part in enumerate(split3(ref[frm, :].T)):
                X[at, k * 256 + q * 128:k * 256 + q * 128 + 128] = part
        return c
    lax.fori_loop(0, 8, leave, 0)
    moves_to = move_ref[...]

    def place(n, c):
        at = pl.multiple_of(n * 128, 128)
        ids = lax.broadcasted_iota(jnp.int32, (128, 1024), 0) + at
        hot = jnp.where(ids == moves_to, 1.0, 0.0).astype(jnp.bfloat16)
        d = jnp.dot(hot, X[...], preferred_element_type=f32)
        send_ref[pl.ds(at, 128), :] = d[:, 0:256] + (d[:, 256:512] + d[:, 512:768])
        return c
    lax.fori_loop(0, 8, place, 0)


def physics(index, t, v, radius, floor_radius, mult, counts, cells, move_list):
    VM = pl.BlockSpec(memory_space=pltpu.VMEM)
    return pl.pallas_call(
        physics_kernel,
        out_shape=(jax.ShapeDtypeStruct((1024, 256), f32), jax.ShapeDtypeStruct((16, 128), f32)),
        in_specs=[pl.BlockSpec(memory_space=pltpu.SMEM)] + [VM] * 8,
        out_specs=[VM] * 2,
        scratch_shapes=[pltpu.VMEM((1024, 128), f32)] * 5 + [pltpu.VMEM((N_CE * 8, 128), f32), pltpu.VMEM((1024, 768), jnp.bfloat16), pltpu.VMEM((8, 128), f32), pltpu.VMEM((8, 128), f32)],
        compiler_params=pltpu.CompilerParams(vmem_limit_bytes=20 * 2**20),
        cost_estimate=pl.CostEstimate(flops=1_700_000_000, bytes_accessed=3_000_000, transcendentals=1_000_000),
        name="physics",
    )(index, t, v, radius, floor_radius, mult, counts, cells, move_list)


def mod(a, n):
    return lax.rem(a + n, n)


def split2(x):
    hi = x.astype(jnp.bfloat16)
    lo = (x - hi.astype(f32)).astype(jnp.bfloat16)
    return hi, lo


def comm_kernel(nx, ny, send_ref, t_ref, v_ref, u_ref, vv_ref, w_ref, cell_ref, zed_ref, heat_ref,
                to_ref, vo_ref, recv_ref,
                E, AX, AL, AH, AZ, AD, UE, VE, yout, yin, vout, vin, W,
                a2a_send, a2a_recv, xs, xr, ys, yr, ws, wr, rows):
    ix, iy = lax.axis_index("gx"), lax.axis_index("gy")
    me = ix * ny + iy
    count = nx * ny
    right, left = (mod(ix + 1, nx), iy), (mod(ix - 1, nx), iy)
    upper, lower = (ix, mod(iy + 1, ny)), (ix, mod(iy - 1, ny))

    barrier = pltpu.get_barrier_semaphore()

    for i in range(1, ny):
        pl.semaphore_signal(barrier, inc=1, device_id=(ix, mod(iy + i, ny)), device_id_type=MESH)
    for i in range(1, nx):
        pl.semaphore_signal(barrier, inc=1, device_id=(mod(ix + i, nx), iy), device_id_type=MESH)

    vout[0] = vv_ref[pl.ds(31, 64, stride=32), :]
    vout[1] = vv_ref[pl.ds(0, 64, stride=32), :]
    pl.semaphore_wait(barrier, nx + ny - 2)
    for i in range(1, ny):
        pl.semaphore_signal(rows, inc=1, device_id=(ix, mod(iy + i, ny)), device_id_type=MESH)

    def remote(src, dst, s, r, to):
        return pltpu.make_async_remote_copy(src_ref=src, dst_ref=dst, send_sem=s, recv_sem=r, device_id=to, device_id_type=MESH)

    winds = [
        remote(u_ref.at[pl.ds(63 * 32, 32), :], UE.at[0], ws.at[0], wr.at[0], right),
        remote(u_ref.at[pl.ds(0, 32), :], UE.at[1], ws.at[1], wr.at[1], left),
        remote(vout.at[0], vin.at[0], ws.at[2], wr.at[2], upper),
        remote(vout.at[1], vin.at[1], ws.at[3], wr.at[3], lower),
    ]
    for c in winds:
        c.start()

    def chunk(i):
        p = mod(me + i, count)
        return remote(
            send_ref.at[pl.ds(pl.multiple_of(p * 8, 8), 8), :],
            recv_ref.at[pl.ds(pl.multiple_of(me * 8, 8), 8), :],
            a2a_send, a2a_recv, (p // ny, lax.rem(p, ny)))

    def send_some(lo, hi):
        def body(i, c):
            chunk(i).start()
            return c
        lax.fori_loop(lo, hi, body, 0)

    pl.semaphore_wait(rows, ny - 1)
    send_some(1, count // 3)
    mine = pl.ds(pl.multiple_of(me * 8, 8), 8)
    recv_ref[mine, :] = send_ref[mine, :]

    zed = lax.rem(zed_ref[...], 128).astype(f32).T.astype(jnp.int32)
    heat = heat_ref[...].T
    lanes = lax.broadcasted_iota(jnp.int32, (128, 128), 1)
    for g in range(8):
        level = lanes == zed[:, g:g + 1]
        at = pl.ds(g * 128, 128)
        for q in range(2):
            h = jnp.where(level, heat[:, q * 8 + g:q * 8 + g + 1], 0.0)
            hi, lo = split2(h)
            W[at, q * 128:q * 128 + 128] = hi
            W[at, 256 + q * 128:256 + q * 128 + 128] = lo
    cells = lax.shift_right_logical(cell_ref[...], 7)

    def scatter(k, c):
        at = pl.multiple_of(k * 128, 128)
        ids = lax.broadcasted_iota(jnp.int32, (128, 1024), 0) + at
        hot = jnp.where(ids == cells, 1.0, 0.0).astype(jnp.bfloat16)
        d = jnp.dot(hot, W[...], preferred_element_type=f32)
        for q, ref in ((0, t_ref), (1, v_ref)):
            add = d[:, q * 128:q * 128 + 128] + d[:, 256 + q * 128:256 + q * 128 + 128]
            new = ref[pl.ds(at, 128), :] + add
            for j in range(4):
                E[q, pl.ds(pl.multiple_of((k * 4 + j + 1) * WY + 8, 8), 32), :] = new[j * 32:j * 32 + 32]
        return c
    lax.fori_loop(0, 16, scatter, 0)

    def plane(x):
        return x * WY + 8

    def exchange(s):
        moves = []
        for q in range(2):
            e = E.at[2 * s + q]
            moves.append(remote(e.at[pl.ds(plane(64), 32), :], e.at[pl.ds(plane(0), 32), :], xs.at[4 * s + 2 * q], xr.at[4 * s + 2 * q], right))
            moves.append(remote(e.at[pl.ds(plane(1), 32), :], e.at[pl.ds(plane(65), 32), :], xs.at[4 * s + 2 * q + 1], xr.at[4 * s + 2 * q + 1], left))
            yout[2 * s, pl.ds(64 * q, 64), :] = E[2 * s + q, pl.ds(plane(1) + 31, 64, stride=WY), :]
            yout[2 * s + 1, pl.ds(64 * q, 64), :] = E[2 * s + q, pl.ds(plane(1), 64, stride=WY), :]
        moves.append(remote(yout.at[2 * s], yin.at[2 * s], ys.at[2 * s], yr.at[2 * s], upper))
        moves.append(remote(yout.at[2 * s + 1], yin.at[2 * s + 1], ys.at[2 * s + 1], yr.at[2 * s + 1], lower))
        for c in moves:
            c.start()
        return moves

    def arrive(s, moves):
        for c in moves:
            c.wait_recv()
        for q in range(2):
            E[2 * s + q, pl.ds(plane(1) - 1, 64, stride=WY), :] = yin[2 * s, pl.ds(64 * q, 64), :]
            E[2 * s + q, pl.ds(plane(1) + 32, 64, stride=WY), :] = yin[2 * s + 1, pl.ds(64 * q, 64), :]

    moves = exchange(0)
    send_some(count // 3, 2 * count // 3)
    for c in winds:
        c.wait_recv()

    AX[pl.ds(0, 32), :] = 0.25 * (UE[0] + u_ref[pl.ds(0, 32), :])
    AX[pl.ds(64 * 32, 32), :] = 0.25 * (u_ref[pl.ds(63 * 32, 32), :] + UE[1])
    VE[pl.ds(7, 64, stride=WY), :] = vin[0]
    VE[pl.ds(40, 64, stride=WY), :] = vin[1]
    lane = lax.broadcasted_iota(jnp.int32, (32, 128), 1)

    def enter(k, c):
        for j in range(8):
            x = k * 8 + j
            VE[pl.ds(pl.multiple_of(x * WY + 8, 8), 32), :] = vv_ref[pl.ds(pl.multiple_of(x * 32, 32), 32), :]
        return c
    lax.fori_loop(0, 8, enter, 0)

    def faces(k, c):
        for j in range(4):
            x = k * 4 + j
            at = pl.ds(pl.multiple_of(x * 32, 32), 32)
            here = vv_ref[at, :]
            AL[at, :] = 0.25 * (here + VE[pl.ds(x * WY + 7, 32), :])
            AH[at, :] = 0.25 * (here + VE[pl.ds(x * WY + 9, 32), :])
            w = w_ref[at, :]
            AZ[at, :] = jnp.where(lane == 127, 0.0, 0.25 * (w + pltpu.roll(w, 127, 1)))
            AD[at, :] = jnp.where(lane == 0, 0.0, 0.25 * (w + pltpu.roll(w, 1, 1)))
        return c
    lax.fori_loop(0, 16, faces, 0)

    def face_x(k, c):
        for j in range(7):
            x = k * 7 + j + 1
            AX[pl.ds(pl.multiple_of(x * 32, 32), 32), :] = 0.25 * (u_ref[pl.ds(pl.multiple_of(x * 32 - 32, 32), 32), :] + u_ref[pl.ds(pl.multiple_of(x * 32, 32), 32), :])
        return c
    lax.fori_loop(0, 9, face_x, 0)

    for s, weight in enumerate((advect_step / 3.0, advect_step / 2.0, advect_step)):
        arrive(s, moves)
        for q in range(2):
            src = E.at[2 * s + q]
            start = E.at[q]
            def step(k, carry, q=q, src=src, start=start, s=s, weight=weight):
                f, low = carry
                for j in range(UNROLL):
                    x = k * UNROLL + j
                    at = pl.ds(pl.multiple_of(x * 32, 32), 32)
                    p = pl.multiple_of((x + 1) * WY + 8, 8)
                    after = src[pl.ds(pl.multiple_of(p + WY, 8), 32), :]
                    high = AX[pl.ds(pl.multiple_of(x * 32 + 32, 32), 32), :] * (f + after)
                    fy = AH[at, :] * (f + src[pl.ds(p + 1, 32), :]) - AL[at, :] * (src[pl.ds(p - 1, 32), :] + f)
                    fz = AZ[at, :] * (f + pltpu.roll(f, 127, 1)) - AD[at, :] * (pltpu.roll(f, 1, 1) + f)
                    out = start[pl.ds(p, 32), :] - weight * ((high - low) + fy + fz)
                    if s < 2:
                        E[2 * s + 2 + q, pl.ds(p, 32), :] = out
                    else:
                        (to_ref, vo_ref)[q][at, :] = out
                    f, low = after, high
                return f, low
            f0 = src[pl.ds(plane(1), 32), :]
            lax.fori_loop(0, 64 // UNROLL, step, (f0, AX[pl.ds(0, 32), :] * (src[pl.ds(plane(0), 32), :] + f0)))
        for c in moves:
            c.wait_send()
        if s < 2:
            moves = exchange(s + 1)
        if s == 0:
            send_some(2 * count // 3, count)
    for c in winds:
        c.wait_send()
    whole = remote(recv_ref.at[pl.ds(8, 8 * (count - 1)), :], recv_ref.at[pl.ds(8, 8 * (count - 1)), :], a2a_send, a2a_recv, right)
    whole.wait_send()
    whole.wait_recv()


def comm(mesh_shape, send, t, v, u, vv, w, cells, zed, heat):
    nx, ny = mesh_shape
    VM = pl.BlockSpec(memory_space=pltpu.VMEM)
    bf16 = jnp.bfloat16
    DMA = pltpu.SemaphoreType.DMA
    return pl.pallas_call(
        functools.partial(comm_kernel, nx, ny),
        out_shape=(jax.ShapeDtypeStruct((2048, 128), f32), jax.ShapeDtypeStruct((2048, 128), f32), jax.ShapeDtypeStruct((1024, 256), f32)),
        in_specs=[VM] * 9,
        out_specs=[VM] * 3,
        scratch_shapes=[
            pltpu.VMEM((6, WX * WY, 128), f32),
            pltpu.VMEM((65 * 32, 128), f32), pltpu.VMEM((2048, 128), f32), pltpu.VMEM((2048, 128), f32), pltpu.VMEM((2048, 128), f32), pltpu.VMEM((2048, 128), f32),
            pltpu.VMEM((2, 32, 128), f32), pltpu.VMEM((64 * WY, 128), f32),
            pltpu.VMEM((6, 128, 128), f32), pltpu.VMEM((6, 128, 128), f32),
            pltpu.VMEM((2, 64, 128), f32), pltpu.VMEM((2, 64, 128), f32),
            pltpu.VMEM((1024, 512), bf16),
            DMA, DMA, DMA((12,)), DMA((12,)), DMA((6,)), DMA((6,)), DMA((4,)), DMA((4,)), pltpu.SemaphoreType.REGULAR,
        ],
        compiler_params=pltpu.CompilerParams(vmem_limit_bytes=32 * 2**20, collective_id=0, has_side_effects=True),
        cost_estimate=pl.CostEstimate(flops=3_000_000_000, bytes_accessed=8_000_000, transcendentals=0),
        name="exchange",
    )(send, t, v, u, vv, w, cells, zed, heat)


def triangle(n):
    return lax.broadcasted_iota(jnp.int32, (n, n), 0) < lax.broadcasted_iota(jnp.int32, (n, n), 1)


def split3(x):
    hi = x.astype(jnp.bfloat16)
    rest = x - hi.astype(f32)
    mid = rest.astype(jnp.bfloat16)
    return hi, mid, (rest - mid.astype(f32)).astype(jnp.bfloat16)


def compact_kernel(recv_ref, ti_ref, vi_ref, to_ref, vo_ref, ro_ref, mo_ref, X):
    to_ref[...] = ti_ref[...]
    vo_ref[...] = vi_ref[...]
    rows = []
    for g in range(8):
        rows.append(recv_ref[pl.ds(g * 128, 128), 128:256].T[0:1])
    first = jnp.concatenate(rows, axis=0)
    taken = jnp.where(first > 0.0, 1.0, 0.0)
    within = jnp.dot(taken.astype(jnp.bfloat16), jnp.where(triangle(128), 1.0, 0.0).astype(jnp.bfloat16), preferred_element_type=f32)
    total = jnp.sum(taken, axis=1, keepdims=True)
    pos = []
    before = jnp.zeros((1, 1), f32)
    for g in range(8):
        pos.append(jnp.where(first[g:g + 1] > 0.0, within[g:g + 1] + before, -1.0))
        before = before + total[g:g + 1]
    pos = jnp.concatenate(pos, axis=1).astype(jnp.int32)
    for g in range(8):
        at = pl.ds(g * 128, 128)
        for k, part in enumerate(split3(recv_ref[at, :])):
            X[at, k * 256:k * 256 + 256] = part
    for n in range(4):
        ids = lax.broadcasted_iota(jnp.int32, (128, 1024), 0) + n * 128
        hot = jnp.where(ids == pos, 1.0, 0.0).astype(jnp.bfloat16)
        d = jnp.dot(hot, X[...], preferred_element_type=f32)
        d = d[:, 0:256] + (d[:, 256:512] + d[:, 512:768])
        ro_ref[pl.ds(n * 128, 128), :] = d[:, 0:128]
        mo_ref[pl.ds(n * 128, 128), :] = d[:, 128:256]


def compacted(recv, t, v):
    VM = pl.BlockSpec(memory_space=pltpu.VMEM)
    field = jax.ShapeDtypeStruct(t.shape, f32)
    drops = jax.ShapeDtypeStruct((512, 128), f32)
    return pl.pallas_call(
        compact_kernel,
        out_shape=(field, field, drops, drops),
        in_specs=[VM] * 3, out_specs=[VM] * 4,
        scratch_shapes=[pltpu.VMEM((1024, 768), jnp.bfloat16)],
        compiler_params=pltpu.CompilerParams(vmem_limit_bytes=12 * 2**20),
        cost_estimate=pl.CostEstimate(flops=800_000_000, bytes_accessed=2_000_000, transcendentals=0),
        name="compact",
    )(recv, t, v)


def body(
    shape,
    tprime,
    vapor,
    wind_u,
    wind_v,
    wind_w,
    radius,
    min_radius,
    multiplicity,
    drop_counts,
    cell_index,
    move_list,
):
    home = radius.shape[0]
    columns = tprime.shape[0] * tprime.shape[1]
    levels = tprime.shape[2]
    flat = [a.reshape(columns, levels) for a in (tprime, vapor, wind_u, wind_v, wind_w)]
    square = (8, home // 8)
    cells = cell_index.reshape(square)
    send, heat = physics(
        cell_index,
        flat[0],
        flat[1],
        radius,
        min_radius,
        multiplicity,
        drop_counts.reshape(square),
        cells,
        move_list.reshape(1, home),
    )
    temperature, humidity, recv = comm(shape, send, *flat, cell_index.reshape(1, home), cells, heat)
    temperature, humidity, radius_out, multiplicity_out = compacted(recv, temperature, humidity)
    return (
        temperature.reshape(tprime.shape),
        humidity.reshape(vapor.shape),
        radius_out,
        multiplicity_out,
    )


def solution(mesh):
    placed = (
        P("gx", "gy", None),
        P("gx", "gy", None),
        P("gx", "gy", None),
        P("gx", "gy", None),
        P("gx", "gy", None),
        P(("gx", "gy"), None),
        P(("gx", "gy"), None),
        P(("gx", "gy"), None),
        P(("gx", "gy")),
        P(("gx", "gy")),
        P(("gx", "gy")),
    )
    return jax.shard_map(
        functools.partial(body, (mesh.shape["gx"], mesh.shape["gy"])),
        mesh=mesh,
        in_specs=placed,
        out_specs=(
            P("gx", "gy", None),
            P("gx", "gy", None),
            P(("gx", "gy"), None),
            P(("gx", "gy"), None),
        ),
        check_vma=False,
    )
```

```python
import functools

import jax
import jax.numpy as jnp
from jax import lax
from jax.experimental import pallas as pl
from jax.experimental.pallas import tpu as pltpu
from jax.sharding import PartitionSpec as P

MESH = pl.DeviceIdType.MESH
f32 = jnp.float32
SUBSTEPS = 6
WX, WY = 66, 48
UNROLL = 8
EARLY, SECOND = 3, 6

clausius = 0.07
growth = 200.0 / 3.0
solute = 0.05
condense = 5e-07
latent = 10.0
collect = 1e-07
time_step = 2.0
advect_step = 0.6


def batcher(n):
    out = []
    p = 1
    while p < n:
        k = p
        while k >= 1:
            for j in range(k % p, n - k, 2 * k):
                for i in range(min(k, n - j - k)):
                    if (i + j) // (2 * p) == (i + j + k) // (2 * p):
                        out.append((i + j, i + j + k))
            k //= 2
        p *= 2
    return out

NET16 = batcher(16)

def halves(top, n=16):
    out = []
    d = top
    while d >= 1:
        for i in range(n):
            if not i & d:
                out.append((i, i + d))
        d //= 2
    return out

def make_passes():
    passes = []
    up, down = list(range(16)), list(range(15, -1, -1))
    passes.append((4, [(lambda t: t * 32, up, up, NET16), (lambda t: t * 32, [16 + o for o in up], [16 + o for o in down], NET16)]))
    for level in (32, 64, 128):
        step = level // 16
        if level == 128:
            passes.append((step, [(lambda t: t, [step * o for o in up], [step * o for o in up], halves(8))]))
        else:
            per = step
            passes.append((128 // level, [(lambda t, b=b, level=level: t * level + b, [step * o for o in up], [step * o for o in up], halves(8)) for b in range(per)]))
        ces = halves(step // 2)
        if level == 128:
            passes.append((8, [(lambda t: t * 16, up, up, ces)]))
        else:
            sets = []
            for s in range(2 * level // 16):
                loads = [16 * s + o for o in up]
                stores = loads if s * 16 < level else [level + 2 * level - 1 - o for o in loads]
                sets.append((lambda t, level=level: t * 2 * level, loads, stores, ces))
            passes.append((128 // (2 * level), sets))
    return passes

PASSES = make_passes()
N_CE = sum(trips * sum(len(s[3]) for s in sets) for trips, sets in PASSES)

def moves(sets):
    return any(set(s[1]) != set(s[2]) for s in sets)

def row(ref, d):
    if isinstance(d, int):
        return ref.at[pl.ds(d * 8, 8), :]
    return ref.at[pl.ds(pl.multiple_of(d * 8, 8), 8), :]

def loop(trips, body):
    if trips == 1:
        body(0)
    else:
        def step(t, c):
            body(t)
            return c
        lax.fori_loop(0, trips, step, 0)

def sort_blocks(keys, vals, marks):
    at = 0
    side = 0
    for trips, sets in PASSES:
        count = sum(len(s[3]) for s in sets)
        key, val = keys[side], vals[side]
        if moves(sets):
            side = 1 - side
        key_to, val_to = keys[side], vals[side]
        def body(t, sets=sets, at=at, count=count, key=key, val=val, key_to=key_to, val_to=val_to):
            m = at + t * count
            for base, loads, stores, ces in sets:
                b = base(t)
                ks = [row(key, b + o)[...] for o in loads]
                vs = [row(val, b + o)[...] for o in loads]
                for i, j in ces:
                    c = ks[i] > ks[j]
                    row(marks, m)[...] = jnp.where(c, 1.0, 0.0)
                    m = m + 1
                    ks[i], ks[j] = jnp.minimum(ks[i], ks[j]), jnp.maximum(ks[i], ks[j])
                    vs[i], vs[j] = jnp.where(c, vs[j], vs[i]), jnp.where(c, vs[i], vs[j])
                for o, k, v in zip(stores, ks, vs):
                    row(key_to, b + o)[...] = k
                    row(val_to, b + o)[...] = v
        loop(trips, body)
        at += trips * count

def unsort_blocks(firsts, seconds, marks):
    at = N_CE
    side = 0
    for trips, sets in reversed(PASSES):
        count = sum(len(s[3]) for s in sets)
        at -= trips * count
        xa, xb = firsts[side], seconds[side]
        if moves(sets):
            side = 1 - side
        xa_to, xb_to = firsts[side], seconds[side]
        def body(t, sets=sets, at=at, count=count, xa=xa, xb=xb, xa_to=xa_to, xb_to=xb_to):
            m = at + t * count
            for base, loads, stores, ces in sets:
                b = base(t)
                xs = [row(xa, b + o)[...] for o in stores]
                ys = [row(xb, b + o)[...] for o in stores]
                for q in reversed(range(len(ces))):
                    i, j = ces[q]
                    c = row(marks, m + q)[...] > 0.5
                    xs[i], xs[j] = jnp.where(c, xs[j], xs[i]), jnp.where(c, xs[i], xs[j])
                    ys[i], ys[j] = jnp.where(c, ys[j], ys[i]), jnp.where(c, ys[i], ys[j])
                m = m + len(ces)
                for o, x, y in zip(loads, xs, ys):
                    row(xa_to, b + o)[...] = x
                    row(xb_to, b + o)[...] = y
        loop(trips, body)

def gather_cells(index, t_ref, v_ref, cell_ref, ct, cv, T, V):
    def rows(k, c):
        for j in range(16):
            b = k * 16 + j
            at = lax.shift_right_logical(index[b], 7)
            T[pl.ds(b, 1), :] = t_ref[pl.ds(at, 1), :]
            V[pl.ds(b, 1), :] = v_ref[pl.ds(at, 1), :]
        return c
    lax.fori_loop(0, 64, rows, 0)
    level = lax.rem(cell_ref[...], 128)
    depth = lax.broadcasted_iota(jnp.int32, (128, 128), 0)
    for g in range(8):
        here = depth == level[g:g + 1]
        for staged, cell in ((T, ct), (V, cv)):
            picked = jnp.where(here, staged[pl.ds(g * 128, 128), :].T, 0.0)
            cell[pl.ds(g, 1), :] = jnp.sum(picked, axis=0, keepdims=True)


def condense_blocks(rad_ref, flo_ref, mul_ref, cnt_ref, heat_ref, R, S, C, F, M, ct_ref, cv_ref):

    def enter(g, c):
        to = pl.ds(g, 128, stride=8)
        R[to, :] = rad_ref[g].T
        F[to, :] = flo_ref[g].T
        M[to, :] = mul_ref[g].T
        return c
    lax.fori_loop(0, 8, enter, 0)
    counts = cnt_ref[...]
    zero = jnp.zeros((8, 128), jnp.float32)
    U = 8

    def init(t, w):
        for u in range(U):
            d = t * U + u
            r = row(R, d)[...]
            f = row(F, d)[...]
            m = jnp.where(counts > d, row(M, d)[...], 0.0)
            r2 = r * r
            f2 = f * f
            row(M, d)[...] = m
            row(R, d)[...] = r2
            row(S, d)[...] = lax.rsqrt(r2)
            row(F, d)[...] = f2
            row(C, d)[...] = (growth * solute) * f2 * f
            w = w + m * (r2 * r)
        return w
    weight = lax.fori_loop(0, 128 // U, init, zero)
    temp = ct_ref[...]
    wet = cv_ref[...]
    for _ in range(SUBSTEPS):
        sat = growth * ((1.0 + wet) * jnp.exp(-clausius * temp) - 1.0)
        def sub(t, w):
            for u in range(U):
                d = t * U + u
                r2 = row(R, d)[...]
                rs = row(S, d)[...]
                g = jnp.maximum(r2 + (sat + row(C, d)[...] * (rs * rs * rs)), row(F, d)[...])
                ns = lax.rsqrt(g)
                row(R, d)[...] = g
                row(S, d)[...] = ns
                w = w + row(M, d)[...] * (g * (g * ns))
            return w
        after = lax.fori_loop(0, 128 // U, sub, zero)
        condensed = after - weight
        weight = after
        wet = wet - condense * condensed
        temp = temp + latent * condense * condensed
    heat_ref[0:8, :] = temp - ct_ref[...]
    heat_ref[8:16, :] = wet - cv_ref[...]


def collect_blocks(R, S, C, F, M, marks, X):
    zero = jnp.zeros((8, 128), jnp.float32)
    U = 8

    def radii(t, c):
        for u in range(U):
            d = t * U + u
            row(R, d)[...] = row(R, d)[...] * row(S, d)[...]
        return c
    lax.fori_loop(0, 128 // U, radii, 0)
    sort_blocks((R, S), (M, C), marks)

    def both(t, carry):
        a0, a1, a3, a4, b0, b1, b3, b4 = carry
        for u in range(U):
            d = t * U + u
            r = row(R, d)[...]
            m = row(M, d)[...]
            r2 = r * r
            r3 = r2 * r
            r4 = r2 * r2
            gain = r4 * a0 + 2.0 * (r3 * a1 - r * a3) - a4
            w = m * r3
            a0 = a0 + w
            a1 = a1 + w * r
            a3 = a3 + w * r3
            a4 = a4 + w * r4
            grown = r3 + (time_step * collect) * gain
            row(S, d)[...] = jnp.where(m > 0.0, jnp.exp(jnp.log(grown) * (1.0 / 3.0)), 0.0)
            d = 127 - d
            r = row(R, d)[...]
            m = row(M, d)[...]
            r2 = r * r
            r3 = r2 * r
            r4 = r2 * r2
            loss = b4 + 2.0 * (r * b3 - r3 * b1) - r4 * b0
            b0 = b0 + m
            b1 = b1 + m * r
            b3 = b3 + m * r3
            b4 = b4 + m * r4
            row(C, d)[...] = m * jnp.exp((-time_step * collect) * loss)
        return a0, a1, a3, a4, b0, b1, b3, b4
    lax.fori_loop(0, 128 // U, both, (zero,) * 8)
    unsort_blocks((S, R), (C, F), marks)

    def leave(g, c):
        at = pl.ds(pl.multiple_of(g * 128, 128), 128)
        frm = pl.ds(g, 128, stride=8)
        for q, ref in enumerate((S, C)):
            for k, part in enumerate(split3(ref[frm, :].T)):
                X[at, k * 256 + q * 128:k * 256 + q * 128 + 128] = part
        return c
    lax.fori_loop(0, 8, leave, 0)


def mod(a, n):
    return lax.rem(a + n, n)


def split2(x):
    hi = x.astype(jnp.bfloat16)
    lo = (x - hi.astype(f32)).astype(jnp.bfloat16)
    return hi, lo


def row_moves(nx, ny, ix, iy, k, send_ref, recv_ref, s, r):
    px = mod(ix + k, nx)
    me = ix * ny + iy

    def body(i, c):
        py = mod(iy + i, ny)
        pltpu.make_async_remote_copy(
            src_ref=send_ref.at[pl.ds(pl.multiple_of((px * ny + py) * 8, 8), 8), :],
            dst_ref=recv_ref.at[pl.ds(pl.multiple_of(me * 8, 8), 8), :],
            send_sem=s, recv_sem=r, device_id=(px, py), device_id_type=MESH).start()
        return c
    lax.fori_loop(1 if k == 0 else 0, ny, body, 0)


def step_kernel(nx, ny, index, t_hbm, v_hbm, u_hbm, vv_hbm, w_hbm, rad_hbm, flo_hbm, mul_hbm, cnt_ref, square_ref, cell_ref, move_ref,
                to_ref, vo_ref, recv_ref,
                t_ref, v_ref, u_ref, vv_ref, w_ref, rad_ref, flo_ref, mul_ref, send_ref, heat_ref, R, S, C, F, M, marks, X, ct_ref, cv_ref,
                E, AX, AL, AH, AZ, AD, UE, VE, xin, yout, yin, vout, vin, W,
                a2a_send, a2a_recv, xs, xr, ys, yr, ws, wr, rows, loads):
    ix, iy = lax.axis_index("gx"), lax.axis_index("gy")
    me = ix * ny + iy
    right, left = (mod(ix + 1, nx), iy), (mod(ix - 1, nx), iy)
    upper, lower = (ix, mod(iy + 1, ny)), (ix, mod(iy - 1, ny))

    fetched = []
    for n, (src, dst) in enumerate(((t_hbm, t_ref), (v_hbm, v_ref), (rad_hbm, rad_ref), (flo_hbm, flo_ref), (mul_hbm, mul_ref), (vv_hbm, vv_ref), (u_hbm, u_ref), (w_hbm, w_ref))):
        fetched.append(pltpu.make_async_copy(src, dst, loads.at[n]))
        fetched[-1].start()
    barrier = pltpu.get_barrier_semaphore()
    for i in range(1, ny):
        pl.semaphore_signal(barrier, inc=1, device_id=(ix, mod(iy + i, ny)), device_id_type=MESH)
    for i in range(1, nx):
        pl.semaphore_signal(barrier, inc=1, device_id=(mod(ix + i, nx), iy), device_id_type=MESH)

    def remote(src, dst, s, r, to):
        return pltpu.make_async_remote_copy(src_ref=src, dst_ref=dst, send_sem=s, recv_sem=r, device_id=to, device_id_type=MESH)

    fetched[0].wait()
    fetched[1].wait()
    gather_cells(index, t_ref, v_ref, square_ref, ct_ref, cv_ref, S, C)
    for n in (2, 3, 4):
        fetched[n].wait()
    condense_blocks(rad_ref, flo_ref, mul_ref, cnt_ref, heat_ref, R, S, C, F, M, ct_ref, cv_ref)
    fetched[5].wait()
    fetched[6].wait()
    vout[0] = vv_ref[pl.ds(31, 64, stride=32), :]
    vout[1] = vv_ref[pl.ds(0, 64, stride=32), :]
    for e in range(6):
        for at in (WY + 7, WY + 40):
            E[e, pl.ds(at, 64, stride=WY), :] = jnp.zeros((64, 128), f32)
    pl.semaphore_wait(barrier, nx + ny - 2)
    for i in range(1, ny):
        pl.semaphore_signal(rows, inc=1, device_id=(ix, mod(iy + i, ny)), device_id_type=MESH)
    winds = [
        remote(u_ref.at[pl.ds(63 * 32, 32), :], UE.at[0], ws.at[0], wr.at[0], right),
        remote(u_ref.at[pl.ds(0, 32), :], UE.at[1], ws.at[1], wr.at[1], left),
        remote(vout.at[0], vin.at[0], ws.at[2], wr.at[2], upper),
        remote(vout.at[1], vin.at[1], ws.at[3], wr.at[3], lower),
    ]
    for c in winds:
        c.start()
    collect_blocks(R, S, C, F, M, marks, X)
    moves_to = move_ref[...]

    def place(k):
        at = pl.multiple_of(mod(ix + k, nx) * (ny * 8), ny * 8)
        ids = lax.broadcasted_iota(jnp.int32, (ny * 8, 1024), 0) + at
        hot = jnp.where(ids == moves_to, 1.0, 0.0).astype(jnp.bfloat16)
        d = jnp.dot(hot, X[...], preferred_element_type=f32)
        send_ref[pl.ds(at, ny * 8), :] = d[:, 0:256] + (d[:, 256:512] + d[:, 512:768])

    def send_row(k):
        row_moves(nx, ny, ix, iy, k, send_ref, recv_ref, a2a_send, a2a_recv)

    place(0)
    pl.semaphore_wait(rows, ny - 1)
    send_row(0)
    for k in range(1, nx):
        place(k)
        if k < EARLY:
            send_row(k)
    mine = pl.ds(pl.multiple_of(me * 8, 8), 8)
    recv_ref[mine, :] = send_ref[mine, :]

    zed = lax.rem(square_ref[...], 128).astype(f32).T.astype(jnp.int32)
    heat = heat_ref[...].T
    lanes = lax.broadcasted_iota(jnp.int32, (128, 128), 1)
    for g in range(8):
        level = lanes == zed[:, g:g + 1]
        at = pl.ds(g * 128, 128)
        for q in range(2):
            h = jnp.where(level, heat[:, q * 8 + g:q * 8 + g + 1], 0.0)
            hi, lo = split2(h)
            W[at, q * 128:q * 128 + 128] = hi
            W[at, 256 + q * 128:256 + q * 128 + 128] = lo
    cells = lax.shift_right_logical(cell_ref[...], 7)

    def scatter(k, c):
        at = pl.multiple_of(k * 128, 128)
        ids = lax.broadcasted_iota(jnp.int32, (128, 1024), 0) + at
        hot = jnp.where(ids == cells, 1.0, 0.0).astype(jnp.bfloat16)
        d = jnp.dot(hot, W[...], preferred_element_type=f32)
        for q, ref in ((0, t_ref), (1, v_ref)):
            add = d[:, q * 128:q * 128 + 128] + d[:, 256 + q * 128:256 + q * 128 + 128]
            new = ref[pl.ds(at, 128), :] + add
            for j in range(4):
                E[q, pl.ds(pl.multiple_of((k * 4 + j + 1) * WY + 8, 8), 32), :] = new[j * 32:j * 32 + 32]
        return c
    lax.fori_loop(0, 16, scatter, 0)

    def plane(x):
        return x * WY + 8

    def exchange(s):
        moves = []
        for q in range(2):
            e = E.at[2 * s + q]
            n = 4 * s + 2 * q
            moves.append(remote(e.at[pl.ds(plane(64), 32), :], xin.at[n], xs.at[n], xr.at[n], right))
            moves.append(remote(e.at[pl.ds(plane(1), 32), :], xin.at[n + 1], xs.at[n + 1], xr.at[n + 1], left))
            yout[2 * s, pl.ds(64 * q, 64), :] = E[2 * s + q, pl.ds(plane(1) + 31, 64, stride=WY), :]
            yout[2 * s + 1, pl.ds(64 * q, 64), :] = E[2 * s + q, pl.ds(plane(1), 64, stride=WY), :]
        moves.append(remote(yout.at[2 * s], yin.at[2 * s], ys.at[2 * s], yr.at[2 * s], upper))
        moves.append(remote(yout.at[2 * s + 1], yin.at[2 * s + 1], ys.at[2 * s + 1], yr.at[2 * s + 1], lower))
        for c in moves:
            c.start()
        return moves

    moves = exchange(0)
    for k in range(EARLY, SECOND):
        send_row(k)
    fetched[7].wait()
    for c in winds:
        c.wait_recv()

    AX[pl.ds(0, 32), :] = 0.25 * (UE[0] + u_ref[pl.ds(0, 32), :])
    AX[pl.ds(64 * 32, 32), :] = 0.25 * (u_ref[pl.ds(63 * 32, 32), :] + UE[1])
    VE[pl.ds(7, 64, stride=WY), :] = vin[0]
    VE[pl.ds(40, 64, stride=WY), :] = vin[1]
    lane = lax.broadcasted_iota(jnp.int32, (32, 128), 1)

    def enter(k, c):
        for j in range(8):
            x = k * 8 + j
            VE[pl.ds(pl.multiple_of(x * WY + 8, 8), 32), :] = vv_ref[pl.ds(pl.multiple_of(x * 32, 32), 32), :]
        return c
    lax.fori_loop(0, 8, enter, 0)

    def faces(k, c):
        for j in range(4):
            x = k * 4 + j
            at = pl.ds(pl.multiple_of(x * 32, 32), 32)
            here = vv_ref[at, :]
            AL[at, :] = 0.25 * (here + VE[pl.ds(x * WY + 7, 32), :])
            AH[at, :] = 0.25 * (here + VE[pl.ds(x * WY + 9, 32), :])
            w = w_ref[at, :]
            AZ[at, :] = jnp.where(lane == 127, 0.0, 0.25 * (w + pltpu.roll(w, 127, 1)))
            AD[at, :] = jnp.where(lane == 0, 0.0, 0.25 * (w + pltpu.roll(w, 1, 1)))
        return c
    lax.fori_loop(0, 16, faces, 0)

    def face_x(k, c):
        for j in range(7):
            x = k * 7 + j + 1
            AX[pl.ds(pl.multiple_of(x * 32, 32), 32), :] = 0.25 * (u_ref[pl.ds(pl.multiple_of(x * 32 - 32, 32), 32), :] + u_ref[pl.ds(pl.multiple_of(x * 32, 32), 32), :])
        return c
    lax.fori_loop(0, 9, face_x, 0)

    for s, weight in enumerate((advect_step / 3.0, advect_step / 2.0, advect_step)):
        for q in range(2):
            src = E.at[2 * s + q]
            start = E.at[q]
            def step(k, carry, q=q, src=src, start=start, s=s, weight=weight):
                f, low = carry
                for j in range(UNROLL):
                    x = k * UNROLL + j
                    at = pl.ds(pl.multiple_of(x * 32, 32), 32)
                    p = pl.multiple_of((x + 1) * WY + 8, 8)
                    after = src[pl.ds(pl.multiple_of(p + WY, 8), 32), :]
                    high = AX[pl.ds(pl.multiple_of(x * 32 + 32, 32), 32), :] * (f + after)
                    fy = AH[at, :] * (f + src[pl.ds(p + 1, 32), :]) - AL[at, :] * (src[pl.ds(p - 1, 32), :] + f)
                    fz = AZ[at, :] * (f + pltpu.roll(f, 127, 1)) - AD[at, :] * (pltpu.roll(f, 1, 1) + f)
                    out = start[pl.ds(p, 32), :] - weight * ((high - low) + fy + fz)
                    if s < 2:
                        E[2 * s + 2 + q, pl.ds(p, 32), :] = out
                    else:
                        (to_ref, vo_ref)[q][at, :] = out
                    f, low = after, high
                return f, low
            f0 = src[pl.ds(plane(1), 32), :]
            lax.fori_loop(0, 64 // UNROLL, step, (f0, AX[pl.ds(0, 32), :] * f0))
        for c in moves:
            c.wait_recv()
        for q in range(2):
            if s < 2:
                dst, base, wide = E.at[2 * s + 2 + q], plane(1), WY
            else:
                dst, base, wide = (to_ref, vo_ref)[q], 0, 32
            n = 4 * s + 2 * q
            first, last = pl.ds(base, 32), pl.ds(base + 63 * wide, 32)
            dst[first, :] = dst[first, :] + weight * (AX[pl.ds(0, 32), :] * xin[n])
            dst[last, :] = dst[last, :] - weight * (AX[pl.ds(64 * 32, 32), :] * xin[n + 1])
            bottom, top = pl.ds(base, 64, stride=wide), pl.ds(base + 31, 64, stride=wide)
            dst[bottom, :] = dst[bottom, :] + weight * (AL[pl.ds(0, 64, stride=32), :] * yin[2 * s, pl.ds(64 * q, 64), :])
            dst[top, :] = dst[top, :] - weight * (AH[pl.ds(31, 64, stride=32), :] * yin[2 * s + 1, pl.ds(64 * q, 64), :])
        for c in moves:
            c.wait_send()
        if s < 2:
            moves = exchange(s + 1)
        if s == 0:
            for k in range(SECOND, nx):
                send_row(k)
    for c in winds:
        c.wait_send()
    rest = pl.ds(8, 8 * (nx * ny - 1))
    whole = remote(recv_ref.at[rest, :], recv_ref.at[rest, :], a2a_send, a2a_recv, right)
    whole.wait_send()
    whole.wait_recv()


def step_call(mesh_shape, index, fields, droplets, counts, square, cells, moves):
    nx, ny = mesh_shape
    VM = pl.BlockSpec(memory_space=pltpu.VMEM)
    HB = pl.BlockSpec(memory_space=pltpu.HBM)
    bf16 = jnp.bfloat16
    DMA = pltpu.SemaphoreType.DMA
    plane = pltpu.VMEM((2048, 128), f32)
    block = pltpu.VMEM((1024, 128), f32)
    return pl.pallas_call(
        functools.partial(step_kernel, nx, ny),
        out_shape=(jax.ShapeDtypeStruct((2048, 128), f32), jax.ShapeDtypeStruct((2048, 128), f32), jax.ShapeDtypeStruct((1024, 256), f32)),
        in_specs=[pl.BlockSpec(memory_space=pltpu.SMEM)] + [HB] * 8 + [VM] * 4,
        out_specs=[VM] * 3,
        scratch_shapes=[plane] * 5 + [pltpu.VMEM((8, 128, 128), f32)] * 3 + [pltpu.VMEM((1024, 256), f32), pltpu.VMEM((16, 128), f32)] + [block] * 5
        + [pltpu.VMEM((N_CE * 8, 128), f32), pltpu.VMEM((1024, 768), bf16), pltpu.VMEM((8, 128), f32), pltpu.VMEM((8, 128), f32)]
        + [
            pltpu.VMEM((6, WX * WY, 128), f32), pltpu.VMEM((65 * 32, 128), f32), plane, plane, plane, plane,
            pltpu.VMEM((2, 32, 128), f32), pltpu.VMEM((64 * WY, 128), f32),
            pltpu.VMEM((12, 32, 128), f32), pltpu.VMEM((6, 128, 128), f32), pltpu.VMEM((6, 128, 128), f32),
            pltpu.VMEM((2, 64, 128), f32), pltpu.VMEM((2, 64, 128), f32), pltpu.VMEM((1024, 512), bf16),
            DMA, DMA, DMA((12,)), DMA((12,)), DMA((6,)), DMA((6,)), DMA((4,)), DMA((4,)), pltpu.SemaphoreType.REGULAR, DMA((8,)),
        ],
        compiler_params=pltpu.CompilerParams(vmem_limit_bytes=50 * 2**20, collective_id=0, has_side_effects=True),
        cost_estimate=pl.CostEstimate(flops=5_000_000_000, bytes_accessed=8_000_000, transcendentals=0),
        name="step",
    )(index, *fields, *droplets, counts, square, cells, moves)


def triangle(n):
    return lax.broadcasted_iota(jnp.int32, (n, n), 0) < lax.broadcasted_iota(jnp.int32, (n, n), 1)


def split3(x):
    hi = x.astype(jnp.bfloat16)
    rest = x - hi.astype(f32)
    mid = rest.astype(jnp.bfloat16)
    return hi, mid, (rest - mid.astype(f32)).astype(jnp.bfloat16)


def compact_kernel(recv_ref, ti_ref, vi_ref, to_ref, vo_ref, ro_ref, mo_ref, X):
    to_ref[...] = ti_ref[...]
    vo_ref[...] = vi_ref[...]
    rows = []
    for g in range(8):
        rows.append(recv_ref[pl.ds(g * 128, 128), 128:256].T[0:1])
    first = jnp.concatenate(rows, axis=0)
    taken = jnp.where(first > 0.0, 1.0, 0.0)
    within = jnp.dot(taken.astype(jnp.bfloat16), jnp.where(triangle(128), 1.0, 0.0).astype(jnp.bfloat16), preferred_element_type=f32)
    total = jnp.sum(taken, axis=1, keepdims=True)
    pos = []
    before = jnp.zeros((1, 1), f32)
    for g in range(8):
        pos.append(jnp.where(first[g:g + 1] > 0.0, within[g:g + 1] + before, -1.0))
        before = before + total[g:g + 1]
    pos = jnp.concatenate(pos, axis=1).astype(jnp.int32)
    for g in range(8):
        at = pl.ds(g * 128, 128)
        for k, part in enumerate(split3(recv_ref[at, :])):
            X[at, k * 256:k * 256 + 256] = part
    for n in range(4):
        ids = lax.broadcasted_iota(jnp.int32, (128, 1024), 0) + n * 128
        hot = jnp.where(ids == pos, 1.0, 0.0).astype(jnp.bfloat16)
        d = jnp.dot(hot, X[...], preferred_element_type=f32)
        d = d[:, 0:256] + (d[:, 256:512] + d[:, 512:768])
        ro_ref[pl.ds(n * 128, 128), :] = d[:, 0:128]
        mo_ref[pl.ds(n * 128, 128), :] = d[:, 128:256]


def compacted(recv, t, v):
    VM = pl.BlockSpec(memory_space=pltpu.VMEM)
    field = jax.ShapeDtypeStruct(t.shape, f32)
    drops = jax.ShapeDtypeStruct((512, 128), f32)
    return pl.pallas_call(
        compact_kernel,
        out_shape=(field, field, drops, drops),
        in_specs=[VM] * 3, out_specs=[VM] * 4,
        scratch_shapes=[pltpu.VMEM((1024, 768), jnp.bfloat16)],
        compiler_params=pltpu.CompilerParams(vmem_limit_bytes=12 * 2**20),
        cost_estimate=pl.CostEstimate(flops=800_000_000, bytes_accessed=2_000_000, transcendentals=0),
        name="compact",
    )(recv, t, v)


def body(
    shape,
    tprime,
    vapor,
    wind_u,
    wind_v,
    wind_w,
    radius,
    min_radius,
    multiplicity,
    drop_counts,
    cell_index,
    move_list,
):
    home = radius.shape[0]
    columns = tprime.shape[0] * tprime.shape[1]
    levels = tprime.shape[2]
    flat = [pltpu.with_memory_space_constraint(a.reshape(columns, levels), pltpu.HBM) for a in (tprime, vapor, wind_u, wind_v, wind_w)]
    square = (8, home // 8)
    cells = cell_index.reshape(square)
    temperature, humidity, recv = step_call(
        shape,
        cell_index,
        flat,
        [pltpu.with_memory_space_constraint(a.reshape(8, home // 8, a.shape[1]), pltpu.HBM) for a in (radius, min_radius, multiplicity)],
        drop_counts.reshape(square),
        cells,
        cell_index.reshape(1, home),
        move_list.reshape(1, home),
    )
    temperature, humidity, radius_out, multiplicity_out = compacted(recv, temperature, humidity)
    return (
        temperature.reshape(tprime.shape),
        humidity.reshape(vapor.shape),
        radius_out,
        multiplicity_out,
    )


def solution(mesh):
    placed = (
        P("gx", "gy", None),
        P("gx", "gy", None),
        P("gx", "gy", None),
        P("gx", "gy", None),
        P("gx", "gy", None),
        P(("gx", "gy"), None),
        P(("gx", "gy"), None),
        P(("gx", "gy"), None),
        P(("gx", "gy")),
        P(("gx", "gy")),
        P(("gx", "gy")),
    )
    return jax.shard_map(
        functools.partial(body, (mesh.shape["gx"], mesh.shape["gy"])),
        mesh=mesh,
        in_specs=placed,
        out_specs=(
            P("gx", "gy", None),
            P("gx", "gy", None),
            P(("gx", "gy"), None),
            P(("gx", "gy"), None),
        ),
        check_vma=False,
    )
```

```python
import functools

import jax
import jax.numpy as jnp
from jax import lax
from jax.experimental import pallas as pl
from jax.experimental.pallas import tpu as pltpu
from jax.sharding import PartitionSpec as P

MESH = pl.DeviceIdType.MESH
f32 = jnp.float32
SUBSTEPS = 6
WX, WY = 66, 48
UNROLL = 8

clausius = 0.07
growth = 200.0 / 3.0
solute = 0.05
condense = 5e-07
latent = 10.0
collect = 1e-07
time_step = 2.0
advect_step = 0.6


def batcher(n):
    out = []
    p = 1
    while p < n:
        k = p
        while k >= 1:
            for j in range(k % p, n - k, 2 * k):
                for i in range(min(k, n - j - k)):
                    if (i + j) // (2 * p) == (i + j + k) // (2 * p):
                        out.append((i + j, i + j + k))
            k //= 2
        p *= 2
    return out

NET16 = batcher(16)

def halves(top, n=16):
    out = []
    d = top
    while d >= 1:
        for i in range(n):
            if not i & d:
                out.append((i, i + d))
        d //= 2
    return out

def make_passes():
    passes = []
    up, down = list(range(16)), list(range(15, -1, -1))
    passes.append((4, [(lambda t: t * 32, up, up, NET16), (lambda t: t * 32, [16 + o for o in up], [16 + o for o in down], NET16)]))
    for level in (32, 64, 128):
        step = level // 16
        if level == 128:
            passes.append((step, [(lambda t: t, [step * o for o in up], [step * o for o in up], halves(8))]))
        else:
            per = step
            passes.append((128 // level, [(lambda t, b=b, level=level: t * level + b, [step * o for o in up], [step * o for o in up], halves(8)) for b in range(per)]))
        ces = halves(step // 2)
        if level == 128:
            passes.append((8, [(lambda t: t * 16, up, up, ces)]))
        else:
            sets = []
            for s in range(2 * level // 16):
                loads = [16 * s + o for o in up]
                stores = loads if s * 16 < level else [level + 2 * level - 1 - o for o in loads]
                sets.append((lambda t, level=level: t * 2 * level, loads, stores, ces))
            passes.append((128 // (2 * level), sets))
    return passes

PASSES = make_passes()
N_CE = sum(trips * sum(len(s[3]) for s in sets) for trips, sets in PASSES)

def moves(sets):
    return any(set(s[1]) != set(s[2]) for s in sets)

def row(ref, d):
    if isinstance(d, int):
        return ref.at[pl.ds(d * 8, 8), :]
    return ref.at[pl.ds(pl.multiple_of(d * 8, 8), 8), :]

def loop(trips, body):
    if trips == 1:
        body(0)
    else:
        def step(t, c):
            body(t)
            return c
        lax.fori_loop(0, trips, step, 0)

def sort_blocks(keys, vals, marks):
    at = 0
    side = 0
    for trips, sets in PASSES:
        count = sum(len(s[3]) for s in sets)
        key, val = keys[side], vals[side]
        if moves(sets):
            side = 1 - side
        key_to, val_to = keys[side], vals[side]
        def body(t, sets=sets, at=at, count=count, key=key, val=val, key_to=key_to, val_to=val_to):
            m = at + t * count
            for base, loads, stores, ces in sets:
                b = base(t)
                ks = [row(key, b + o)[...] for o in loads]
                vs = [row(val, b + o)[...] for o in loads]
                for i, j in ces:
                    c = ks[i] > ks[j]
                    row(marks, m)[...] = jnp.where(c, 1.0, 0.0)
                    m = m + 1
                    ks[i], ks[j] = jnp.minimum(ks[i], ks[j]), jnp.maximum(ks[i], ks[j])
                    vs[i], vs[j] = jnp.where(c, vs[j], vs[i]), jnp.where(c, vs[i], vs[j])
                for o, k, v in zip(stores, ks, vs):
                    row(key_to, b + o)[...] = k
                    row(val_to, b + o)[...] = v
        loop(trips, body)
        at += trips * count

def unsort_blocks(firsts, seconds, marks):
    at = N_CE
    side = 0
    for trips, sets in reversed(PASSES):
        count = sum(len(s[3]) for s in sets)
        at -= trips * count
        xa, xb = firsts[side], seconds[side]
        if moves(sets):
            side = 1 - side
        xa_to, xb_to = firsts[side], seconds[side]
        def body(t, sets=sets, at=at, count=count, xa=xa, xb=xb, xa_to=xa_to, xb_to=xb_to):
            m = at + t * count
            for base, loads, stores, ces in sets:
                b = base(t)
                xs = [row(xa, b + o)[...] for o in stores]
                ys = [row(xb, b + o)[...] for o in stores]
                for q in reversed(range(len(ces))):
                    i, j = ces[q]
                    c = row(marks, m + q)[...] > 0.5
                    xs[i], xs[j] = jnp.where(c, xs[j], xs[i]), jnp.where(c, xs[i], xs[j])
                    ys[i], ys[j] = jnp.where(c, ys[j], ys[i]), jnp.where(c, ys[i], ys[j])
                m = m + len(ces)
                for o, x, y in zip(loads, xs, ys):
                    row(xa_to, b + o)[...] = x
                    row(xb_to, b + o)[...] = y
        loop(trips, body)

def gather_cells(index, t_ref, v_ref, cell_ref, ct, cv, T, V):
    def rows(k, c):
        for j in range(16):
            b = k * 16 + j
            at = lax.shift_right_logical(index[b], 7)
            T[pl.ds(b, 1), :] = t_ref[pl.ds(at, 1), :]
            V[pl.ds(b, 1), :] = v_ref[pl.ds(at, 1), :]
        return c
    lax.fori_loop(0, 64, rows, 0)
    level = lax.rem(cell_ref[...], 128)
    depth = lax.broadcasted_iota(jnp.int32, (128, 128), 0)
    for g in range(8):
        here = depth == level[g:g + 1]
        for staged, cell in ((T, ct), (V, cv)):
            picked = jnp.where(here, staged[pl.ds(g * 128, 128), :].T, 0.0)
            cell[pl.ds(g, 1), :] = jnp.sum(picked, axis=0, keepdims=True)


def condense_blocks(rad_ref, flo_ref, mul_ref, cnt_ref, heat_ref, R, S, C, F, M, ct_ref, cv_ref):

    def enter(g, c):
        to = pl.ds(g, 128, stride=8)
        R[to, :] = rad_ref[g].T
        F[to, :] = flo_ref[g].T
        M[to, :] = mul_ref[g].T
        return c
    lax.fori_loop(0, 8, enter, 0)
    counts = cnt_ref[...]
    zero = jnp.zeros((8, 128), jnp.float32)
    U = 32

    def init(t, w):
        for u in range(U):
            d = t * U + u
            r = row(R, d)[...]
            f = row(F, d)[...]
            m = jnp.where(counts > d, row(M, d)[...], 0.0)
            r2 = r * r
            f2 = f * f
            row(M, d)[...] = m
            row(R, d)[...] = r2
            row(S, d)[...] = lax.rsqrt(r2)
            row(F, d)[...] = f2
            row(C, d)[...] = (growth * solute) * f2 * f
            w = w + m * (r2 * r)
        return w
    weight = lax.fori_loop(0, 128 // U, init, zero)
    temp = ct_ref[...]
    wet = cv_ref[...]
    for _ in range(SUBSTEPS):
        sat = growth * ((1.0 + wet) * jnp.exp(-clausius * temp) - 1.0)
        def sub(t, w):
            for u in range(U):
                d = t * U + u
                r2 = row(R, d)[...]
                rs = row(S, d)[...]
                g = jnp.maximum(r2 + (sat + row(C, d)[...] * (rs * rs * rs)), row(F, d)[...])
                ns = lax.rsqrt(g)
                row(R, d)[...] = g
                row(S, d)[...] = ns
                w = w + row(M, d)[...] * (g * (g * ns))
            return w
        after = lax.fori_loop(0, 128 // U, sub, zero)
        condensed = after - weight
        weight = after
        wet = wet - condense * condensed
        temp = temp + latent * condense * condensed
    heat_ref[0:8, :] = temp - ct_ref[...]
    heat_ref[8:16, :] = wet - cv_ref[...]


def collect_blocks(R, S, C, F, M, marks, X):
    zero = jnp.zeros((8, 128), jnp.float32)
    U = 16

    def radii(t, c):
        for u in range(U):
            d = t * U + u
            row(R, d)[...] = row(R, d)[...] * row(S, d)[...]
        return c
    lax.fori_loop(0, 128 // U, radii, 0)
    sort_blocks((R, S), (M, C), marks)

    def both(t, carry):
        a0, a1, a3, a4, b0, b1, b3, b4 = carry
        for u in range(U):
            d = t * U + u
            r = row(R, d)[...]
            m = row(M, d)[...]
            r2 = r * r
            r3 = r2 * r
            r4 = r2 * r2
            gain = r4 * a0 + 2.0 * (r3 * a1 - r * a3) - a4
            w = m * r3
            a0 = a0 + w
            a1 = a1 + w * r
            a3 = a3 + w * r3
            a4 = a4 + w * r4
            grown = r3 + (time_step * collect) * gain
            row(S, d)[...] = jnp.where(m > 0.0, jnp.exp(jnp.log(grown) * (1.0 / 3.0)), 0.0)
            d = 127 - d
            r = row(R, d)[...]
            m = row(M, d)[...]
            r2 = r * r
            r3 = r2 * r
            r4 = r2 * r2
            loss = b4 + 2.0 * (r * b3 - r3 * b1) - r4 * b0
            b0 = b0 + m
            b1 = b1 + m * r
            b3 = b3 + m * r3
            b4 = b4 + m * r4
            row(C, d)[...] = m * jnp.exp((-time_step * collect) * loss)
        return a0, a1, a3, a4, b0, b1, b3, b4
    lax.fori_loop(0, 128 // U, both, (zero,) * 8)
    unsort_blocks((S, R), (C, F), marks)

    def leave(g, c):
        at = pl.ds(pl.multiple_of(g * 128, 128), 128)
        frm = pl.ds(g, 128, stride=8)
        for q, ref in enumerate((S, C)):
            for k, part in enumerate(split2(ref[frm, :].T)):
                X[at, k * 256 + q * 128:k * 256 + q * 128 + 128] = part
        return c
    lax.fori_loop(0, 8, leave, 0)


def mod(a, n):
    return lax.rem(a + n, n)


def split2(x):
    hi = x.astype(jnp.bfloat16)
    lo = (x - hi.astype(f32)).astype(jnp.bfloat16)
    return hi, lo


def row_moves(nx, ny, ix, iy, k, send_ref, recv_ref, s, r):
    px = mod(ix + k, nx)
    me = ix * ny + iy

    def body(i, c):
        py = mod(iy + i, ny)
        pltpu.make_async_remote_copy(
            src_ref=send_ref.at[pl.ds(pl.multiple_of((px * ny + py) * 8, 8), 8), :],
            dst_ref=recv_ref.at[pl.ds(pl.multiple_of(me * 8, 8), 8), :],
            send_sem=s, recv_sem=r, device_id=(px, py), device_id_type=MESH).start()
        return c
    lax.fori_loop(1 if k == 0 else 0, ny, body, 0)


def step_kernel(nx, ny, index, t_hbm, v_hbm, u_hbm, vv_hbm, w_hbm, rad_hbm, flo_hbm, mul_hbm, cnt_ref, square_ref, cell_ref, move_ref,
                to_ref, vo_ref, recv_ref,
                t_ref, v_ref, u_ref, vv_ref, w_ref, rad_ref, flo_ref, mul_ref, send_ref, heat_ref, R, S, C, F, M, marks, X, ct_ref, cv_ref,
                E, AX, AL, AH, AZ, AD, UE, VE, xin, yout, yin, vout, vin, W,
                a2a_send, a2a_recv, xs, xr, ys, yr, ws, wr, rows, loads):
    ix, iy = lax.axis_index("gx"), lax.axis_index("gy")
    me = ix * ny + iy
    right, left = (mod(ix + 1, nx), iy), (mod(ix - 1, nx), iy)
    upper, lower = (ix, mod(iy + 1, ny)), (ix, mod(iy - 1, ny))

    fetched = []
    for n, (src, dst) in enumerate(((t_hbm, t_ref), (v_hbm, v_ref), (rad_hbm, rad_ref), (flo_hbm, flo_ref), (mul_hbm, mul_ref), (vv_hbm, vv_ref), (u_hbm, u_ref), (w_hbm, w_ref))):
        fetched.append(pltpu.make_async_copy(src, dst, loads.at[n]))
        fetched[-1].start()
    barrier = pltpu.get_barrier_semaphore()
    for i in range(1, ny):
        pl.semaphore_signal(barrier, inc=1, device_id=(ix, mod(iy + i, ny)), device_id_type=MESH)
    for i in range(1, nx):
        pl.semaphore_signal(barrier, inc=1, device_id=(mod(ix + i, nx), iy), device_id_type=MESH)

    def remote(src, dst, s, r, to):
        return pltpu.make_async_remote_copy(src_ref=src, dst_ref=dst, send_sem=s, recv_sem=r, device_id=to, device_id_type=MESH)

    fetched[0].wait()
    fetched[1].wait()
    gather_cells(index, t_ref, v_ref, square_ref, ct_ref, cv_ref, S, C)
    for n in (2, 3, 4):
        fetched[n].wait()
    condense_blocks(rad_ref, flo_ref, mul_ref, cnt_ref, heat_ref, R, S, C, F, M, ct_ref, cv_ref)
    fetched[5].wait()
    fetched[6].wait()
    vout[0] = vv_ref[pl.ds(31, 64, stride=32), :]
    vout[1] = vv_ref[pl.ds(0, 64, stride=32), :]
    for e in range(6):
        for at in (WY + 7, WY + 40):
            E[e, pl.ds(at, 64, stride=WY), :] = jnp.zeros((64, 128), f32)
        E[e, pl.ds(65 * WY + 8, 32), :] = jnp.zeros((32, 128), f32)
    pl.semaphore_wait(barrier, nx + ny - 2)
    for i in range(1, ny):
        pl.semaphore_signal(rows, inc=1, device_id=(ix, mod(iy + i, ny)), device_id_type=MESH)
    winds = [
        remote(u_ref.at[pl.ds(63 * 32, 32), :], UE.at[0], ws.at[0], wr.at[0], right),
        remote(u_ref.at[pl.ds(0, 32), :], UE.at[1], ws.at[1], wr.at[1], left),
        remote(vout.at[0], vin.at[0], ws.at[2], wr.at[2], upper),
        remote(vout.at[1], vin.at[1], ws.at[3], wr.at[3], lower),
    ]
    for c in winds:
        c.start()
    zed = lax.rem(square_ref[...], 128).astype(f32).T.astype(jnp.int32)
    heat = heat_ref[...].T
    lanes = lax.broadcasted_iota(jnp.int32, (128, 128), 1)
    for g in range(8):
        level = lanes == zed[:, g:g + 1]
        at = pl.ds(g * 128, 128)
        for q in range(2):
            h = jnp.where(level, heat[:, q * 8 + g:q * 8 + g + 1], 0.0)
            hi, lo = split2(h)
            W[at, q * 128:q * 128 + 128] = hi
            W[at, 256 + q * 128:256 + q * 128 + 128] = lo
    cells = lax.shift_right_logical(cell_ref[...], 7)

    def scatter(k, c):
        at = pl.multiple_of(k * 128, 128)
        ids = lax.broadcasted_iota(jnp.int32, (128, 1024), 0) + at
        hot = jnp.where(ids == cells, 1.0, 0.0).astype(jnp.bfloat16)
        d = jnp.dot(hot, W[...], preferred_element_type=f32)
        for q, ref in ((0, t_ref), (1, v_ref)):
            add = d[:, q * 128:q * 128 + 128] + d[:, 256 + q * 128:256 + q * 128 + 128]
            new = ref[pl.ds(at, 128), :] + add
            for j in range(4):
                E[q, pl.ds(pl.multiple_of((k * 4 + j + 1) * WY + 8, 8), 32), :] = new[j * 32:j * 32 + 32]
        return c
    lax.fori_loop(0, 16, scatter, 0)

    def plane(x):
        return x * WY + 8

    def exchange(s, q):
        n = 4 * s + 2 * q
        e = E.at[2 * s + q]
        yout[n] = E[2 * s + q, pl.ds(plane(1) + 31, 64, stride=WY), :]
        yout[n + 1] = E[2 * s + q, pl.ds(plane(1), 64, stride=WY), :]
        moves = [
            remote(yout.at[n], yin.at[n], ys.at[n], yr.at[n], upper),
            remote(yout.at[n + 1], yin.at[n + 1], ys.at[n + 1], yr.at[n + 1], lower),
            remote(e.at[pl.ds(plane(64), 32), :], xin.at[n], xs.at[n], xr.at[n], right),
            remote(e.at[pl.ds(plane(1), 32), :], xin.at[n + 1], xs.at[n + 1], xr.at[n + 1], left),
        ]
        for c in moves:
            c.start()
        return moves

    moves = [exchange(0, 0), exchange(0, 1)]
    sent = [*winds, *moves[0], *moves[1]]
    collect_blocks(R, S, C, F, M, marks, X)
    moves_to = move_ref[...]

    def place(k):
        at = pl.multiple_of(mod(ix + k, nx) * (ny * 8), ny * 8)
        ids = lax.broadcasted_iota(jnp.int32, (ny * 8, 1024), 0) + at
        hot = jnp.where(ids == moves_to, 1.0, 0.0).astype(jnp.bfloat16)
        d = jnp.dot(hot, X[...], preferred_element_type=f32)
        send_ref[pl.ds(at, ny * 8), :] = d[:, 0:256] + d[:, 256:512]

    def send_row(k):
        row_moves(nx, ny, ix, iy, k, send_ref, recv_ref, a2a_send, a2a_recv)

    place(0)
    pl.semaphore_wait(rows, ny - 1)
    send_row(0)
    for k in range(1, nx):
        place(k)
        send_row(k)
    mine = pl.ds(pl.multiple_of(me * 8, 8), 8)
    recv_ref[mine, :] = send_ref[mine, :]

    fetched[7].wait()
    for c in winds:
        c.wait_recv()

    AX[pl.ds(0, 32), :] = 0.25 * (UE[0] + u_ref[pl.ds(0, 32), :])
    AX[pl.ds(64 * 32, 32), :] = 0.25 * (u_ref[pl.ds(63 * 32, 32), :] + UE[1])
    VE[pl.ds(7, 64, stride=WY), :] = vin[0]
    VE[pl.ds(40, 64, stride=WY), :] = vin[1]
    lane = lax.broadcasted_iota(jnp.int32, (32, 128), 1)

    def enter(k, c):
        for j in range(8):
            x = k * 8 + j
            VE[pl.ds(pl.multiple_of(x * WY + 8, 8), 32), :] = vv_ref[pl.ds(pl.multiple_of(x * 32, 32), 32), :]
        return c
    lax.fori_loop(0, 8, enter, 0)

    def faces(k, c):
        for j in range(4):
            x = k * 4 + j
            at = pl.ds(pl.multiple_of(x * 32, 32), 32)
            here = vv_ref[at, :]
            AL[at, :] = 0.25 * (here + VE[pl.ds(x * WY + 7, 32), :])
            AH[at, :] = 0.25 * (here + VE[pl.ds(x * WY + 9, 32), :])
            w = w_ref[at, :]
            AZ[at, :] = jnp.where(lane == 127, 0.0, 0.25 * (w + pltpu.roll(w, 127, 1)))
            AD[at, :] = jnp.where(lane == 0, 0.0, 0.25 * (w + pltpu.roll(w, 1, 1)))
        return c
    lax.fori_loop(0, 16, faces, 0)

    def face_x(k, c):
        for j in range(7):
            x = k * 7 + j + 1
            AX[pl.ds(pl.multiple_of(x * 32, 32), 32), :] = 0.25 * (u_ref[pl.ds(pl.multiple_of(x * 32 - 32, 32), 32), :] + u_ref[pl.ds(pl.multiple_of(x * 32, 32), 32), :])
        return c
    lax.fori_loop(0, 9, face_x, 0)

    for s, weight in enumerate((advect_step / 3.0, advect_step / 2.0, advect_step)):
        for q in range(2):
            src = E.at[2 * s + q]
            start = E.at[q]
            def step(k, carry, q=q, src=src, start=start, s=s, weight=weight):
                f, low = carry
                for j in range(UNROLL):
                    x = k * UNROLL + j
                    at = pl.ds(pl.multiple_of(x * 32, 32), 32)
                    p = pl.multiple_of((x + 1) * WY + 8, 8)
                    after = src[pl.ds(pl.multiple_of(p + WY, 8), 32), :]
                    high = AX[pl.ds(pl.multiple_of(x * 32 + 32, 32), 32), :] * (f + after)
                    fy = AH[at, :] * (f + src[pl.ds(p + 1, 32), :]) - AL[at, :] * (src[pl.ds(p - 1, 32), :] + f)
                    fz = AZ[at, :] * (f + pltpu.roll(f, 127, 1)) - AD[at, :] * (pltpu.roll(f, 1, 1) + f)
                    out = start[pl.ds(p, 32), :] - weight * ((high - low) + fy + fz)
                    if s < 2:
                        E[2 * s + 2 + q, pl.ds(p, 32), :] = out
                    else:
                        (to_ref, vo_ref)[q][at, :] = out
                    f, low = after, high
                return f, low
            f0 = src[pl.ds(plane(1), 32), :]
            lax.fori_loop(0, 64 // UNROLL, step, (f0, AX[pl.ds(0, 32), :] * f0))
            for c in moves[q]:
                c.wait_recv()
            if s < 2:
                dst, base, wide = E.at[2 * s + 2 + q], plane(1), WY
            else:
                dst, base, wide = (to_ref, vo_ref)[q], 0, 32
            n = 4 * s + 2 * q
            first, last = pl.ds(base, 32), pl.ds(base + 63 * wide, 32)
            dst[first, :] = dst[first, :] + weight * (AX[pl.ds(0, 32), :] * xin[n])
            dst[last, :] = dst[last, :] - weight * (AX[pl.ds(64 * 32, 32), :] * xin[n + 1])
            bottom, top = pl.ds(base, 64, stride=wide), pl.ds(base + 31, 64, stride=wide)
            dst[bottom, :] = dst[bottom, :] + weight * (AL[pl.ds(0, 64, stride=32), :] * yin[n])
            dst[top, :] = dst[top, :] - weight * (AH[pl.ds(31, 64, stride=32), :] * yin[n + 1])
            if s < 2:
                moves[q] = exchange(s + 1, q)
                sent += moves[q]
    for c in sent:
        c.wait_send()
    rest = pl.ds(8, 8 * (nx * ny - 1))
    whole = remote(recv_ref.at[rest, :], recv_ref.at[rest, :], a2a_send, a2a_recv, right)
    whole.wait_send()
    whole.wait_recv()


def step_call(mesh_shape, index, fields, droplets, counts, square, cells, moves):
    nx, ny = mesh_shape
    VM = pl.BlockSpec(memory_space=pltpu.VMEM)
    HB = pl.BlockSpec(memory_space=pltpu.HBM)
    bf16 = jnp.bfloat16
    DMA = pltpu.SemaphoreType.DMA
    plane = pltpu.VMEM((2048, 128), f32)
    block = pltpu.VMEM((1024, 128), f32)
    return pl.pallas_call(
        functools.partial(step_kernel, nx, ny),
        out_shape=(jax.ShapeDtypeStruct((2048, 128), f32), jax.ShapeDtypeStruct((2048, 128), f32), jax.ShapeDtypeStruct((1024, 256), f32)),
        in_specs=[pl.BlockSpec(memory_space=pltpu.SMEM)] + [HB] * 8 + [VM] * 4,
        out_specs=[VM] * 3,
        scratch_shapes=[plane] * 5 + [pltpu.VMEM((8, 128, 128), f32)] * 3 + [pltpu.VMEM((1024, 256), f32), pltpu.VMEM((16, 128), f32)] + [block] * 5
        + [pltpu.VMEM((N_CE * 8, 128), f32), pltpu.VMEM((1024, 512), bf16), pltpu.VMEM((8, 128), f32), pltpu.VMEM((8, 128), f32)]
        + [
            pltpu.VMEM((6, WX * WY, 128), f32), pltpu.VMEM((65 * 32, 128), f32), plane, plane, plane, plane,
            pltpu.VMEM((2, 32, 128), f32), pltpu.VMEM((64 * WY, 128), f32),
            pltpu.VMEM((12, 32, 128), f32), pltpu.VMEM((12, 64, 128), f32), pltpu.VMEM((12, 64, 128), f32),
            pltpu.VMEM((2, 64, 128), f32), pltpu.VMEM((2, 64, 128), f32), pltpu.VMEM((1024, 512), bf16),
            DMA, DMA, DMA((12,)), DMA((12,)), DMA((12,)), DMA((12,)), DMA((4,)), DMA((4,)), pltpu.SemaphoreType.REGULAR, DMA((8,)),
        ],
        compiler_params=pltpu.CompilerParams(vmem_limit_bytes=50 * 2**20, collective_id=0, has_side_effects=True),
        cost_estimate=pl.CostEstimate(flops=5_000_000_000, bytes_accessed=8_000_000, transcendentals=0),
        name="step",
    )(index, *fields, *droplets, counts, square, cells, moves)


def triangle(n):
    return lax.broadcasted_iota(jnp.int32, (n, n), 0) < lax.broadcasted_iota(jnp.int32, (n, n), 1)


def compact_kernel(recv_ref, ti_ref, vi_ref, to_ref, vo_ref, ro_ref, mo_ref, X, sems):
    passing = [pltpu.make_async_copy(ti_ref, to_ref, sems.at[0]), pltpu.make_async_copy(vi_ref, vo_ref, sems.at[1])]
    for c in passing:
        c.start()
    rows = []
    for g in range(8):
        rows.append(recv_ref[pl.ds(g * 128, 128), 128:256].T[0:1])
    first = jnp.concatenate(rows, axis=0)
    taken = jnp.where(first > 0.0, 1.0, 0.0)
    within = jnp.dot(taken.astype(jnp.bfloat16), jnp.where(triangle(128), 1.0, 0.0).astype(jnp.bfloat16), preferred_element_type=f32)
    total = jnp.sum(taken, axis=1, keepdims=True)
    pos = []
    before = jnp.zeros((1, 1), f32)
    for g in range(8):
        pos.append(jnp.where(first[g:g + 1] > 0.0, within[g:g + 1] + before, -1.0))
        before = before + total[g:g + 1]
    pos = jnp.concatenate(pos, axis=1).astype(jnp.int32)
    for g in range(8):
        at = pl.ds(g * 128, 128)
        for k, part in enumerate(split2(recv_ref[at, :])):
            X[at, k * 256:k * 256 + 256] = part
    for n in range(4):
        ids = lax.broadcasted_iota(jnp.int32, (128, 1024), 0) + n * 128
        hot = jnp.where(ids == pos, 1.0, 0.0).astype(jnp.bfloat16)
        d = jnp.dot(hot, X[...], preferred_element_type=f32)
        d = d[:, 0:256] + d[:, 256:512]
        ro_ref[pl.ds(n * 128, 128), :] = d[:, 0:128]
        mo_ref[pl.ds(n * 128, 128), :] = d[:, 128:256]
    for c in passing:
        c.wait()


def compacted(recv, t, v):
    VM = pl.BlockSpec(memory_space=pltpu.VMEM)
    field = jax.ShapeDtypeStruct(t.shape, f32)
    drops = jax.ShapeDtypeStruct((512, 128), f32)
    return pl.pallas_call(
        compact_kernel,
        out_shape=(field, field, drops, drops),
        in_specs=[VM] * 3, out_specs=[pl.BlockSpec(memory_space=pltpu.HBM)] * 2 + [VM] * 2,
        scratch_shapes=[pltpu.VMEM((1024, 512), jnp.bfloat16), pltpu.SemaphoreType.DMA((2,))],
        compiler_params=pltpu.CompilerParams(vmem_limit_bytes=12 * 2**20),
        cost_estimate=pl.CostEstimate(flops=800_000_000, bytes_accessed=2_000_000, transcendentals=0),
        name="compact",
    )(recv, t, v)


def body(
    shape,
    tprime,
    vapor,
    wind_u,
    wind_v,
    wind_w,
    radius,
    min_radius,
    multiplicity,
    drop_counts,
    cell_index,
    move_list,
):
    home = radius.shape[0]
    columns = tprime.shape[0] * tprime.shape[1]
    levels = tprime.shape[2]
    flat = [pltpu.with_memory_space_constraint(a.reshape(columns, levels), pltpu.HBM) for a in (tprime, vapor, wind_u, wind_v, wind_w)]
    square = (8, home // 8)
    cells = cell_index.reshape(square)
    temperature, humidity, recv = step_call(
        shape,
        cell_index,
        flat,
        [pltpu.with_memory_space_constraint(a.reshape(8, home // 8, a.shape[1]), pltpu.HBM) for a in (radius, min_radius, multiplicity)],
        drop_counts.reshape(square),
        cells,
        cell_index.reshape(1, home),
        move_list.reshape(1, home),
    )
    temperature, humidity, radius_out, multiplicity_out = compacted(recv, temperature, humidity)
    return (
        temperature.reshape(tprime.shape),
        humidity.reshape(vapor.shape),
        radius_out,
        multiplicity_out,
    )


def solution(mesh):
    placed = (
        P("gx", "gy", None),
        P("gx", "gy", None),
        P("gx", "gy", None),
        P("gx", "gy", None),
        P("gx", "gy", None),
        P(("gx", "gy"), None),
        P(("gx", "gy"), None),
        P(("gx", "gy"), None),
        P(("gx", "gy")),
        P(("gx", "gy")),
        P(("gx", "gy")),
    )
    return jax.shard_map(
        functools.partial(body, (mesh.shape["gx"], mesh.shape["gy"])),
        mesh=mesh,
        in_specs=placed,
        out_specs=(
            P("gx", "gy", None),
            P("gx", "gy", None),
            P(("gx", "gy"), None),
            P(("gx", "gy"), None),
        ),
        check_vma=False,
    )
```

```python
import functools

import jax
import jax.numpy as jnp
from jax import lax
from jax.experimental import pallas as pl
from jax.experimental.pallas import tpu as pltpu
from jax.sharding import PartitionSpec as P

MESH = pl.DeviceIdType.MESH
f32 = jnp.float32
SUBSTEPS = 6
WX, WY = 66, 48
UNROLL = 8

clausius = 0.07
growth = 200.0 / 3.0
solute = 0.05
condense = 5e-07
latent = 10.0
collect = 1e-07
time_step = 2.0
advect_step = 0.6


def batcher(n):
    out = []
    p = 1
    while p < n:
        k = p
        while k >= 1:
            for j in range(k % p, n - k, 2 * k):
                for i in range(min(k, n - j - k)):
                    if (i + j) // (2 * p) == (i + j + k) // (2 * p):
                        out.append((i + j, i + j + k))
            k //= 2
        p *= 2
    return out

NET16 = batcher(16)

def halves(top, n=16):
    out = []
    d = top
    while d >= 1:
        for i in range(n):
            if not i & d:
                out.append((i, i + d))
        d //= 2
    return out

def make_passes():
    passes = []
    up, down = list(range(16)), list(range(15, -1, -1))
    passes.append((4, [(lambda t: t * 32, up, up, NET16), (lambda t: t * 32, [16 + o for o in up], [16 + o for o in down], NET16)]))
    for level in (32, 64, 128):
        step = level // 16
        if level == 128:
            passes.append((step, [(lambda t: t, [step * o for o in up], [step * o for o in up], halves(8))]))
        else:
            per = step
            passes.append((128 // level, [(lambda t, b=b, level=level: t * level + b, [step * o for o in up], [step * o for o in up], halves(8)) for b in range(per)]))
        ces = halves(step // 2)
        if level == 128:
            passes.append((8, [(lambda t: t * 16, up, up, ces)]))
        else:
            sets = []
            for s in range(2 * level // 16):
                loads = [16 * s + o for o in up]
                stores = loads if s * 16 < level else [level + 2 * level - 1 - o for o in loads]
                sets.append((lambda t, level=level: t * 2 * level, loads, stores, ces))
            passes.append((128 // (2 * level), sets))
    return passes

PASSES = make_passes()
N_CE = sum(trips * sum(len(s[3]) for s in sets) for trips, sets in PASSES)

def moves(sets):
    return any(set(s[1]) != set(s[2]) for s in sets)

def row(ref, d):
    if isinstance(d, int):
        return ref.at[pl.ds(d * 8, 8), :]
    return ref.at[pl.ds(pl.multiple_of(d * 8, 8), 8), :]

def loop(trips, body):
    if trips == 1:
        body(0)
    else:
        def step(t, c):
            body(t)
            return c
        lax.fori_loop(0, trips, step, 0)

def sort_blocks(keys, vals, marks):
    at = 0
    side = 0
    for trips, sets in PASSES:
        count = sum(len(s[3]) for s in sets)
        key, val = keys[side], vals[side]
        if moves(sets):
            side = 1 - side
        key_to, val_to = keys[side], vals[side]
        def body(t, sets=sets, at=at, count=count, key=key, val=val, key_to=key_to, val_to=val_to):
            m = at + t * count
            for base, loads, stores, ces in sets:
                b = base(t)
                ks = [row(key, b + o)[...] for o in loads]
                vs = [row(val, b + o)[...] for o in loads]
                for i, j in ces:
                    c = ks[i] > ks[j]
                    row(marks, m)[...] = jnp.where(c, 1.0, 0.0)
                    m = m + 1
                    ks[i], ks[j] = jnp.minimum(ks[i], ks[j]), jnp.maximum(ks[i], ks[j])
                    vs[i], vs[j] = jnp.where(c, vs[j], vs[i]), jnp.where(c, vs[i], vs[j])
                for o, k, v in zip(stores, ks, vs):
                    row(key_to, b + o)[...] = k
                    row(val_to, b + o)[...] = v
        loop(trips, body)
        at += trips * count

def unsort_blocks(firsts, seconds, marks):
    at = N_CE
    side = 0
    for trips, sets in reversed(PASSES):
        count = sum(len(s[3]) for s in sets)
        at -= trips * count
        xa, xb = firsts[side], seconds[side]
        if moves(sets):
            side = 1 - side
        xa_to, xb_to = firsts[side], seconds[side]
        def body(t, sets=sets, at=at, count=count, xa=xa, xb=xb, xa_to=xa_to, xb_to=xb_to):
            m = at + t * count
            for base, loads, stores, ces in sets:
                b = base(t)
                xs = [row(xa, b + o)[...] for o in stores]
                ys = [row(xb, b + o)[...] for o in stores]
                for q in reversed(range(len(ces))):
                    i, j = ces[q]
                    c = row(marks, m + q)[...] > 0.5
                    xs[i], xs[j] = jnp.where(c, xs[j], xs[i]), jnp.where(c, xs[i], xs[j])
                    ys[i], ys[j] = jnp.where(c, ys[j], ys[i]), jnp.where(c, ys[i], ys[j])
                m = m + len(ces)
                for o, x, y in zip(loads, xs, ys):
                    row(xa_to, b + o)[...] = x
                    row(xb_to, b + o)[...] = y
        loop(trips, body)

def gather_cells(index, t_ref, v_ref, cell_ref, ct, cv, T, V):
    def rows(k, c):
        for j in range(16):
            b = k * 16 + j
            at = lax.shift_right_logical(index[b], 7)
            T[pl.ds(b, 1), :] = t_ref[pl.ds(at, 1), :]
            V[pl.ds(b, 1), :] = v_ref[pl.ds(at, 1), :]
        return c
    lax.fori_loop(0, 64, rows, 0)
    level = lax.rem(cell_ref[...], 128)
    depth = lax.broadcasted_iota(jnp.int32, (128, 128), 0)
    for g in range(8):
        here = depth == level[g:g + 1]
        for staged, cell in ((T, ct), (V, cv)):
            picked = jnp.where(here, staged[pl.ds(g * 128, 128), :].T, 0.0)
            cell[pl.ds(g, 1), :] = jnp.sum(picked, axis=0, keepdims=True)


def enter_blocks(rad_ref, flo_ref, mul_ref, R, F, M):
    def enter(g, c):
        to = pl.ds(g, 128, stride=8)
        R[to, :] = rad_ref[g].T
        F[to, :] = flo_ref[g].T
        M[to, :] = mul_ref[g].T
        return c
    lax.fori_loop(0, 8, enter, 0)


def condense_blocks(cnt_ref, heat_ref, R, S, C, F, M, ct_ref, cv_ref):
    counts = cnt_ref[...]
    zero = jnp.zeros((8, 128), jnp.float32)
    U = 32

    def init(t, w):
        for u in range(U):
            d = t * U + u
            r = row(R, d)[...]
            f = row(F, d)[...]
            m = jnp.where(counts > d, row(M, d)[...], 0.0)
            r2 = r * r
            f2 = f * f
            row(M, d)[...] = m
            row(R, d)[...] = r2
            row(S, d)[...] = lax.rsqrt(r2)
            row(F, d)[...] = f2
            row(C, d)[...] = (growth * solute) * f2 * f
            w = w + m * (r2 * r)
        return w
    weight = lax.fori_loop(0, 128 // U, init, zero)
    temp = ct_ref[...]
    wet = cv_ref[...]
    for _ in range(SUBSTEPS):
        sat = growth * ((1.0 + wet) * jnp.exp(-clausius * temp) - 1.0)
        def sub(t, w):
            for u in range(U):
                d = t * U + u
                r2 = row(R, d)[...]
                rs = row(S, d)[...]
                g = jnp.maximum(r2 + (sat + row(C, d)[...] * (rs * rs * rs)), row(F, d)[...])
                ns = lax.rsqrt(g)
                row(R, d)[...] = g
                row(S, d)[...] = ns
                w = w + row(M, d)[...] * (g * (g * ns))
            return w
        after = lax.fori_loop(0, 128 // U, sub, zero)
        condensed = after - weight
        weight = after
        wet = wet - condense * condensed
        temp = temp + latent * condense * condensed
    heat_ref[0:8, :] = temp - ct_ref[...]
    heat_ref[8:16, :] = wet - cv_ref[...]


def collect_blocks(R, S, C, F, M, marks, X):
    zero = jnp.zeros((8, 128), jnp.float32)
    U = 16

    def radii(t, c):
        for u in range(U):
            d = t * U + u
            row(R, d)[...] = row(R, d)[...] * row(S, d)[...]
        return c
    lax.fori_loop(0, 128 // U, radii, 0)
    sort_blocks((R, S), (M, C), marks)

    def both(t, carry):
        a0, a1, a3, a4, b0, b1, b3, b4 = carry
        for u in range(U):
            d = t * U + u
            r = row(R, d)[...]
            m = row(M, d)[...]
            r2 = r * r
            r3 = r2 * r
            r4 = r2 * r2
            gain = r4 * a0 + 2.0 * (r3 * a1 - r * a3) - a4
            w = m * r3
            a0 = a0 + w
            a1 = a1 + w * r
            a3 = a3 + w * r3
            a4 = a4 + w * r4
            grown = r3 + (time_step * collect) * gain
            row(S, d)[...] = jnp.where(m > 0.0, jnp.exp(jnp.log(grown) * (1.0 / 3.0)), 0.0)
            d = 127 - d
            r = row(R, d)[...]
            m = row(M, d)[...]
            r2 = r * r
            r3 = r2 * r
            r4 = r2 * r2
            loss = b4 + 2.0 * (r * b3 - r3 * b1) - r4 * b0
            b0 = b0 + m
            b1 = b1 + m * r
            b3 = b3 + m * r3
            b4 = b4 + m * r4
            row(C, d)[...] = m * jnp.exp((-time_step * collect) * loss)
        return a0, a1, a3, a4, b0, b1, b3, b4
    lax.fori_loop(0, 128 // U, both, (zero,) * 8)
    unsort_blocks((S, R), (C, F), marks)

    def leave(g, c):
        at = pl.ds(pl.multiple_of(g * 128, 128), 128)
        frm = pl.ds(g, 128, stride=8)
        for q, ref in enumerate((S, C)):
            for k, part in enumerate(split2(ref[frm, :].T)):
                X[at, k * 256 + q * 128:k * 256 + q * 128 + 128] = part
        return c
    lax.fori_loop(0, 8, leave, 0)


def mod(a, n):
    return lax.rem(a + n, n)


def split2(x):
    hi = x.astype(jnp.bfloat16)
    lo = (x - hi.astype(f32)).astype(jnp.bfloat16)
    return hi, lo


def row_moves(nx, ny, ix, iy, k, send_ref, recv_ref, s, r):
    px = mod(ix + k, nx)
    me = ix * ny + iy

    def body(i, c):
        py = mod(iy + i, ny)
        pltpu.make_async_remote_copy(
            src_ref=send_ref.at[pl.ds(pl.multiple_of((px * ny + py) * 8, 8), 8), :],
            dst_ref=recv_ref.at[pl.ds(pl.multiple_of(me * 8, 8), 8), :],
            send_sem=s, recv_sem=r, device_id=(px, py), device_id_type=MESH).start()
        return c
    lax.fori_loop(1 if k == 0 else 0, ny, body, 0)


def step_kernel(nx, ny, index, t_hbm, v_hbm, u_hbm, vv_hbm, w_hbm, rad_hbm, flo_hbm, mul_hbm, cnt_ref, square_ref, cell_ref, move_ref,
                to_ref, vo_ref, recv_ref,
                t_ref, v_ref, u_ref, vv_ref, w_ref, rad_ref, flo_ref, mul_ref, send_ref, heat_ref, R, S, C, F, M, marks, X, ct_ref, cv_ref,
                E, AX, AL, AH, AZ, AD, UE, VE, xin, yout, yin, vout, vin, W,
                a2a_send, a2a_recv, xs, xr, ys, yr, ws, wr, rows, loads):
    ix, iy = lax.axis_index("gx"), lax.axis_index("gy")
    me = ix * ny + iy
    right, left = (mod(ix + 1, nx), iy), (mod(ix - 1, nx), iy)
    upper, lower = (ix, mod(iy + 1, ny)), (ix, mod(iy - 1, ny))

    fetched = []
    for n, (src, dst) in enumerate(((rad_hbm, rad_ref), (flo_hbm, flo_ref), (mul_hbm, mul_ref), (t_hbm, t_ref), (v_hbm, v_ref), (vv_hbm, vv_ref), (u_hbm, u_ref), (w_hbm, w_ref))):
        fetched.append(pltpu.make_async_copy(src, dst, loads.at[n]))
        fetched[-1].start()
    barrier = pltpu.get_barrier_semaphore()
    for i in range(1, ny):
        pl.semaphore_signal(barrier, inc=1, device_id=(ix, mod(iy + i, ny)), device_id_type=MESH)
    for i in range(1, nx):
        pl.semaphore_signal(barrier, inc=1, device_id=(mod(ix + i, nx), iy), device_id_type=MESH)

    def remote(src, dst, s, r, to):
        return pltpu.make_async_remote_copy(src_ref=src, dst_ref=dst, send_sem=s, recv_sem=r, device_id=to, device_id_type=MESH)

    for n in (0, 1, 2):
        fetched[n].wait()
    enter_blocks(rad_ref, flo_ref, mul_ref, R, F, M)
    fetched[3].wait()
    fetched[4].wait()
    gather_cells(index, t_ref, v_ref, square_ref, ct_ref, cv_ref, S, C)
    condense_blocks(cnt_ref, heat_ref, R, S, C, F, M, ct_ref, cv_ref)
    fetched[5].wait()
    fetched[6].wait()
    vout[0] = vv_ref[pl.ds(31, 64, stride=32), :]
    vout[1] = vv_ref[pl.ds(0, 64, stride=32), :]
    for e in range(6):
        for at in (WY + 7, WY + 40):
            E[e, pl.ds(at, 64, stride=WY), :] = jnp.zeros((64, 128), f32)
        E[e, pl.ds(65 * WY + 8, 32), :] = jnp.zeros((32, 128), f32)
    pl.semaphore_wait(barrier, nx + ny - 2)
    for i in range(1, ny):
        pl.semaphore_signal(rows, inc=1, device_id=(ix, mod(iy + i, ny)), device_id_type=MESH)
    winds = [
        remote(u_ref.at[pl.ds(63 * 32, 32), :], UE.at[0], ws.at[0], wr.at[0], right),
        remote(u_ref.at[pl.ds(0, 32), :], UE.at[1], ws.at[1], wr.at[1], left),
        remote(vout.at[0], vin.at[0], ws.at[2], wr.at[2], upper),
        remote(vout.at[1], vin.at[1], ws.at[3], wr.at[3], lower),
    ]
    for c in winds:
        c.start()
    def plane(x):
        return x * WY + 8

    def exchange(s, q):
        n = 4 * s + 2 * q
        e = E.at[2 * s + q]
        yout[n] = E[2 * s + q, pl.ds(plane(1) + 31, 64, stride=WY), :]
        yout[n + 1] = E[2 * s + q, pl.ds(plane(1), 64, stride=WY), :]
        moves = [
            remote(yout.at[n], yin.at[n], ys.at[n], yr.at[n], upper),
            remote(yout.at[n + 1], yin.at[n + 1], ys.at[n + 1], yr.at[n + 1], lower),
            remote(e.at[pl.ds(plane(64), 32), :], xin.at[n], xs.at[n], xr.at[n], right),
            remote(e.at[pl.ds(plane(1), 32), :], xin.at[n + 1], xs.at[n + 1], xr.at[n + 1], left),
        ]
        for c in moves:
            c.start()
        return moves

    collect_blocks(R, S, C, F, M, marks, X)
    moves_to = move_ref[...]

    def place(k):
        at = pl.multiple_of(mod(ix + k, nx) * (ny * 8), ny * 8)
        ids = lax.broadcasted_iota(jnp.int32, (ny * 8, 1024), 0) + at
        hot = jnp.where(ids == moves_to, 1.0, 0.0).astype(jnp.bfloat16)
        d = jnp.dot(hot, X[...], preferred_element_type=f32)
        send_ref[pl.ds(at, ny * 8), :] = d[:, 0:256] + d[:, 256:512]

    def send_row(k):
        row_moves(nx, ny, ix, iy, k, send_ref, recv_ref, a2a_send, a2a_recv)

    order = sorted(range(nx), key=lambda k: -min(k, nx - k))
    place(order[0])
    pl.semaphore_wait(rows, ny - 1)
    send_row(order[0])
    for n, k in enumerate(order[1:]):
        place(k)
        if n < 3:
            send_row(k)
    mine = pl.ds(pl.multiple_of(me * 8, 8), 8)
    recv_ref[mine, :] = send_ref[mine, :]

    zed = lax.rem(square_ref[...], 128).astype(f32).T.astype(jnp.int32)
    heat = heat_ref[...].T
    lanes = lax.broadcasted_iota(jnp.int32, (128, 128), 1)
    for g in range(8):
        level = lanes == zed[:, g:g + 1]
        at = pl.ds(g * 128, 128)
        for q in range(2):
            h = jnp.where(level, heat[:, q * 8 + g:q * 8 + g + 1], 0.0)
            hi, lo = split2(h)
            W[at, q * 128:q * 128 + 128] = hi
            W[at, 256 + q * 128:256 + q * 128 + 128] = lo
    cells = lax.shift_right_logical(cell_ref[...], 7)

    def scatter(k, c):
        at = pl.multiple_of(k * 128, 128)
        ids = lax.broadcasted_iota(jnp.int32, (128, 1024), 0) + at
        hot = jnp.where(ids == cells, 1.0, 0.0).astype(jnp.bfloat16)
        d = jnp.dot(hot, W[...], preferred_element_type=f32)
        for q, ref in ((0, t_ref), (1, v_ref)):
            add = d[:, q * 128:q * 128 + 128] + d[:, 256 + q * 128:256 + q * 128 + 128]
            new = ref[pl.ds(at, 128), :] + add
            for j in range(4):
                E[q, pl.ds(pl.multiple_of((k * 4 + j + 1) * WY + 8, 8), 32), :] = new[j * 32:j * 32 + 32]
        return c
    lax.fori_loop(0, 16, scatter, 0)

    moves = [exchange(0, 0), exchange(0, 1)]
    sent = [*winds, *moves[0], *moves[1]]
    send_row(order[4])
    send_row(order[5])

    fetched[7].wait()
    for c in winds:
        c.wait_recv()

    AX[pl.ds(0, 32), :] = 0.25 * (UE[0] + u_ref[pl.ds(0, 32), :])
    AX[pl.ds(64 * 32, 32), :] = 0.25 * (u_ref[pl.ds(63 * 32, 32), :] + UE[1])
    VE[pl.ds(7, 64, stride=WY), :] = vin[0]
    VE[pl.ds(40, 64, stride=WY), :] = vin[1]
    lane = lax.broadcasted_iota(jnp.int32, (32, 128), 1)

    def enter(k, c):
        for j in range(8):
            x = k * 8 + j
            VE[pl.ds(pl.multiple_of(x * WY + 8, 8), 32), :] = vv_ref[pl.ds(pl.multiple_of(x * 32, 32), 32), :]
        return c
    lax.fori_loop(0, 8, enter, 0)

    def faces(k, c):
        for j in range(4):
            x = k * 4 + j
            at = pl.ds(pl.multiple_of(x * 32, 32), 32)
            here = vv_ref[at, :]
            AL[at, :] = 0.25 * (here + VE[pl.ds(x * WY + 7, 32), :])
            AH[at, :] = 0.25 * (here + VE[pl.ds(x * WY + 9, 32), :])
            w = w_ref[at, :]
            AZ[at, :] = jnp.where(lane == 127, 0.0, 0.25 * (w + pltpu.roll(w, 127, 1)))
            AD[at, :] = jnp.where(lane == 0, 0.0, 0.25 * (w + pltpu.roll(w, 1, 1)))
        return c
    lax.fori_loop(0, 16, faces, 0)

    def face_x(k, c):
        for j in range(7):
            x = k * 7 + j + 1
            AX[pl.ds(pl.multiple_of(x * 32, 32), 32), :] = 0.25 * (u_ref[pl.ds(pl.multiple_of(x * 32 - 32, 32), 32), :] + u_ref[pl.ds(pl.multiple_of(x * 32, 32), 32), :])
        return c
    lax.fori_loop(0, 9, face_x, 0)

    for s, weight in enumerate((advect_step / 3.0, advect_step / 2.0, advect_step)):
        for q in range(2):
            src = E.at[2 * s + q]
            start = E.at[q]
            def step(k, carry, q=q, src=src, start=start, s=s, weight=weight):
                f, low = carry
                for j in range(UNROLL):
                    x = k * UNROLL + j
                    at = pl.ds(pl.multiple_of(x * 32, 32), 32)
                    p = pl.multiple_of((x + 1) * WY + 8, 8)
                    after = src[pl.ds(pl.multiple_of(p + WY, 8), 32), :]
                    high = AX[pl.ds(pl.multiple_of(x * 32 + 32, 32), 32), :] * (f + after)
                    fy = AH[at, :] * (f + src[pl.ds(p + 1, 32), :]) - AL[at, :] * (src[pl.ds(p - 1, 32), :] + f)
                    fz = AZ[at, :] * (f + pltpu.roll(f, 127, 1)) - AD[at, :] * (pltpu.roll(f, 1, 1) + f)
                    out = start[pl.ds(p, 32), :] - weight * ((high - low) + fy + fz)
                    if s < 2:
                        E[2 * s + 2 + q, pl.ds(p, 32), :] = out
                    else:
                        (to_ref, vo_ref)[q][at, :] = out
                    f, low = after, high
                return f, low
            f0 = src[pl.ds(plane(1), 32), :]
            lax.fori_loop(0, 64 // UNROLL, step, (f0, AX[pl.ds(0, 32), :] * f0))
            if s == 0:
                send_row(order[6 + q])
            for c in moves[q]:
                c.wait_recv()
            if s < 2:
                dst, base, wide = E.at[2 * s + 2 + q], plane(1), WY
            else:
                dst, base, wide = (to_ref, vo_ref)[q], 0, 32
            n = 4 * s + 2 * q
            first, last = pl.ds(base, 32), pl.ds(base + 63 * wide, 32)
            dst[first, :] = dst[first, :] + weight * (AX[pl.ds(0, 32), :] * xin[n])
            dst[last, :] = dst[last, :] - weight * (AX[pl.ds(64 * 32, 32), :] * xin[n + 1])
            bottom, top = pl.ds(base, 64, stride=wide), pl.ds(base + 31, 64, stride=wide)
            dst[bottom, :] = dst[bottom, :] + weight * (AL[pl.ds(0, 64, stride=32), :] * yin[n])
            dst[top, :] = dst[top, :] - weight * (AH[pl.ds(31, 64, stride=32), :] * yin[n + 1])
            if s < 2:
                moves[q] = exchange(s + 1, q)
                sent += moves[q]
    for c in sent:
        c.wait_send()
    rest = pl.ds(8, 8 * (nx * ny - 1))
    whole = remote(recv_ref.at[rest, :], recv_ref.at[rest, :], a2a_send, a2a_recv, right)
    whole.wait_send()
    whole.wait_recv()


def step_call(mesh_shape, index, fields, droplets, counts, square, cells, moves):
    nx, ny = mesh_shape
    VM = pl.BlockSpec(memory_space=pltpu.VMEM)
    HB = pl.BlockSpec(memory_space=pltpu.HBM)
    bf16 = jnp.bfloat16
    DMA = pltpu.SemaphoreType.DMA
    plane = pltpu.VMEM((2048, 128), f32)
    block = pltpu.VMEM((1024, 128), f32)
    return pl.pallas_call(
        functools.partial(step_kernel, nx, ny),
        out_shape=(jax.ShapeDtypeStruct((2048, 128), f32), jax.ShapeDtypeStruct((2048, 128), f32), jax.ShapeDtypeStruct((1024, 256), f32)),
        in_specs=[pl.BlockSpec(memory_space=pltpu.SMEM)] + [HB] * 8 + [VM] * 4,
        out_specs=[VM] * 3,
        scratch_shapes=[plane] * 5 + [pltpu.VMEM((8, 128, 128), f32)] * 3 + [pltpu.VMEM((1024, 256), f32), pltpu.VMEM((16, 128), f32)] + [block] * 5
        + [pltpu.VMEM((N_CE * 8, 128), f32), pltpu.VMEM((1024, 512), bf16), pltpu.VMEM((8, 128), f32), pltpu.VMEM((8, 128), f32)]
        + [
            pltpu.VMEM((6, WX * WY, 128), f32), pltpu.VMEM((65 * 32, 128), f32), plane, plane, plane, plane,
            pltpu.VMEM((2, 32, 128), f32), pltpu.VMEM((64 * WY, 128), f32),
            pltpu.VMEM((12, 32, 128), f32), pltpu.VMEM((12, 64, 128), f32), pltpu.VMEM((12, 64, 128), f32),
            pltpu.VMEM((2, 64, 128), f32), pltpu.VMEM((2, 64, 128), f32), pltpu.VMEM((1024, 512), bf16),
            DMA, DMA, DMA((12,)), DMA((12,)), DMA((12,)), DMA((12,)), DMA((4,)), DMA((4,)), pltpu.SemaphoreType.REGULAR, DMA((8,)),
        ],
        compiler_params=pltpu.CompilerParams(vmem_limit_bytes=50 * 2**20, collective_id=0, has_side_effects=True),
        cost_estimate=pl.CostEstimate(flops=5_000_000_000, bytes_accessed=8_000_000, transcendentals=0),
        name="step",
    )(index, *fields, *droplets, counts, square, cells, moves)


def triangle(n):
    return lax.broadcasted_iota(jnp.int32, (n, n), 0) < lax.broadcasted_iota(jnp.int32, (n, n), 1)


def compact_kernel(recv_ref, ti_ref, vi_ref, to_ref, vo_ref, ro_ref, mo_ref, X, sems):
    passing = [pltpu.make_async_copy(ti_ref, to_ref, sems.at[0]), pltpu.make_async_copy(vi_ref, vo_ref, sems.at[1])]
    for c in passing:
        c.start()
    rows = []
    for g in range(8):
        rows.append(recv_ref[pl.ds(g * 128, 128), 128:256].T[0:1])
    first = jnp.concatenate(rows, axis=0)
    taken = jnp.where(first > 0.0, 1.0, 0.0)
    within = jnp.dot(taken.astype(jnp.bfloat16), jnp.where(triangle(128), 1.0, 0.0).astype(jnp.bfloat16), preferred_element_type=f32)
    total = jnp.sum(taken, axis=1, keepdims=True)
    pos = []
    before = jnp.zeros((1, 1), f32)
    for g in range(8):
        pos.append(jnp.where(first[g:g + 1] > 0.0, within[g:g + 1] + before, -1.0))
        before = before + total[g:g + 1]
    pos = jnp.concatenate(pos, axis=1).astype(jnp.int32)
    for g in range(8):
        at = pl.ds(g * 128, 128)
        for k, part in enumerate(split2(recv_ref[at, :])):
            X[at, k * 256:k * 256 + 256] = part
    for n in range(4):
        ids = lax.broadcasted_iota(jnp.int32, (128, 1024), 0) + n * 128
        hot = jnp.where(ids == pos, 1.0, 0.0).astype(jnp.bfloat16)
        d = jnp.dot(hot, X[...], preferred_element_type=f32)
        d = d[:, 0:256] + d[:, 256:512]
        ro_ref[pl.ds(n * 128, 128), :] = d[:, 0:128]
        mo_ref[pl.ds(n * 128, 128), :] = d[:, 128:256]
    for c in passing:
        c.wait()


def compacted(recv, t, v):
    VM = pl.BlockSpec(memory_space=pltpu.VMEM)
    field = jax.ShapeDtypeStruct(t.shape, f32)
    drops = jax.ShapeDtypeStruct((512, 128), f32)
    return pl.pallas_call(
        compact_kernel,
        out_shape=(field, field, drops, drops),
        in_specs=[VM] * 3, out_specs=[pl.BlockSpec(memory_space=pltpu.HBM)] * 2 + [VM] * 2,
        scratch_shapes=[pltpu.VMEM((1024, 512), jnp.bfloat16), pltpu.SemaphoreType.DMA((2,))],
        compiler_params=pltpu.CompilerParams(vmem_limit_bytes=12 * 2**20),
        cost_estimate=pl.CostEstimate(flops=800_000_000, bytes_accessed=2_000_000, transcendentals=0),
        name="compact",
    )(recv, t, v)


def body(
    shape,
    tprime,
    vapor,
    wind_u,
    wind_v,
    wind_w,
    radius,
    min_radius,
    multiplicity,
    drop_counts,
    cell_index,
    move_list,
):
    home = radius.shape[0]
    columns = tprime.shape[0] * tprime.shape[1]
    levels = tprime.shape[2]
    flat = [pltpu.with_memory_space_constraint(a.reshape(columns, levels), pltpu.HBM) for a in (tprime, vapor, wind_u, wind_v, wind_w)]
    square = (8, home // 8)
    cells = cell_index.reshape(square)
    temperature, humidity, recv = step_call(
        shape,
        cell_index,
        flat,
        [pltpu.with_memory_space_constraint(a.reshape(8, home // 8, a.shape[1]), pltpu.HBM) for a in (radius, min_radius, multiplicity)],
        drop_counts.reshape(square),
        cells,
        cell_index.reshape(1, home),
        move_list.reshape(1, home),
    )
    temperature, humidity, radius_out, multiplicity_out = compacted(recv, temperature, humidity)
    return (
        temperature.reshape(tprime.shape),
        humidity.reshape(vapor.shape),
        radius_out,
        multiplicity_out,
    )


def solution(mesh):
    placed = (
        P("gx", "gy", None),
        P("gx", "gy", None),
        P("gx", "gy", None),
        P("gx", "gy", None),
        P("gx", "gy", None),
        P(("gx", "gy"), None),
        P(("gx", "gy"), None),
        P(("gx", "gy"), None),
        P(("gx", "gy")),
        P(("gx", "gy")),
        P(("gx", "gy")),
    )
    return jax.shard_map(
        functools.partial(body, (mesh.shape["gx"], mesh.shape["gy"])),
        mesh=mesh,
        in_specs=placed,
        out_specs=(
            P("gx", "gy", None),
            P("gx", "gy", None),
            P(("gx", "gy"), None),
            P(("gx", "gy"), None),
        ),
        check_vma=False,
    )
```

```python
import functools

import jax
import jax.numpy as jnp
from jax import lax
from jax.experimental import pallas as pl
from jax.experimental.pallas import tpu as pltpu
from jax.sharding import PartitionSpec as P

MESH = pl.DeviceIdType.MESH
f32 = jnp.float32
SUBSTEPS = 6
WX, WY = 66, 48
UNROLL = 16

clausius = 0.07
growth = 200.0 / 3.0
solute = 0.05
condense = 5e-07
latent = 10.0
collect = 1e-07
time_step = 2.0
advect_step = 0.6


def batcher(n):
    out = []
    p = 1
    while p < n:
        k = p
        while k >= 1:
            for j in range(k % p, n - k, 2 * k):
                for i in range(min(k, n - j - k)):
                    if (i + j) // (2 * p) == (i + j + k) // (2 * p):
                        out.append((i + j, i + j + k))
            k //= 2
        p *= 2
    return out

NET16 = batcher(16)

def halves(top, n=16):
    out = []
    d = top
    while d >= 1:
        for i in range(n):
            if not i & d:
                out.append((i, i + d))
        d //= 2
    return out

def make_passes():
    passes = []
    up, down = list(range(16)), list(range(15, -1, -1))
    passes.append((4, [(lambda t: t * 32, up, up, NET16), (lambda t: t * 32, [16 + o for o in up], [16 + o for o in down], NET16)]))
    for level in (32, 64, 128):
        step = level // 16
        if level == 128:
            passes.append((step, [(lambda t: t, [step * o for o in up], [step * o for o in up], halves(8))]))
        else:
            per = step
            passes.append((128 // level, [(lambda t, b=b, level=level: t * level + b, [step * o for o in up], [step * o for o in up], halves(8)) for b in range(per)]))
        ces = halves(step // 2)
        if level == 128:
            passes.append((8, [(lambda t: t * 16, up, up, ces)]))
        else:
            sets = []
            for s in range(2 * level // 16):
                loads = [16 * s + o for o in up]
                stores = loads if s * 16 < level else [level + 2 * level - 1 - o for o in loads]
                sets.append((lambda t, level=level: t * 2 * level, loads, stores, ces))
            passes.append((128 // (2 * level), sets))
    return passes

PASSES = make_passes()
N_CE = sum(trips * sum(len(s[3]) for s in sets) for trips, sets in PASSES)

def moves(sets):
    return any(set(s[1]) != set(s[2]) for s in sets)

def row(ref, d):
    if isinstance(d, int):
        return ref.at[pl.ds(d * 8, 8), :]
    return ref.at[pl.ds(pl.multiple_of(d * 8, 8), 8), :]

def loop(trips, body):
    if trips == 1:
        body(0)
    else:
        def step(t, c):
            body(t)
            return c
        lax.fori_loop(0, trips, step, 0)

def sort_blocks(keys, vals, marks):
    at = 0
    side = 0
    for trips, sets in PASSES:
        count = sum(len(s[3]) for s in sets)
        key, val = keys[side], vals[side]
        if moves(sets):
            side = 1 - side
        key_to, val_to = keys[side], vals[side]
        def body(t, sets=sets, at=at, count=count, key=key, val=val, key_to=key_to, val_to=val_to):
            m = at + t * count
            for base, loads, stores, ces in sets:
                b = base(t)
                ks = [row(key, b + o)[...] for o in loads]
                vs = [row(val, b + o)[...] for o in loads]
                for i, j in ces:
                    c = ks[i] > ks[j]
                    row(marks, m)[...] = jnp.where(c, 1.0, 0.0)
                    m = m + 1
                    ks[i], ks[j] = jnp.minimum(ks[i], ks[j]), jnp.maximum(ks[i], ks[j])
                    vs[i], vs[j] = jnp.where(c, vs[j], vs[i]), jnp.where(c, vs[i], vs[j])
                for o, k, v in zip(stores, ks, vs):
                    row(key_to, b + o)[...] = k
                    row(val_to, b + o)[...] = v
        loop(trips, body)
        at += trips * count

def unsort_blocks(firsts, seconds, marks):
    at = N_CE
    side = 0
    for trips, sets in reversed(PASSES):
        count = sum(len(s[3]) for s in sets)
        at -= trips * count
        xa, xb = firsts[side], seconds[side]
        if moves(sets):
            side = 1 - side
        xa_to, xb_to = firsts[side], seconds[side]
        def body(t, sets=sets, at=at, count=count, xa=xa, xb=xb, xa_to=xa_to, xb_to=xb_to):
            m = at + t * count
            for base, loads, stores, ces in sets:
                b = base(t)
                xs = [row(xa, b + o)[...] for o in stores]
                ys = [row(xb, b + o)[...] for o in stores]
                for q in reversed(range(len(ces))):
                    i, j = ces[q]
                    c = row(marks, m + q)[...] > 0.5
                    xs[i], xs[j] = jnp.where(c, xs[j], xs[i]), jnp.where(c, xs[i], xs[j])
                    ys[i], ys[j] = jnp.where(c, ys[j], ys[i]), jnp.where(c, ys[i], ys[j])
                m = m + len(ces)
                for o, x, y in zip(loads, xs, ys):
                    row(xa_to, b + o)[...] = x
                    row(xb_to, b + o)[...] = y
        loop(trips, body)

def gather_cells(index, t_ref, v_ref, cell_ref, ct, cv, T, V):
    def rows(k, c):
        for j in range(32):
            b = k * 32 + j
            at = lax.shift_right_logical(index[b], 7)
            T[pl.ds(b, 1), :] = t_ref[pl.ds(at, 1), :]
            V[pl.ds(b, 1), :] = v_ref[pl.ds(at, 1), :]
        return c
    lax.fori_loop(0, 32, rows, 0)
    level = lax.rem(cell_ref[...], 128)
    depth = lax.broadcasted_iota(jnp.int32, (128, 128), 0)
    for g in range(8):
        here = depth == level[g:g + 1]
        for staged, cell in ((T, ct), (V, cv)):
            picked = jnp.where(here, staged[pl.ds(g * 128, 128), :].T, 0.0)
            cell[pl.ds(g, 1), :] = jnp.sum(picked, axis=0, keepdims=True)


def enter_blocks(rad_ref, flo_ref, mul_ref, R, F, M):
    def enter(g, c):
        to = pl.ds(g, 128, stride=8)
        R[to, :] = rad_ref[g].T
        F[to, :] = flo_ref[g].T
        M[to, :] = mul_ref[g].T
        return c
    lax.fori_loop(0, 8, enter, 0)


def condense_blocks(cnt_ref, heat_ref, R, S, C, F, M, ct_ref, cv_ref):
    counts = cnt_ref[...]
    zero = jnp.zeros((8, 128), jnp.float32)
    U = 32

    def init(t, w):
        for u in range(U):
            d = t * U + u
            r = row(R, d)[...]
            f = row(F, d)[...]
            m = jnp.where(counts > d, row(M, d)[...], 0.0)
            r2 = r * r
            f2 = f * f
            row(M, d)[...] = m
            row(R, d)[...] = r2
            row(S, d)[...] = lax.rsqrt(r2)
            row(F, d)[...] = f2
            row(C, d)[...] = (growth * solute) * f2 * f
            w = w + m * (r2 * r)
        return w
    weight = lax.fori_loop(0, 128 // U, init, zero)
    temp = ct_ref[...]
    wet = cv_ref[...]
    for _ in range(SUBSTEPS):
        sat = growth * ((1.0 + wet) * jnp.exp(-clausius * temp) - 1.0)
        def sub(t, w):
            for u in range(U):
                d = t * U + u
                r2 = row(R, d)[...]
                rs = row(S, d)[...]
                g = jnp.maximum(r2 + (sat + row(C, d)[...] * (rs * rs * rs)), row(F, d)[...])
                ns = lax.rsqrt(g)
                row(R, d)[...] = g
                row(S, d)[...] = ns
                w = w + row(M, d)[...] * (g * (g * ns))
            return w
        after = lax.fori_loop(0, 128 // U, sub, zero)
        condensed = after - weight
        weight = after
        wet = wet - condense * condensed
        temp = temp + latent * condense * condensed
    heat_ref[0:8, :] = temp - ct_ref[...]
    heat_ref[8:16, :] = wet - cv_ref[...]


def collect_blocks(R, S, C, F, M, marks, X):
    zero = jnp.zeros((8, 128), jnp.float32)
    U = 16

    def radii(t, c):
        for u in range(U):
            d = t * U + u
            row(R, d)[...] = row(R, d)[...] * row(S, d)[...]
        return c
    lax.fori_loop(0, 128 // U, radii, 0)
    sort_blocks((R, S), (M, C), marks)

    def both(t, carry):
        a0, a1, a3, a4, b0, b1, b3, b4 = carry
        for u in range(U):
            d = t * U + u
            r = row(R, d)[...]
            m = row(M, d)[...]
            r2 = r * r
            r3 = r2 * r
            r4 = r2 * r2
            gain = r4 * a0 + 2.0 * (r3 * a1 - r * a3) - a4
            w = m * r3
            a0 = a0 + w
            a1 = a1 + w * r
            a3 = a3 + w * r3
            a4 = a4 + w * r4
            grown = r3 + (time_step * collect) * gain
            row(S, d)[...] = jnp.where(m > 0.0, jnp.exp(jnp.log(grown) * (1.0 / 3.0)), 0.0)
            d = 127 - d
            r = row(R, d)[...]
            m = row(M, d)[...]
            r2 = r * r
            r3 = r2 * r
            r4 = r2 * r2
            loss = b4 + 2.0 * (r * b3 - r3 * b1) - r4 * b0
            b0 = b0 + m
            b1 = b1 + m * r
            b3 = b3 + m * r3
            b4 = b4 + m * r4
            row(C, d)[...] = m * jnp.exp((-time_step * collect) * loss)
        return a0, a1, a3, a4, b0, b1, b3, b4
    lax.fori_loop(0, 128 // U, both, (zero,) * 8)
    unsort_blocks((S, R), (C, F), marks)

    def leave(g, c):
        at = pl.ds(pl.multiple_of(g * 128, 128), 128)
        frm = pl.ds(g, 128, stride=8)
        for q, ref in enumerate((S, C)):
            for k, part in enumerate(split2(ref[frm, :].T)):
                X[at, k * 256 + q * 128:k * 256 + q * 128 + 128] = part
        return c
    lax.fori_loop(0, 8, leave, 0)


def mod(a, n):
    return lax.rem(a + n, n)


def split2(x):
    hi = x.astype(jnp.bfloat16)
    lo = (x - hi.astype(f32)).astype(jnp.bfloat16)
    return hi, lo


def row_moves(nx, ny, ix, iy, k, send_ref, recv_ref, s, r):
    px = mod(ix + k, nx)
    me = ix * ny + iy

    def body(i, c):
        py = mod(iy + i, ny)
        pltpu.make_async_remote_copy(
            src_ref=send_ref.at[pl.ds(pl.multiple_of((px * ny + py) * 8, 8), 8), :],
            dst_ref=recv_ref.at[pl.ds(pl.multiple_of(me * 8, 8), 8), :],
            send_sem=s, recv_sem=r, device_id=(px, py), device_id_type=MESH).start()
        return c
    lax.fori_loop(1 if k == 0 else 0, ny, body, 0)


def step_kernel(nx, ny, index, t_hbm, v_hbm, u_hbm, vv_hbm, w_hbm, rad_hbm, flo_hbm, mul_hbm, cnt_ref, square_ref, cell_ref, move_ref,
                to_ref, vo_ref, recv_ref,
                t_ref, v_ref, u_ref, vv_ref, w_ref, rad_ref, flo_ref, mul_ref, send_ref, heat_ref, R, S, C, F, M, marks, X, ct_ref, cv_ref,
                E, AX, AL, AH, AZ, AD, UE, VE, xin, yout, yin, vout, vin, W,
                a2a_send, a2a_recv, xs, xr, ys, yr, ws, wr, rows, loads):
    ix, iy = lax.axis_index("gx"), lax.axis_index("gy")
    me = ix * ny + iy
    right, left = (mod(ix + 1, nx), iy), (mod(ix - 1, nx), iy)
    upper, lower = (ix, mod(iy + 1, ny)), (ix, mod(iy - 1, ny))

    fetched = []
    for n, (src, dst) in enumerate(((rad_hbm, rad_ref), (flo_hbm, flo_ref), (mul_hbm, mul_ref), (t_hbm, t_ref), (v_hbm, v_ref), (vv_hbm, vv_ref), (u_hbm, u_ref), (w_hbm, w_ref))):
        fetched.append(pltpu.make_async_copy(src, dst, loads.at[n]))
        fetched[-1].start()
    barrier = pltpu.get_barrier_semaphore()
    for i in range(1, ny):
        pl.semaphore_signal(barrier, inc=1, device_id=(ix, mod(iy + i, ny)), device_id_type=MESH)
    for i in range(1, nx):
        pl.semaphore_signal(barrier, inc=1, device_id=(mod(ix + i, nx), iy), device_id_type=MESH)

    def remote(src, dst, s, r, to):
        return pltpu.make_async_remote_copy(src_ref=src, dst_ref=dst, send_sem=s, recv_sem=r, device_id=to, device_id_type=MESH)

    for n in (0, 1, 2):
        fetched[n].wait()
    enter_blocks(rad_ref, flo_ref, mul_ref, R, F, M)
    fetched[3].wait()
    fetched[4].wait()
    gather_cells(index, t_ref, v_ref, square_ref, ct_ref, cv_ref, S, C)
    condense_blocks(cnt_ref, heat_ref, R, S, C, F, M, ct_ref, cv_ref)
    fetched[5].wait()
    fetched[6].wait()
    vout[0] = vv_ref[pl.ds(31, 64, stride=32), :]
    vout[1] = vv_ref[pl.ds(0, 64, stride=32), :]
    for e in range(6):
        for at in (WY + 7, WY + 40):
            E[e, pl.ds(at, 64, stride=WY), :] = jnp.zeros((64, 128), f32)
        E[e, pl.ds(65 * WY + 8, 32), :] = jnp.zeros((32, 128), f32)
    pl.semaphore_wait(barrier, nx + ny - 2)
    for i in range(1, ny):
        pl.semaphore_signal(rows, inc=1, device_id=(ix, mod(iy + i, ny)), device_id_type=MESH)
    winds = [
        remote(u_ref.at[pl.ds(63 * 32, 32), :], UE.at[0], ws.at[0], wr.at[0], right),
        remote(u_ref.at[pl.ds(0, 32), :], UE.at[1], ws.at[1], wr.at[1], left),
        remote(vout.at[0], vin.at[0], ws.at[2], wr.at[2], upper),
        remote(vout.at[1], vin.at[1], ws.at[3], wr.at[3], lower),
    ]
    for c in winds:
        c.start()
    def plane(x):
        return x * WY + 8

    def exchange(s, q):
        n = 4 * s + 2 * q
        e = E.at[2 * s + q]
        yout[n] = E[2 * s + q, pl.ds(plane(1) + 31, 64, stride=WY), :]
        yout[n + 1] = E[2 * s + q, pl.ds(plane(1), 64, stride=WY), :]
        moves = [
            remote(yout.at[n], yin.at[n], ys.at[n], yr.at[n], upper),
            remote(yout.at[n + 1], yin.at[n + 1], ys.at[n + 1], yr.at[n + 1], lower),
            remote(e.at[pl.ds(plane(64), 32), :], xin.at[n], xs.at[n], xr.at[n], right),
            remote(e.at[pl.ds(plane(1), 32), :], xin.at[n + 1], xs.at[n + 1], xr.at[n + 1], left),
        ]
        for c in moves:
            c.start()
        return moves

    collect_blocks(R, S, C, F, M, marks, X)
    moves_to = move_ref[...]

    def place(k):
        at = pl.multiple_of(mod(ix + k, nx) * (ny * 8), ny * 8)
        ids = lax.broadcasted_iota(jnp.int32, (ny * 8, 1024), 0) + at
        hot = jnp.where(ids == moves_to, 1.0, 0.0).astype(jnp.bfloat16)
        d = jnp.dot(hot, X[...], preferred_element_type=f32)
        send_ref[pl.ds(at, ny * 8), :] = d[:, 0:256] + d[:, 256:512]

    def send_row(k):
        row_moves(nx, ny, ix, iy, k, send_ref, recv_ref, a2a_send, a2a_recv)

    order = sorted(range(nx), key=lambda k: -min(k, nx - k))
    place(order[0])
    pl.semaphore_wait(rows, ny - 1)
    send_row(order[0])
    for n, k in enumerate(order[1:]):
        place(k)
        if n < 3:
            send_row(k)
    mine = pl.ds(pl.multiple_of(me * 8, 8), 8)
    recv_ref[mine, :] = send_ref[mine, :]

    zed = lax.rem(square_ref[...], 128).astype(f32).T.astype(jnp.int32)
    heat = heat_ref[...].T
    lanes = lax.broadcasted_iota(jnp.int32, (128, 128), 1)
    for g in range(8):
        level = lanes == zed[:, g:g + 1]
        at = pl.ds(g * 128, 128)
        for q in range(2):
            h = jnp.where(level, heat[:, q * 8 + g:q * 8 + g + 1], 0.0)
            hi, lo = split2(h)
            W[at, q * 128:q * 128 + 128] = hi
            W[at, 256 + q * 128:256 + q * 128 + 128] = lo
    cells = lax.shift_right_logical(cell_ref[...], 7)

    def scatter(k, c):
        at = pl.multiple_of(k * 128, 128)
        ids = lax.broadcasted_iota(jnp.int32, (128, 1024), 0) + at
        hot = jnp.where(ids == cells, 1.0, 0.0).astype(jnp.bfloat16)
        d = jnp.dot(hot, W[...], preferred_element_type=f32)
        for q, ref in ((0, t_ref), (1, v_ref)):
            add = d[:, q * 128:q * 128 + 128] + d[:, 256 + q * 128:256 + q * 128 + 128]
            new = ref[pl.ds(at, 128), :] + add
            for j in range(4):
                E[q, pl.ds(pl.multiple_of((k * 4 + j + 1) * WY + 8, 8), 32), :] = new[j * 32:j * 32 + 32]
        return c
    lax.fori_loop(0, 16, scatter, 0)

    moves = [exchange(0, 0), exchange(0, 1)]
    sent = [*winds, *moves[0], *moves[1]]
    send_row(order[4])
    send_row(order[5])

    fetched[7].wait()
    for c in winds:
        c.wait_recv()

    AX[pl.ds(0, 32), :] = 0.25 * (UE[0] + u_ref[pl.ds(0, 32), :])
    AX[pl.ds(64 * 32, 32), :] = 0.25 * (u_ref[pl.ds(63 * 32, 32), :] + UE[1])
    VE[pl.ds(7, 64, stride=WY), :] = vin[0]
    VE[pl.ds(40, 64, stride=WY), :] = vin[1]
    lane = lax.broadcasted_iota(jnp.int32, (32, 128), 1)

    def enter(k, c):
        for j in range(8):
            x = k * 8 + j
            VE[pl.ds(pl.multiple_of(x * WY + 8, 8), 32), :] = vv_ref[pl.ds(pl.multiple_of(x * 32, 32), 32), :]
        return c
    lax.fori_loop(0, 8, enter, 0)

    def faces(k, c):
        for j in range(8):
            x = k * 8 + j
            at = pl.ds(pl.multiple_of(x * 32, 32), 32)
            here = vv_ref[at, :]
            AL[at, :] = 0.25 * (here + VE[pl.ds(x * WY + 7, 32), :])
            AH[at, :] = 0.25 * (here + VE[pl.ds(x * WY + 9, 32), :])
            w = w_ref[at, :]
            AZ[at, :] = jnp.where(lane == 127, 0.0, 0.25 * (w + pltpu.roll(w, 127, 1)))
            AD[at, :] = jnp.where(lane == 0, 0.0, 0.25 * (w + pltpu.roll(w, 1, 1)))
        return c
    lax.fori_loop(0, 8, faces, 0)

    def face_x(k, c):
        for j in range(7):
            x = k * 7 + j + 1
            AX[pl.ds(pl.multiple_of(x * 32, 32), 32), :] = 0.25 * (u_ref[pl.ds(pl.multiple_of(x * 32 - 32, 32), 32), :] + u_ref[pl.ds(pl.multiple_of(x * 32, 32), 32), :])
        return c
    lax.fori_loop(0, 9, face_x, 0)

    for s, weight in enumerate((advect_step / 3.0, advect_step / 2.0, advect_step)):
        for q in range(2):
            src = E.at[2 * s + q]
            start = E.at[q]
            def step(k, carry, q=q, src=src, start=start, s=s, weight=weight):
                f, low = carry
                for j in range(UNROLL):
                    x = k * UNROLL + j
                    at = pl.ds(pl.multiple_of(x * 32, 32), 32)
                    p = pl.multiple_of((x + 1) * WY + 8, 8)
                    after = src[pl.ds(pl.multiple_of(p + WY, 8), 32), :]
                    high = AX[pl.ds(pl.multiple_of(x * 32 + 32, 32), 32), :] * (f + after)
                    fy = AH[at, :] * (f + src[pl.ds(p + 1, 32), :]) - AL[at, :] * (src[pl.ds(p - 1, 32), :] + f)
                    fz = AZ[at, :] * (f + pltpu.roll(f, 127, 1)) - AD[at, :] * (pltpu.roll(f, 1, 1) + f)
                    out = start[pl.ds(p, 32), :] - weight * ((high - low) + fy + fz)
                    if s < 2:
                        E[2 * s + 2 + q, pl.ds(p, 32), :] = out
                    else:
                        (to_ref, vo_ref)[q][at, :] = out
                    f, low = after, high
                return f, low
            f0 = src[pl.ds(plane(1), 32), :]
            lax.fori_loop(0, 64 // UNROLL, step, (f0, AX[pl.ds(0, 32), :] * f0))
            if s == 0:
                send_row(order[6 + q])
            for c in moves[q]:
                c.wait_recv()
            if s < 2:
                dst, base, wide = E.at[2 * s + 2 + q], plane(1), WY
            else:
                dst, base, wide = (to_ref, vo_ref)[q], 0, 32
            n = 4 * s + 2 * q
            first, last = pl.ds(base, 32), pl.ds(base + 63 * wide, 32)
            dst[first, :] = dst[first, :] + weight * (AX[pl.ds(0, 32), :] * xin[n])
            dst[last, :] = dst[last, :] - weight * (AX[pl.ds(64 * 32, 32), :] * xin[n + 1])
            bottom, top = pl.ds(base, 64, stride=wide), pl.ds(base + 31, 64, stride=wide)
            dst[bottom, :] = dst[bottom, :] + weight * (AL[pl.ds(0, 64, stride=32), :] * yin[n])
            dst[top, :] = dst[top, :] - weight * (AH[pl.ds(31, 64, stride=32), :] * yin[n + 1])
            if s < 2:
                moves[q] = exchange(s + 1, q)
                sent += moves[q]
    for c in sent:
        c.wait_send()
    rest = pl.ds(8, 8 * (nx * ny - 1))
    whole = remote(recv_ref.at[rest, :], recv_ref.at[rest, :], a2a_send, a2a_recv, right)
    whole.wait_send()
    whole.wait_recv()


def step_call(mesh_shape, index, fields, droplets, counts, square, cells, moves):
    nx, ny = mesh_shape
    VM = pl.BlockSpec(memory_space=pltpu.VMEM)
    HB = pl.BlockSpec(memory_space=pltpu.HBM)
    bf16 = jnp.bfloat16
    DMA = pltpu.SemaphoreType.DMA
    plane = pltpu.VMEM((2048, 128), f32)
    block = pltpu.VMEM((1024, 128), f32)
    return pl.pallas_call(
        functools.partial(step_kernel, nx, ny),
        out_shape=(jax.ShapeDtypeStruct((2048, 128), f32), jax.ShapeDtypeStruct((2048, 128), f32), jax.ShapeDtypeStruct((1024, 256), f32)),
        in_specs=[pl.BlockSpec(memory_space=pltpu.SMEM)] + [HB] * 8 + [VM] * 4,
        out_specs=[VM] * 3,
        scratch_shapes=[plane] * 5 + [pltpu.VMEM((8, 128, 128), f32)] * 3 + [pltpu.VMEM((1024, 256), f32), pltpu.VMEM((16, 128), f32)] + [block] * 5
        + [pltpu.VMEM((N_CE * 8, 128), f32), pltpu.VMEM((1024, 512), bf16), pltpu.VMEM((8, 128), f32), pltpu.VMEM((8, 128), f32)]
        + [
            pltpu.VMEM((6, WX * WY, 128), f32), pltpu.VMEM((65 * 32, 128), f32), plane, plane, plane, plane,
            pltpu.VMEM((2, 32, 128), f32), pltpu.VMEM((64 * WY, 128), f32),
            pltpu.VMEM((12, 32, 128), f32), pltpu.VMEM((12, 64, 128), f32), pltpu.VMEM((12, 64, 128), f32),
            pltpu.VMEM((2, 64, 128), f32), pltpu.VMEM((2, 64, 128), f32), pltpu.VMEM((1024, 512), bf16),
            DMA, DMA, DMA((12,)), DMA((12,)), DMA((12,)), DMA((12,)), DMA((4,)), DMA((4,)), pltpu.SemaphoreType.REGULAR, DMA((8,)),
        ],
        compiler_params=pltpu.CompilerParams(vmem_limit_bytes=50 * 2**20, collective_id=0, has_side_effects=True),
        cost_estimate=pl.CostEstimate(flops=5_000_000_000, bytes_accessed=8_000_000, transcendentals=0),
        name="step",
    )(index, *fields, *droplets, counts, square, cells, moves)


def triangle(n):
    return lax.broadcasted_iota(jnp.int32, (n, n), 0) < lax.broadcasted_iota(jnp.int32, (n, n), 1)


def compact_kernel(recv_ref, ti_ref, vi_ref, to_ref, vo_ref, ro_ref, mo_ref, X, sems):
    passing = [pltpu.make_async_copy(ti_ref, to_ref, sems.at[0]), pltpu.make_async_copy(vi_ref, vo_ref, sems.at[1])]
    for c in passing:
        c.start()
    rows = []
    for g in range(8):
        rows.append(recv_ref[pl.ds(g * 128, 128), 128:256].T[0:1])
    first = jnp.concatenate(rows, axis=0)
    taken = jnp.where(first > 0.0, 1.0, 0.0)
    within = jnp.dot(taken.astype(jnp.bfloat16), jnp.where(triangle(128), 1.0, 0.0).astype(jnp.bfloat16), preferred_element_type=f32)
    total = jnp.sum(taken, axis=1, keepdims=True)
    pos = []
    before = jnp.zeros((1, 1), f32)
    for g in range(8):
        pos.append(jnp.where(first[g:g + 1] > 0.0, within[g:g + 1] + before, -1.0))
        before = before + total[g:g + 1]
    pos = jnp.concatenate(pos, axis=1).astype(jnp.int32)
    for g in range(8):
        at = pl.ds(g * 128, 128)
        for k, part in enumerate(split2(recv_ref[at, :])):
            X[at, k * 256:k * 256 + 256] = part
    for n in range(4):
        ids = lax.broadcasted_iota(jnp.int32, (128, 1024), 0) + n * 128
        hot = jnp.where(ids == pos, 1.0, 0.0).astype(jnp.bfloat16)
        d = jnp.dot(hot, X[...], preferred_element_type=f32)
        d = d[:, 0:256] + d[:, 256:512]
        ro_ref[pl.ds(n * 128, 128), :] = d[:, 0:128]
        mo_ref[pl.ds(n * 128, 128), :] = d[:, 128:256]
    for c in passing:
        c.wait()


def compacted(recv, t, v):
    VM = pl.BlockSpec(memory_space=pltpu.VMEM)
    field = jax.ShapeDtypeStruct(t.shape, f32)
    drops = jax.ShapeDtypeStruct((512, 128), f32)
    return pl.pallas_call(
        compact_kernel,
        out_shape=(field, field, drops, drops),
        in_specs=[VM] * 3, out_specs=[pl.BlockSpec(memory_space=pltpu.HBM)] * 2 + [VM] * 2,
        scratch_shapes=[pltpu.VMEM((1024, 512), jnp.bfloat16), pltpu.SemaphoreType.DMA((2,))],
        compiler_params=pltpu.CompilerParams(vmem_limit_bytes=12 * 2**20),
        cost_estimate=pl.CostEstimate(flops=800_000_000, bytes_accessed=2_000_000, transcendentals=0),
        name="compact",
    )(recv, t, v)


def body(
    shape,
    tprime,
    vapor,
    wind_u,
    wind_v,
    wind_w,
    radius,
    min_radius,
    multiplicity,
    drop_counts,
    cell_index,
    move_list,
):
    home = radius.shape[0]
    columns = tprime.shape[0] * tprime.shape[1]
    levels = tprime.shape[2]
    flat = [pltpu.with_memory_space_constraint(a.reshape(columns, levels), pltpu.HBM) for a in (tprime, vapor, wind_u, wind_v, wind_w)]
    square = (8, home // 8)
    cells = cell_index.reshape(square)
    temperature, humidity, recv = step_call(
        shape,
        cell_index,
        flat,
        [pltpu.with_memory_space_constraint(a.reshape(8, home // 8, a.shape[1]), pltpu.HBM) for a in (radius, min_radius, multiplicity)],
        drop_counts.reshape(square),
        cells,
        cell_index.reshape(1, home),
        move_list.reshape(1, home),
    )
    temperature, humidity, radius_out, multiplicity_out = compacted(recv, temperature, humidity)
    return (
        temperature.reshape(tprime.shape),
        humidity.reshape(vapor.shape),
        radius_out,
        multiplicity_out,
    )


def solution(mesh):
    placed = (
        P("gx", "gy", None),
        P("gx", "gy", None),
        P("gx", "gy", None),
        P("gx", "gy", None),
        P("gx", "gy", None),
        P(("gx", "gy"), None),
        P(("gx", "gy"), None),
        P(("gx", "gy"), None),
        P(("gx", "gy")),
        P(("gx", "gy")),
        P(("gx", "gy")),
    )
    return jax.shard_map(
        functools.partial(body, (mesh.shape["gx"], mesh.shape["gy"])),
        mesh=mesh,
        in_specs=placed,
        out_specs=(
            P("gx", "gy", None),
            P("gx", "gy", None),
            P(("gx", "gy"), None),
            P(("gx", "gy"), None),
        ),
        check_vma=False,
    )
```
